8 devices in a mesh: data: 8 (over z, y, x, core).
Axes of the slice: x: 2, y: 2, z: 1, core: 2. Of those that a mesh axis runs over, the one named last changes fastest.
Arguments:
- x_in: bfloat16 [48, 384, 512], P('data')
- g_out: bfloat16 [48, 384, 512], P('data')
- step_emb: bfloat16 [3, 512], replicated
- w_q: bfloat16 [512, 8, 64], replicated
- w_k: bfloat16 [512, 8, 64], replicated
- w_v: bfloat16 [512, 8, 64], replicated
- w_o: bfloat16 [8, 64, 512], replicated
- w_up: bfloat16 [512, 2048], replicated
- w_down: bfloat16 [2048, 512], replicated
Outputs:
- output 1: float32 [512, 8, 64], replicated
- output 2: float32 [512, 8, 64], replicated
- output 3: float32 [512, 8, 64], replicated
- output 4: float32 [8, 64, 512], replicated
- output 5: float32 [512, 2048], replicated
- output 6: float32 [2048, 512], replicated
- output 7: bfloat16 [48, 384, 512], P('data')
All inputs are finite; a program needn't handle non-finite values.
Results may differ from the reference program's by a relative error of at most 0.02.
Values are sent between devices in bfloat16 or wider.
A program may use at most 1 GiB of HBM per device.

```python
import math
import functools
import jax
import jax.numpy as jnp
from jax import lax

D = 512
FF = 2048
HEADS = 8
SEQ = 384
LAYERS = 3
BATCH = 48
HEAD = D // HEADS
NORM_EPS = 1e-6


def setup_inputs(seed: int = 0) -> dict:
    sub_keys = jax.random.split(jax.random.key(seed), 9)
    out_gain = 2.0 / math.sqrt(LAYERS)
    x_in = jax.random.normal(sub_keys[0], (BATCH, SEQ, D), jnp.float32)
    g_out = jax.random.normal(sub_keys[1], (BATCH, SEQ, D), jnp.float32)
    step_emb = jax.random.normal(sub_keys[2], (LAYERS, D), jnp.float32) / math.sqrt(LAYERS)
    w_q = jax.random.normal(sub_keys[3], (D, HEADS, HEAD), jnp.float32) * D ** -0.5
    w_k = jax.random.normal(sub_keys[4], (D, HEADS, HEAD), jnp.float32) * D ** -0.5
    w_v = jax.random.normal(sub_keys[5], (D, HEADS, HEAD), jnp.float32) * D ** -0.5
    w_o = jax.random.normal(sub_keys[6], (HEADS, HEAD, D), jnp.float32) * (D ** -0.5 * out_gain)
    w_up = jax.random.normal(sub_keys[7], (D, FF), jnp.float32) * D ** -0.5
    w_down = jax.random.normal(sub_keys[8], (FF, D), jnp.float32) * (FF ** -0.5 * out_gain)
    return {
        'x_in': x_in.astype(jnp.bfloat16),
        'g_out': g_out.astype(jnp.bfloat16),
        'step_emb': step_emb.astype(jnp.bfloat16),
        'w_q': w_q.astype(jnp.bfloat16),
        'w_k': w_k.astype(jnp.bfloat16),
        'w_v': w_v.astype(jnp.bfloat16),
        'w_o': w_o.astype(jnp.bfloat16),
        'w_up': w_up.astype(jnp.bfloat16),
        'w_down': w_down.astype(jnp.bfloat16),
    }


def rms_norm(x_val):
    x_f32 = x_val.astype(jnp.float32)
    return (x_f32 * lax.rsqrt(jnp.mean(x_f32 * x_f32, axis=-1, keepdims=True) + NORM_EPS)).astype(jnp.bfloat16)


def shared_block(weight_set, x_prev, step_vec):
    w_q, w_k, w_v, w_o, w_up, w_down = weight_set
    x_cur = x_prev + step_vec
    u_norm = rms_norm(x_cur).astype(jnp.float32)
    q_heads = jnp.einsum('sd,dhe->she', u_norm, w_q).astype(jnp.bfloat16)
    k_heads = jnp.einsum('sd,dhe->she', u_norm, w_k).astype(jnp.bfloat16)
    v_heads = jnp.einsum('sd,dhe->she', u_norm, w_v).astype(jnp.bfloat16)
    scores = jnp.einsum('qhe,khe->hqk', q_heads.astype(jnp.float32), k_heads.astype(jnp.float32)).astype(jnp.bfloat16)
    prob_mat = jax.nn.softmax(scores.astype(jnp.float32) * HEAD ** -0.5, axis=-1).astype(jnp.bfloat16)
    mix_heads = jnp.einsum('hqk,khe->qhe', prob_mat.astype(jnp.float32), v_heads.astype(jnp.float32)).astype(jnp.bfloat16)
    attn_out = jnp.einsum('qhe,hed->qd', mix_heads.astype(jnp.float32), w_o).astype(jnp.bfloat16)
    h_mid = x_cur + attn_out
    m_norm = rms_norm(h_mid).astype(jnp.float32)
    z_up = jnp.dot(m_norm, w_up, preferred_element_type=jnp.float32).astype(jnp.bfloat16)
    g_act = jax.nn.gelu(z_up.astype(jnp.float32), approximate=True).astype(jnp.bfloat16)
    y_down = jnp.dot(g_act.astype(jnp.float32), w_down, preferred_element_type=jnp.float32).astype(jnp.bfloat16)
    return h_mid + y_down


def run_stack(weight_set, x_seq, step_emb):
    def layer_step(x_cur, step_vec):
        return jax.checkpoint(shared_block)(weight_set, x_cur, step_vec), None
    x_out, unused = lax.scan(layer_step, x_seq, step_emb)
    return x_out


def reference(x_in, g_out, step_emb, w_q, w_k, w_v, w_o, w_up, w_down):
    weight_set = tuple(w.astype(jnp.float32) for w in (w_q, w_k, w_v, w_o, w_up, w_down))

    def seq_grads(grad_acc, seq_pair):
        x_seq, g_seq = seq_pair
        x_out, pull_back = jax.vjp(functools.partial(run_stack, step_emb=step_emb), weight_set, x_seq)
        d_weights, d_x = pull_back(g_seq)
        return tuple(a + b for a, b in zip(grad_acc, d_weights)), d_x

    zero_acc = tuple(jnp.zeros_like(w) for w in weight_set)
    grad_sums, grad_x = lax.scan(seq_grads, zero_acc, (x_in, g_out))
    return (grad_sums[0], grad_sums[1], grad_sums[2], grad_sums[3], grad_sums[4], grad_sums[5], grad_x)
```

```python
import functools

import jax
import jax.numpy as jnp
from jax import lax
from jax.experimental import pallas as pl
from jax.experimental.pallas import tpu as pltpu
from jax.sharding import PartitionSpec as P

NORM_EPS = 1e-6
BF = jnp.bfloat16
F32 = jnp.float32
GELU_C = 0.7978845608028654
GELU_A = 0.044715


def mm(a, b):
    return lax.dot_general(a, b, (((1,), (0,)), ((), ())), preferred_element_type=F32)


def mm_nt(a, b):
    return lax.dot_general(a, b, (((1,), (1,)), ((), ())), preferred_element_type=F32)


def mm_tn(a, b):
    return lax.dot_general(a, b, (((0,), (0,)), ((), ())), preferred_element_type=F32)


def rms_scale(xf):
    return lax.rsqrt(jnp.mean(xf * xf, axis=-1, keepdims=True) + NORM_EPS)


def rms_bwd(x, dy):
    xf = x.astype(F32)
    gf = dy.astype(F32)
    r = rms_scale(xf)
    dot = jnp.mean(xf * gf, axis=-1, keepdims=True)
    return (gf * r - xf * (r * r * r * dot)).astype(BF)


def gelu_fwd(z):
    zf = z.astype(F32)
    t = jnp.tanh(GELU_C * (zf + GELU_A * (zf * zf * zf)))
    return (zf * (0.5 * (1.0 + t))).astype(BF)


def gelu_bwd(z, dg):
    zf = z.astype(F32)
    z2 = zf * zf
    t = jnp.tanh(GELU_C * (zf + GELU_A * (zf * z2)))
    slope = 0.5 * (1.0 + t) + (0.5 * zf) * (1.0 - t * t) * (GELU_C + (3.0 * GELU_C * GELU_A) * z2)
    return (dg.astype(F32) * slope).astype(BF)


def head_stack(a4, n_sub, width):
    lane = lax.broadcasted_iota(jnp.int32, a4.shape, 1)
    zero = jnp.zeros_like(a4)
    return jnp.concatenate([jnp.where((lane >= h * width) & (lane < (h + 1) * width), a4, zero) for h in range(n_sub)], axis=0)


def step_kernel(cfg, x_ref, g_ref, emb_ref, wqkv_ref, wo_ref, wup_ref, wdn_ref,
                dx_ref, gqkv_ref, go_ref, gup_ref, gdn_ref,
                xs, uT, qkv, st, stat, mixT, hs, mT, zs, gs, dmid, doutT, dcur,
                a_qkv, a_o, a_up, a_dn, sem):
    S, D, FF, HW, L = cfg
    QW = 256
    NQ = D // QW
    NS = QW // HW
    scale = HW ** -0.5
    step = pl.program_id(0)
    last = pl.num_programs(0) - 1

    @pl.when(step == 0)
    def _():
        a_qkv[...] = jnp.zeros_like(a_qkv)
        a_o[...] = jnp.zeros_like(a_o)
        a_up[...] = jnp.zeros_like(a_up)
        a_dn[...] = jnp.zeros_like(a_dn)

    xs[0] = x_ref[0] + emb_ref[0].astype(BF)

    def fwd(l, carry):
        rows = pl.ds(pl.multiple_of(l * S, S), S)
        x = xs[l]
        xf = x.astype(F32)
        u = (xf * rms_scale(xf)).astype(BF)
        uT[:, rows] = u.T
        for j in range(3):
            cols = slice(j * D, (j + 1) * D)
            qkv[rows, cols] = mm(u, wqkv_ref[:, cols]).astype(BF)
        for c in range(NQ):
            q4 = qkv[rows, c * QW:(c + 1) * QW]
            k4 = qkv[rows, D + c * QW:D + (c + 1) * QW]
            v4 = qkv[rows, 2 * D + c * QW:2 * D + (c + 1) * QW]
            qm = head_stack(q4, NS, HW)
            vT = v4.T
            for pr in range(NS // 2):
                cols = slice(pr * 2 * S, (pr + 1) * 2 * S)
                sb = mm_nt(k4, qm[cols]).astype(BF)
                st[l, c, :, cols] = sb
                s = sb.astype(F32)
                m = jnp.max(s, axis=0, keepdims=True)
                e = jnp.exp((s - m) * scale)
                inv = 1.0 / jnp.sum(e, axis=0, keepdims=True)
                stat[l, c, 0:1, cols] = m
                stat[l, c, 1:2, cols] = inv
                p = (e * inv).astype(BF)
                for hh in range(2):
                    h = pr * 2 + hh
                    o = mm(vT[h * HW:(h + 1) * HW], p[:, hh * S:(hh + 1) * S])
                    mixT[c * QW + h * HW:c * QW + (h + 1) * HW, rows] = o.astype(BF)
        h_mid = x + mm_tn(mixT[:, rows], wo_ref[...]).astype(BF)
        hs[l] = h_mid
        hf = h_mid.astype(F32)
        mn = (hf * rms_scale(hf)).astype(BF)
        mT[:, rows] = mn.T
        for j in range(FF // D):
            cols = slice(j * D, (j + 1) * D)
            z = mm(mn, wup_ref[:, cols]).astype(BF)
            zs[rows, cols] = z
            gs[rows, cols] = gelu_fwd(z)

        @pl.when(l < L - 1)
        def _():
            y = mm(gs[rows, :], wdn_ref[...]).astype(BF)
            xs[l + 1] = (h_mid + y) + emb_ref[l + 1].astype(BF)
        return carry

    lax.fori_loop(0, L, fwd, 0)
    dcur[...] = g_ref[0]

    def bwd(i, carry):
        l = L - 1 - i
        rows = pl.ds(pl.multiple_of(l * S, S), S)
        d_out = dcur[...]
        doutT[:, rows] = d_out.T
        for j in range(FF // D):
            cols = slice(j * D, (j + 1) * D)
            d_act = mm_nt(d_out, wdn_ref[cols, :]).astype(BF)
            zs[rows, cols] = gelu_bwd(zs[rows, cols], d_act)
        d_norm = mm_nt(zs[rows, :], wup_ref[...]).astype(BF)
        d_mid = d_out + rms_bwd(hs[l], d_norm)
        dmid[rows, :] = d_mid
        d_mix = mm_nt(d_mid, wo_ref[...]).astype(BF)
        for c in range(NQ):
            qc = slice(c * QW, (c + 1) * QW)
            kc = slice(D + c * QW, D + (c + 1) * QW)
            vc = slice(2 * D + c * QW, 2 * D + (c + 1) * QW)
            q4 = qkv[rows, qc]
            k4 = qkv[rows, kc]
            v4 = qkv[rows, vc]
            qm = head_stack(q4, NS, HW)
            dom = head_stack(d_mix[:, qc], NS, HW)
            kT = k4.T
            dv = None
            dk = None
            dqT = []
            for pr in range(NS // 2):
                cols = slice(pr * 2 * S, (pr + 1) * 2 * S)
                dp = mm_nt(v4, dom[cols]).astype(BF).astype(F32)
                s = st[l, c, :, cols].astype(F32)
                p = jnp.exp((s - stat[l, c, 0:1, cols]) * scale) * stat[l, c, 1:2, cols]
                dv_p = mm(p.astype(BF), dom[cols])
                delta = jnp.sum(dp * p, axis=0, keepdims=True)
                ds = ((p * (dp - delta)) * scale).astype(BF)
                dk_p = mm(ds, qm[cols])
                dv = dv_p if dv is None else dv + dv_p
                dk = dk_p if dk is None else dk + dk_p
                for hh in range(2):
                    h = pr * 2 + hh
                    dqT.append(mm(kT[h * HW:(h + 1) * HW], ds[:, hh * S:(hh + 1) * S]).astype(BF))
            qkv[rows, qc] = jnp.concatenate(dqT, axis=0).T
            qkv[rows, kc] = dk.astype(BF)
            qkv[rows, vc] = dv.astype(BF)
        d_norm_x = mm_nt(qkv[rows, :], wqkv_ref[...]).astype(BF)
        dcur[...] = d_mid + rms_bwd(xs[l], d_norm_x)
        return carry

    lax.fori_loop(0, L, bwd, 0)
    dx_ref[0] = dcur[...]

    def wg(acc, lhs, rhs, n):
        def body(j, carry):
            cols = pl.ds(pl.multiple_of(j * D, D), D)
            acc[:, cols] = acc[:, cols] + mm(lhs[...], rhs[:, cols])
            return carry
        lax.fori_loop(0, n, body, 0)

    wg(a_qkv, uT, qkv, 3)
    wg(a_o, mixT, dmid, 1)
    wg(a_up, mT, zs, FF // D)
    wg(a_dn, doutT, gs, FF // D)

    @pl.when(step == last)
    def _():
        pairs = ((a_qkv, gqkv_ref), (a_o, go_ref), (a_up, gup_ref), (a_dn, gdn_ref))
        copies = [pltpu.make_async_copy(s_, d_, sem.at[i]) for i, (s_, d_) in enumerate(pairs)]
        for cp in copies:
            cp.start()
        for cp in copies:
            cp.wait()


def local_grads(x, g, emb, wqkv, wo, wup, wdn, HW):
    B, S, D = x.shape
    FF = wup.shape[1]
    L = emb.shape[0]
    emb = emb.astype(F32).reshape(L, 1, D)
    T = L * S
    NQ = D // 256
    NS = 256 // HW
    const = lambda shape: pl.BlockSpec(shape, lambda b: (0,) * len(shape), pipeline_mode=pl.Buffered(1))
    seq = pl.BlockSpec((1, S, D), lambda b: (b, 0, 0))
    hbm = pl.BlockSpec(memory_space=pl.ANY)
    return pl.pallas_call(
        functools.partial(step_kernel, (S, D, FF, HW, L)),
        name='block_grads',
        grid=(B,),
        in_specs=[seq, seq, const(emb.shape), const(wqkv.shape), const(wo.shape), const(wup.shape), const(wdn.shape)],
        out_specs=[seq, hbm, hbm, hbm, hbm],
        out_shape=[
            jax.ShapeDtypeStruct(x.shape, BF),
            jax.ShapeDtypeStruct((D, 3 * D), F32),
            jax.ShapeDtypeStruct((D, D), F32),
            jax.ShapeDtypeStruct((D, FF), F32),
            jax.ShapeDtypeStruct((D, FF), F32),
        ],
        scratch_shapes=[
            pltpu.VMEM((L, S, D), BF),
            pltpu.VMEM((D, T), BF),
            pltpu.VMEM((T, 3 * D), BF),
            pltpu.VMEM((L, NQ, S, NS * S), BF),
            pltpu.VMEM((L, NQ, 8, NS * S), F32),
            pltpu.VMEM((D, T), BF),
            pltpu.VMEM((L, S, D), BF),
            pltpu.VMEM((D, T), BF),
            pltpu.VMEM((T, FF), BF),
            pltpu.VMEM((T, FF), BF),
            pltpu.VMEM((T, D), BF),
            pltpu.VMEM((D, T), BF),
            pltpu.VMEM((S, D), BF),
            pltpu.VMEM((D, 3 * D), F32),
            pltpu.VMEM((D, D), F32),
            pltpu.VMEM((D, FF), F32),
            pltpu.VMEM((D, FF), F32),
            pltpu.SemaphoreType.DMA((4,)),
        ],
        compiler_params=pltpu.CompilerParams(dimension_semantics=('arbitrary',), vmem_limit_bytes=67043328),
    )(x, g, emb, wqkv, wo, wup, wdn)


def solution(mesh):
    batch_spec = P('data', None, None)

    def per_device(x_loc, g_loc, step_emb, w_q, w_k, w_v, w_o, w_up, w_down):
        D, H, HW = w_q.shape
        wqkv = jnp.concatenate([w.reshape(D, H * HW) for w in (w_q, w_k, w_v)], axis=1)
        d_x, gqkv, go, gup, gdnT = local_grads(x_loc, g_loc, step_emb, wqkv, w_o.reshape(H * HW, D), w_up, w_down, HW)
        gqkv, go, gup, gdnT = lax.psum((gqkv, go, gup, gdnT), 'data')
        parts = [gqkv[:, i * H * HW:(i + 1) * H * HW].reshape(D, H, HW) for i in range(3)]
        return (parts[0], parts[1], parts[2], go.reshape(H, HW, D), gup, gdnT.T, d_x)

    return jax.shard_map(per_device, mesh=mesh, in_specs=(batch_spec, batch_spec, P(), P(), P(), P(), P(), P(), P()), out_specs=(P(), P(), P(), P(), P(), P(), batch_spec), check_vma=False)
```

```python
import functools

import jax
import jax.numpy as jnp
from jax import lax
from jax.experimental import pallas as pl
from jax.experimental.pallas import tpu as pltpu
from jax.sharding import PartitionSpec as P

NORM_EPS = 1e-6
BF = jnp.bfloat16
F32 = jnp.float32
GELU_C = 0.7978845608028654
GELU_A = 0.044715
LOG2E = 1.4426950408889634
MESH = pl.DeviceIdType.MESH
UNIT = 512
QW = 256
VMEM_MAX = 67043328


def mm(a, b):
    return lax.dot_general(a, b, (((1,), (0,)), ((), ())), preferred_element_type=F32)


def mm_nt(a, b):
    return lax.dot_general(a, b, (((1,), (1,)), ((), ())), preferred_element_type=F32)


def mm_tn(a, b):
    return lax.dot_general(a, b, (((0,), (0,)), ((), ())), preferred_element_type=F32)


def rms_scale(xf):
    return lax.rsqrt(jnp.mean(xf * xf, axis=-1, keepdims=True) + NORM_EPS)


def rms_bwd(x, dy):
    xf = x.astype(F32)
    gf = dy.astype(F32)
    r = rms_scale(xf)
    dot = jnp.mean(xf * gf, axis=-1, keepdims=True)
    return (gf * r - xf * (r * r * r * dot)).astype(BF)


def gelu_fwd(z):
    zf = z.astype(F32)
    t = jnp.tanh(zf * (GELU_C + (GELU_C * GELU_A) * (zf * zf)))
    half = 0.5 * zf
    return (half + half * t).astype(BF)


def gelu_bwd(z, dg):
    zf = z.astype(F32)
    z2 = zf * zf
    t = jnp.tanh(zf * (GELU_C + (GELU_C * GELU_A) * z2))
    slope = (0.5 + 0.5 * t) + (1.0 - t * t) * (zf * ((0.5 * GELU_C) + (1.5 * GELU_C * GELU_A) * z2))
    return (dg.astype(F32) * slope).astype(BF)


def head_stack(a4, width):
    lane = lax.broadcasted_iota(jnp.int32, a4.shape, 1)
    zero = jnp.zeros_like(a4)
    n_sub = a4.shape[1] // width
    return jnp.concatenate([jnp.where((lane >= h * width) & (lane < (h + 1) * width), a4, zero) for h in range(n_sub)], axis=0)


def soft_stats(sb, scale):
    m = jnp.max(sb, axis=0, keepdims=True).astype(F32)
    e = jnp.exp2((sb.astype(F32) - m) * (scale * LOG2E))
    inv = 1.0 / jnp.sum(e, axis=0, keepdims=True)
    return m, e, inv


def attn_bwd_quad(q4, k4, v4, do4, HW, get_p):
    S = q4.shape[0]
    ns = QW // HW
    scale = HW ** -0.5
    qm = head_stack(q4, HW)
    dom = head_stack(do4, HW)
    kT = k4.T
    dv = None
    dk = None
    dqT = []
    for pr in range(ns // 2):
        cols = slice(pr * 2 * S, (pr + 1) * 2 * S)
        p = get_p(qm[cols], k4, cols)
        dp = mm_nt(v4, dom[cols]).astype(BF).astype(F32)
        dv_p = mm(p.astype(BF), dom[cols])
        delta = jnp.sum(dp * p, axis=0, keepdims=True)
        ds = ((p * (dp - delta)) * scale).astype(BF)
        dk_p = mm(ds, qm[cols])
        dv = dv_p if dv is None else dv + dv_p
        dk = dk_p if dk is None else dk + dk_p
        for hh in range(2):
            h = pr * 2 + hh
            dqT.append(mm(kT[h * HW:(h + 1) * HW], ds[:, hh * S:(hh + 1) * S]).astype(BF))
    return jnp.concatenate(dqT, axis=0).T, dk.astype(BF), dv.astype(BF)


def step_kernel(cfg, x_ref, g_ref, emb_ref, wq_h, wk_h, wv_h, wo_ref, wup_ref, wdn_ref,
                acc_h, qkv0_ref, u0_ref, mix0_ref, dmid0_ref,
                xs, us, qkv, st, stat, mixT, hs, mT, zs, gs, dmid, dout, dcur, wqkvT, acc, sem, wsem):
    S, D, FF, HW, L = cfg
    NQ = D // QW
    NS = QW // HW
    scale = HW ** -0.5
    step = pl.program_id(0)
    last = pl.num_programs(0) - 1
    n_ff = FF // UNIT

    @pl.when(step == 0)
    def _():
        loads = [pltpu.make_async_copy(w, wqkvT.at[j * D:(j + 1) * D], wsem.at[j]) for j, w in enumerate((wq_h, wk_h, wv_h))]
        for cp in loads:
            cp.start()
        acc[...] = jnp.zeros_like(acc)
        for cp in loads:
            cp.wait()

    emb = emb_ref[...].astype(F32)
    xs[0] = x_ref[0] + emb[0:1].astype(BF)

    def fwd(l, carry):
        rows = pl.ds(pl.multiple_of(l * S, S), S)
        x = xs[l]
        xf = x.astype(F32)
        u = (xf * rms_scale(xf)).astype(BF)
        us[rows, :] = u
        for j in range(3):
            cols = slice(j * D, (j + 1) * D)
            qkv[rows, cols] = mm_nt(u, wqkvT[cols, :]).astype(BF)
        for c in range(NQ):
            q4 = qkv[rows, c * QW:(c + 1) * QW]
            k4 = qkv[rows, D + c * QW:D + (c + 1) * QW]
            v4 = qkv[rows, 2 * D + c * QW:2 * D + (c + 1) * QW]
            qm = head_stack(q4, HW)
            vT = v4.T
            for pr in range(NS // 2):
                cols = slice(pr * 2 * S, (pr + 1) * 2 * S)
                sb = mm_nt(k4, qm[cols]).astype(BF)
                st[l, c, :, cols] = sb
                m, e, inv = soft_stats(sb, scale)
                stat[l, c, 0:1, cols] = m
                stat[l, c, 1:2, cols] = inv
                p = (e * inv).astype(BF)
                for hh in range(2):
                    h = pr * 2 + hh
                    o = mm(vT[h * HW:(h + 1) * HW], p[:, hh * S:(hh + 1) * S])
                    mixT[c * QW + h * HW:c * QW + (h + 1) * HW, rows] = o.astype(BF)
        h_mid = x + mm_tn(mixT[:, rows], wo_ref[...]).astype(BF)
        hs[l] = h_mid
        hf = h_mid.astype(F32)
        mn = (hf * rms_scale(hf)).astype(BF)
        mT[:, rows] = mn.T
        for j in range(n_ff):
            cols = slice(j * UNIT, (j + 1) * UNIT)
            z = mm(mn, wup_ref[:, cols]).astype(BF)
            zs[rows, cols] = z
            gs[rows, cols] = gelu_fwd(z)

        @pl.when(l < L - 1)
        def _():
            y = mm(gs[rows, :], wdn_ref[...]).astype(BF)
            nxt = emb[1:2]
            for j in range(2, L):
                nxt = jnp.where(l + 1 == j, emb[j:j + 1], nxt)
            xs[l + 1] = (h_mid + y) + nxt.astype(BF)
        return carry

    lax.fori_loop(0, L, fwd, 0)
    dcur[...] = g_ref[0]
    qkv0_ref[0] = qkv[0:S, :]
    u0_ref[0] = us[0:S, :]
    mix0_ref[...] = mixT[:, 0:S]

    def bwd(i, carry):
        l = L - 1 - i
        rows = pl.ds(pl.multiple_of(l * S, S), S)
        d_out = dcur[...]
        dout[rows, :] = d_out
        for j in range(n_ff):
            cols = slice(j * UNIT, (j + 1) * UNIT)
            d_act = mm_nt(d_out, wdn_ref[cols, :]).astype(BF)
            zs[rows, cols] = gelu_bwd(zs[rows, cols], d_act)
        d_norm = mm_nt(zs[rows, :], wup_ref[...]).astype(BF)
        dmid[rows, :] = d_out + rms_bwd(hs[l], d_norm)

        @pl.when(l > 0)
        def _():
            d_mid = dmid[rows, :]
            d_mix = mm_nt(d_mid, wo_ref[...]).astype(BF)
            for c in range(NQ):
                qc = slice(c * QW, (c + 1) * QW)
                kc = slice(D + c * QW, D + (c + 1) * QW)
                vc = slice(2 * D + c * QW, 2 * D + (c + 1) * QW)

                def get_p(qs, k4, cols):
                    s = st[l, c, :, cols].astype(F32)
                    return jnp.exp2((s - stat[l, c, 0:1, cols]) * (scale * LOG2E)) * stat[l, c, 1:2, cols]

                dq, dk, dv = attn_bwd_quad(qkv[rows, qc], qkv[rows, kc], qkv[rows, vc], d_mix[:, qc], HW, get_p)
                qkv[rows, qc] = dq
                qkv[rows, kc] = dk
                qkv[rows, vc] = dv
            d_norm_x = mm(qkv[rows, :], wqkvT[...]).astype(BF)
            dcur[...] = d_mid + rms_bwd(xs[l], d_norm_x)
        return carry

    lax.fori_loop(0, L, bwd, 0)
    dmid0_ref[0] = dmid[0:S, :]

    def flush(k):
        @pl.when(step == last)
        def _():
            pltpu.make_async_copy(acc.at[k], acc_h.at[k], sem.at[k]).start()

    def attn_unit(j, carry):
        cols = pl.ds(pl.multiple_of(j * UNIT, UNIT), UNIT)
        acc[8 + j] = acc[8 + j] + mm_tn(qkv[S:, cols], us[S:, :])
        flush(8 + j)
        return carry

    lax.fori_loop(0, 3, attn_unit, 0)
    acc[11] = acc[11] + mm(mixT[:, S:], dmid[S:, :])
    flush(11)

    def mlp_unit(j, carry):
        cols = pl.ds(pl.multiple_of(j * UNIT, UNIT), UNIT)
        acc[j] = acc[j] + mm_tn(gs[:, cols], dout[...])
        flush(j)
        acc[4 + j] = acc[4 + j] + mm(mT[...], zs[:, cols])
        flush(4 + j)
        return carry

    lax.fori_loop(0, n_ff, mlp_unit, 0)

    @pl.when(step == last)
    def _():
        for k in range(12):
            pltpu.make_async_copy(acc.at[k], acc_h.at[k], sem.at[k]).wait()


def reduce_kernel(cfg, x_ref, emb_ref, qkv_ref, u_ref, mix_ref, dmid_ref, wo_ref, wq_h, wk_h, wv_h, acc_h,
                  dx_ref, dn_h, up_h, q_h, k_h, v_h, o_h,
                  wqkvT, dqkv, acc2, aw, r1, r2, r3, res, send, recv, lsem, osem, wsem):
    S, D, HW = cfg
    NQ = D // QW
    scale = HW ** -0.5
    step = pl.program_id(0)
    me = lax.axis_index('data')
    core = lax.rem(me, 2)
    bit_x = lax.rem(me // 2, 2)
    bit_y = me // 4
    core_peer = me + 1 - 2 * core
    x_peer = me + 2 - 4 * bit_x
    y_peer = me + 4 - 8 * bit_y
    half = UNIT // 2
    N_EARLY = 8
    N_ALL = 12

    def order(k):
        if k % 2 == 0:
            return (bit_x, x_peer), (bit_y, y_peer)
        return (bit_y, y_peer), (bit_x, x_peer)

    def aligned(v, n):
        return pl.ds(pl.multiple_of(v, n), n)

    def remote(stage, k, src, dst, peer):
        return pltpu.make_async_remote_copy(src_ref=src, dst_ref=dst, send_sem=send.at[stage, k], recv_sem=recv.at[stage, k], device_id=(peer,), device_id_type=MESH)

    def copy_of(stage, k):
        (b1, p1), (b2, p2) = order(k)
        if stage == 0:
            rows = aligned((1 - core) * half, half)
            src = acc_h.at[k, rows] if k < N_EARLY else acc2.at[k - N_EARLY, rows]
            return remote(0, k, src, r1.at[k], core_peer)
        if stage == 1:
            return remote(1, k, aw.at[k, aligned((1 - b1) * 128, 128)], r2.at[k], p1)
        if stage == 2:
            return remote(2, k, aw.at[k, aligned(b1 * 128 + (1 - b2) * 64, 64)], r3.at[k], p2)
        if stage == 3:
            mine = res.at[k, aligned(core * half + b1 * 128 + b2 * 64, 64)]
            return remote(3, k, mine, mine, p2)
        if stage == 4:
            mine = res.at[k, aligned(core * half + b1 * 128, 128)]
            return remote(4, k, mine, mine, p1)
        mine = res.at[k, aligned(core * half, half)]
        return remote(5, k, mine, mine, core_peer)

    def out_copy(k):
        if k < 4:
            dst = dn_h.at[k * UNIT:(k + 1) * UNIT]
        elif k < 8:
            dst = up_h.at[:, (k - 4) * UNIT:(k - 3) * UNIT]
        else:
            dst = (q_h, k_h, v_h, o_h)[k - 8]
        return pltpu.make_async_copy(res.at[k], dst, osem.at[k])

    def own_load(k):
        return pltpu.make_async_copy(acc_h.at[k, aligned(core * half, half)], aw.at[k], lsem.at[k])

    def late_load(k):
        return pltpu.make_async_copy(acc_h.at[k], acc2.at[k - N_EARLY], lsem.at[k])

    def serve(stage, k):
        (b1, _), (b2, _) = order(k)
        if stage == 0:
            if k < N_EARLY:
                own_load(k).wait()
                copy_of(0, k).wait_recv()
                aw[k] = aw[k] + r1[k]
            else:
                copy_of(0, k).wait_recv()
                aw[k] = acc2[k - N_EARLY, aligned(core * half, half)] + r1[k]
        elif stage == 1:
            copy_of(1, k).wait_recv()
            rows = aligned(b1 * 128, 128)
            aw[k, rows] = aw[k, rows] + r2[k]
        elif stage == 2:
            copy_of(2, k).wait_recv()
            res[k, aligned(core * half + b1 * 128 + b2 * 64, 64)] = aw[k, aligned(b1 * 128 + b2 * 64, 64)] + r3[k]
        else:
            copy_of(stage, k).wait_recv()
        if stage < 5:
            copy_of(stage + 1, k).start()
        else:
            out_copy(k).start()

    def at_step(i, events):
        @pl.when(step == i)
        def _():
            for stage, k in events:
                serve(stage, k)

    @pl.when(step == 0)
    def _():
        barrier = pltpu.get_barrier_semaphore()
        for peer in (core_peer, x_peer, y_peer):
            pl.semaphore_signal(barrier, inc=1, device_id=(peer,), device_id_type=MESH)
        loads = [pltpu.make_async_copy(w, wqkvT.at[j * D:(j + 1) * D], wsem.at[j]) for j, w in enumerate((wq_h, wk_h, wv_h))]
        for k in range(N_EARLY):
            own_load(k).start()
        pl.semaphore_wait(barrier, 3)
        for k in range(N_EARLY):
            copy_of(0, k).start()
        for cp in loads:
            cp.start()
        for k in range(N_EARLY, N_ALL):
            late_load(k).start()
        for k in range(4):
            serve(0, k)
        for cp in loads:
            cp.wait()
        for k in range(N_EARLY, N_ALL):
            late_load(k).wait()

    d_mid = dmid_ref[0]
    d_mix = mm_nt(d_mid, wo_ref[...]).astype(BF)
    for c in range(NQ):
        qc = slice(c * QW, (c + 1) * QW)
        kc = slice(D + c * QW, D + (c + 1) * QW)
        vc = slice(2 * D + c * QW, 2 * D + (c + 1) * QW)

        def get_p(qs, k4, cols):
            m, e, inv = soft_stats(mm_nt(k4, qs).astype(BF), scale)
            return e * inv

        dq, dk, dv = attn_bwd_quad(qkv_ref[0, :, qc], qkv_ref[0, :, kc], qkv_ref[0, :, vc], d_mix[:, qc], HW, get_p)
        dqkv[:, qc] = dq
        dqkv[:, kc] = dk
        dqkv[:, vc] = dv
    d_norm_x = mm(dqkv[...], wqkvT[...]).astype(BF)
    x = x_ref[0] + emb_ref[0:1, :]
    dx_ref[0] = d_mid + rms_bwd(x, d_norm_x)

    def attn_unit(j, carry):
        cols = pl.ds(pl.multiple_of(j * UNIT, UNIT), UNIT)
        acc2[j] = acc2[j] + mm_tn(dqkv[:, cols], u_ref[0])
        return carry

    lax.fori_loop(0, 3, attn_unit, 0)
    acc2[3] = acc2[3] + mm(mix_ref[...], d_mid)

    at_step(0, [(0, k) for k in range(4, 8)])
    at_step(1, [(1, 0), (1, 1)])
    at_step(2, [(1, 2), (1, 3)])
    at_step(3, [(1, 4), (1, 5), (2, 0), (2, 1)])
    at_step(4, [(1, 6), (1, 7), (2, 2), (2, 3)])

    @pl.when(step == 5)
    def _():
        for k in range(N_EARLY, N_ALL):
            copy_of(0, k).start()
        plan = [(2, 4), (2, 5), (3, 0), (3, 1), (0, 8), (0, 9), (0, 10), (0, 11), (2, 6), (2, 7), (3, 2), (3, 3),
                (1, 8), (1, 9), (3, 4), (3, 5), (1, 10), (1, 11), (4, 0), (4, 1), (3, 6), (3, 7), (2, 8), (2, 9),
                (4, 2), (4, 3), (5, 0), (5, 1), (2, 10), (2, 11), (4, 4), (4, 5), (5, 2), (5, 3), (3, 8), (3, 9),
                (4, 6), (4, 7), (3, 10), (3, 11), (5, 4), (5, 5), (5, 6), (5, 7), (4, 8), (4, 9), (4, 10), (4, 11),
                (5, 8), (5, 9), (5, 10), (5, 11)]
        for stage, k in plan:
            serve(stage, k)
        for k in range(N_ALL):
            for stage in range(6):
                copy_of(stage, k).wait_send()
        for k in range(N_ALL):
            out_copy(k).wait()


def solution(mesh):
    batch_spec = P('data', None, None)

    def per_device(x, g, emb, w_q, w_k, w_v, w_o, wup, wdn):
        D, H, HW = w_q.shape
        B, S, _ = x.shape
        FF = wup.shape[1]
        L = emb.shape[0]
        T = L * S
        NQ = D // QW
        NS = QW // HW
        w_t = [w.transpose(1, 2, 0).reshape(D, D) for w in (w_q, w_k, w_v)]
        wo = w_o.reshape(D, D)
        const = lambda shape: pl.BlockSpec(shape, lambda b: (0,) * len(shape), pipeline_mode=pl.Buffered(1))
        per_seq = lambda cols: pl.BlockSpec((1, S, cols), lambda b: (b, 0, 0))
        col_seq = pl.BlockSpec((D, S), lambda b: (0, b))
        hbm = pl.BlockSpec(memory_space=pl.ANY)
        sds = jax.ShapeDtypeStruct
        acc, qkv0, u0, mix0, dmid0 = pl.pallas_call(
            functools.partial(step_kernel, (S, D, FF, HW, L)),
            name='block_grads',
            grid=(B,),
            in_specs=[per_seq(D), per_seq(D), const(emb.shape), hbm, hbm, hbm, const(wo.shape), const(wup.shape), const(wdn.shape)],
            out_specs=[hbm, per_seq(3 * D), per_seq(D), col_seq, per_seq(D)],
            out_shape=[sds((12, UNIT, UNIT), F32), sds((B, S, 3 * D), BF), sds((B, S, D), BF), sds((D, B * S), BF), sds((B, S, D), BF)],
            scratch_shapes=[
                pltpu.VMEM((L, S, D), BF),
                pltpu.VMEM((T, D), BF),
                pltpu.VMEM((T, 3 * D), BF),
                pltpu.VMEM((L, NQ, S, NS * S), BF),
                pltpu.VMEM((L, NQ, 8, NS * S), F32),
                pltpu.VMEM((D, T), BF),
                pltpu.VMEM((L, S, D), BF),
                pltpu.VMEM((D, T), BF),
                pltpu.VMEM((T, FF), BF),
                pltpu.VMEM((T, FF), BF),
                pltpu.VMEM((T, D), BF),
                pltpu.VMEM((T, D), BF),
                pltpu.VMEM((S, D), BF),
                pltpu.VMEM((3 * D, D), BF),
                pltpu.VMEM((12, UNIT, UNIT), F32),
                pltpu.SemaphoreType.DMA((12,)),
                pltpu.SemaphoreType.DMA((3,)),
            ],
            compiler_params=pltpu.CompilerParams(dimension_semantics=('arbitrary',), vmem_limit_bytes=VMEM_MAX),
        )(x, g, emb, *w_t, wo, wup, wdn)
        outs = pl.pallas_call(
            functools.partial(reduce_kernel, (S, D, HW)),
            name='attn_reduce',
            grid=(B,),
            in_specs=[per_seq(D), const(emb.shape), per_seq(3 * D), per_seq(D), col_seq, per_seq(D), const(wo.shape), hbm, hbm, hbm, hbm],
            out_specs=[per_seq(D)] + [hbm] * 6,
            out_shape=[sds(x.shape, BF), sds((FF, D), F32), sds((D, FF), F32)] + [sds((D, D), F32)] * 4,
            scratch_shapes=[
                pltpu.VMEM((3 * D, D), BF),
                pltpu.VMEM((S, 3 * D), BF),
                pltpu.VMEM((4, UNIT, UNIT), F32),
                pltpu.VMEM((12, UNIT // 2, UNIT), F32),
                pltpu.VMEM((12, UNIT // 2, UNIT), F32),
                pltpu.VMEM((12, 128, UNIT), F32),
                pltpu.VMEM((12, 64, UNIT), F32),
                pltpu.VMEM((12, UNIT, UNIT), F32),
                pltpu.SemaphoreType.DMA((6, 12)),
                pltpu.SemaphoreType.DMA((6, 12)),
                pltpu.SemaphoreType.DMA((12,)),
                pltpu.SemaphoreType.DMA((12,)),
                pltpu.SemaphoreType.DMA((3,)),
            ],
            compiler_params=pltpu.CompilerParams(dimension_semantics=('arbitrary',), vmem_limit_bytes=VMEM_MAX, collective_id=0, has_side_effects=True),
        )(x, emb, qkv0, u0, mix0, dmid0, wo, *w_t, acc)
        d_x, dn, up, gq, gk, gv, go = outs
        back = lambda a: a.reshape(H, HW, D).transpose(2, 0, 1)
        return back(gq), back(gk), back(gv), go.reshape(H, HW, D), up, dn, d_x

    return jax.shard_map(per_device, mesh=mesh, in_specs=(batch_spec, batch_spec, P(), P(), P(), P(), P(), P(), P()), out_specs=(P(), P(), P(), P(), P(), P(), batch_spec), check_vma=False)
```

```python
import functools

import jax
import jax.numpy as jnp
from jax import lax
from jax.experimental import pallas as pl
from jax.experimental.pallas import tpu as pltpu
from jax.sharding import PartitionSpec as P

NORM_EPS = 1e-6
BF = jnp.bfloat16
F32 = jnp.float32
GELU_C = 0.7978845608028654
GELU_A = 0.044715
LOG2E = 1.4426950408889634
MESH = pl.DeviceIdType.MESH
UNIT = 512
QW = 256
VMEM_MAX = 67043328


def mm(a, b):
    return lax.dot_general(a, b, (((1,), (0,)), ((), ())), preferred_element_type=F32)


def mm_nt(a, b):
    return lax.dot_general(a, b, (((1,), (1,)), ((), ())), preferred_element_type=F32)


def mm_tn(a, b):
    return lax.dot_general(a, b, (((0,), (0,)), ((), ())), preferred_element_type=F32)


def rms_scale(xf):
    return lax.rsqrt(jnp.mean(xf * xf, axis=-1, keepdims=True) + NORM_EPS)


def rms_bwd(x, dy):
    xf = x.astype(F32)
    gf = dy.astype(F32)
    r = rms_scale(xf)
    dot = jnp.mean(xf * gf, axis=-1, keepdims=True)
    return (gf * r - xf * (r * r * r * dot)).astype(BF)


def gelu_fwd(z):
    zf = z.astype(F32)
    t = jnp.tanh(zf * (GELU_C + (GELU_C * GELU_A) * (zf * zf)))
    half = 0.5 * zf
    return (half + half * t).astype(BF)


def gelu_bwd(z, dg):
    zf = z.astype(F32)
    z2 = zf * zf
    t = jnp.tanh(zf * (GELU_C + (GELU_C * GELU_A) * z2))
    slope = (0.5 + 0.5 * t) + ((1.0 - t * t) * zf) * ((0.5 * GELU_C) + (1.5 * GELU_C * GELU_A) * z2)
    return (dg.astype(F32) * slope).astype(BF)


def head_stack(a4, width):
    lane = lax.broadcasted_iota(jnp.int32, a4.shape, 1)
    zero = jnp.zeros_like(a4)
    n_sub = a4.shape[1] // width
    return jnp.concatenate([jnp.where((lane >= h * width) & (lane < (h + 1) * width), a4, zero) for h in range(n_sub)], axis=0)


def soft_stats(sb, scale):
    m = jnp.max(sb, axis=0, keepdims=True).astype(F32)
    e = jnp.exp2((sb.astype(F32) - m) * (scale * LOG2E))
    inv = 1.0 / jnp.sum(e, axis=0, keepdims=True)
    return m, e, inv


def attn_bwd_quad(q4, k4, v4, do4, HW, get_p):
    S = q4.shape[0]
    ns = QW // HW
    scale = HW ** -0.5
    qm = head_stack(q4, HW)
    dom = head_stack(do4, HW)
    kT = k4.T
    dv = None
    dk = None
    dqT = []
    for pr in range(ns // 2):
        cols = slice(pr * 2 * S, (pr + 1) * 2 * S)
        p = get_p(qm[cols], k4, cols)
        dp = mm_nt(v4, dom[cols]).astype(BF).astype(F32)
        dv_p = mm(p.astype(BF), dom[cols])
        delta = jnp.sum(dp * p, axis=0, keepdims=True)
        ds = ((p * (dp - delta)) * scale).astype(BF)
        dk_p = mm(ds, qm[cols])
        dv = dv_p if dv is None else dv + dv_p
        dk = dk_p if dk is None else dk + dk_p
        for hh in range(2):
            h = pr * 2 + hh
            dqT.append(mm(kT[h * HW:(h + 1) * HW], ds[:, hh * S:(hh + 1) * S]).astype(BF))
    return jnp.concatenate(dqT, axis=0).T, dk.astype(BF), dv.astype(BF)


def step_kernel(cfg, x_ref, g_ref, emb_ref, wq_h, wk_h, wv_h, wo_ref, wup_ref, wdn_ref,
                acc_h, qkv0_h, u0_h, mix0_h, z0_h, mT0_h, h0_h, dout0_h,
                xs, us, qkv, st, stat, mixT, hs, mT, zs, gs, dmid, dout, dcur, wqkvT, acc, sem, wsem, ssem):
    S, D, FF, HW, L = cfg
    NQ = D // QW
    NS = QW // HW
    scale = HW ** -0.5
    step = pl.program_id(0)
    last = pl.num_programs(0) - 1
    n_ff = FF // UNIT

    @pl.when(step == 0)
    def _():
        loads = [pltpu.make_async_copy(w, wqkvT.at[j * D:(j + 1) * D], wsem.at[j]) for j, w in enumerate((wq_h, wk_h, wv_h))]
        for cp in loads:
            cp.start()
        acc[...] = jnp.zeros_like(acc)
        for cp in loads:
            cp.wait()

    emb = emb_ref[...].astype(F32)
    xs[0] = x_ref[0] + emb[0:1].astype(BF)

    def fwd(l, carry):
        rows = pl.ds(pl.multiple_of(l * S, S), S)
        x = xs[l]
        xf = x.astype(F32)
        u = (xf * rms_scale(xf)).astype(BF)
        us[rows, :] = u
        for j in range(3):
            cols = slice(j * D, (j + 1) * D)
            qkv[rows, cols] = mm_nt(u, wqkvT[cols, :]).astype(BF)
        for c in range(NQ):
            q4 = qkv[rows, c * QW:(c + 1) * QW]
            k4 = qkv[rows, D + c * QW:D + (c + 1) * QW]
            v4 = qkv[rows, 2 * D + c * QW:2 * D + (c + 1) * QW]
            qm = head_stack(q4, HW)
            vT = v4.T
            for pr in range(NS // 2):
                cols = slice(pr * 2 * S, (pr + 1) * 2 * S)
                sb = mm_nt(k4, qm[cols]).astype(BF)
                st[l, c, :, cols] = sb
                m, e, inv = soft_stats(sb, scale)
                stat[l, c, 0:1, cols] = m
                stat[l, c, 1:2, cols] = inv
                p = (e * inv).astype(BF)
                for hh in range(2):
                    h = pr * 2 + hh
                    o = mm(vT[h * HW:(h + 1) * HW], p[:, hh * S:(hh + 1) * S])
                    mixT[c * QW + h * HW:c * QW + (h + 1) * HW, rows] = o.astype(BF)
        h_mid = x + mm_tn(mixT[:, rows], wo_ref[...]).astype(BF)
        hs[l] = h_mid
        hf = h_mid.astype(F32)
        mn = (hf * rms_scale(hf)).astype(BF)
        mT[:, rows] = mn.T
        for j in range(n_ff):
            cols = slice(j * UNIT, (j + 1) * UNIT)
            z = mm(mn, wup_ref[:, cols]).astype(BF)
            zs[rows, cols] = z
            gs[rows, cols] = gelu_fwd(z)

        @pl.when(l < L - 1)
        def _():
            y = mm(gs[rows, :], wdn_ref[...]).astype(BF)
            nxt = emb[1:2]
            for j in range(2, L):
                nxt = jnp.where(l + 1 == j, emb[j:j + 1], nxt)
            xs[l + 1] = (h_mid + y) + nxt.astype(BF)
        return carry

    lax.fori_loop(0, L, fwd, 0)
    dcur[...] = g_ref[0]
    saves = [pltpu.make_async_copy(src, dst.at[step], ssem.at[n]) for n, (src, dst) in enumerate((
        (qkv.at[0:S], qkv0_h), (us.at[0:S], u0_h), (mixT.at[:, 0:S], mix0_h), (zs.at[0:S], z0_h),
        (mT.at[:, 0:S], mT0_h), (hs.at[0], h0_h), (dout.at[0:S], dout0_h)))]
    for cp in saves[:-1]:
        cp.start()

    def bwd(i, carry):
        l = L - 1 - i
        rows = pl.ds(pl.multiple_of(l * S, S), S)
        d_out = dcur[...]
        dout[rows, :] = d_out
        for j in range(n_ff):
            cols = slice(j * UNIT, (j + 1) * UNIT)
            d_act = mm_nt(d_out, wdn_ref[cols, :]).astype(BF)
            zs[rows, cols] = gelu_bwd(zs[rows, cols], d_act)
        d_norm = mm_nt(zs[rows, :], wup_ref[...]).astype(BF)
        dmid[rows, :] = d_out + rms_bwd(hs[l], d_norm)

        d_mid = dmid[rows, :]
        d_mix = mm_nt(d_mid, wo_ref[...]).astype(BF)
        for c in range(NQ):
            qc = slice(c * QW, (c + 1) * QW)
            kc = slice(D + c * QW, D + (c + 1) * QW)
            vc = slice(2 * D + c * QW, 2 * D + (c + 1) * QW)

            def get_p(qs, k4, cols):
                s = st[l, c, :, cols].astype(F32)
                return jnp.exp2((s - stat[l, c, 0:1, cols]) * (scale * LOG2E)) * stat[l, c, 1:2, cols]

            dq, dk, dv = attn_bwd_quad(qkv[rows, qc], qkv[rows, kc], qkv[rows, vc], d_mix[:, qc], HW, get_p)
            qkv[rows, qc] = dq
            qkv[rows, kc] = dk
            qkv[rows, vc] = dv
        d_norm_x = mm(qkv[rows, :], wqkvT[...]).astype(BF)
        dcur[...] = d_mid + rms_bwd(xs[l], d_norm_x)
        return carry

    lax.fori_loop(0, L - 1, bwd, 0)
    dout[0:S, :] = dcur[...]
    saves[-1].start()

    def flush(k):
        @pl.when(step == last)
        def _():
            pltpu.make_async_copy(acc.at[k], acc_h.at[k], sem.at[k]).start()

    def attn_unit(j, carry):
        cols = pl.ds(pl.multiple_of(j * UNIT, UNIT), UNIT)
        acc[8 + j] = acc[8 + j] + mm_tn(qkv[S:, cols], us[S:, :])
        flush(8 + j)
        return carry

    lax.fori_loop(0, 3, attn_unit, 0)
    acc[11] = acc[11] + mm(mixT[:, S:], dmid[S:, :])
    flush(11)

    def mlp_unit(j, carry):
        cols = pl.ds(pl.multiple_of(j * UNIT, UNIT), UNIT)
        acc[j] = acc[j] + mm_tn(gs[:, cols], dout[...])
        flush(j)
        acc[4 + j] = acc[4 + j] + mm(mT[:, S:], zs[S:, cols])
        flush(4 + j)
        return carry

    lax.fori_loop(0, n_ff, mlp_unit, 0)
    for cp in saves:
        cp.wait()

    @pl.when(step == last)
    def _():
        for k in range(12):
            pltpu.make_async_copy(acc.at[k], acc_h.at[k], sem.at[k]).wait()


def reduce_kernel(cfg, x_ref, emb_ref, qkv_ref, u_ref, mix_ref, z_ref, mT_ref, h_ref, dout_ref, wo_ref, wq_h, wk_h, wv_h, wup_h, wdn_h, acc_h,
                  dx_ref, dn_h, up_h, q_h, k_h, v_h, o_h,
                  wqkvT, wup, wdn, dup, dmid, dqkv, acc2, aw, r1, r2, r3, res, send, recv, lsem, osem, wsem):
    B, S, D, FF, HW = cfg
    NQ = D // QW
    n_ff = FF // UNIT
    scale = HW ** -0.5
    step = pl.program_id(0)
    me = lax.axis_index('data')
    core = lax.rem(me, 2)
    bit_x = lax.rem(me // 2, 2)
    bit_y = me // 4
    core_peer = me + 1 - 2 * core
    x_peer = me + 2 - 4 * bit_x
    y_peer = me + 4 - 8 * bit_y
    half = UNIT // 2
    N_EARLY = n_ff
    N_ALL = 12

    def order(k):
        if k % 2 == 0:
            return (bit_x, x_peer), (bit_y, y_peer)
        return (bit_y, y_peer), (bit_x, x_peer)

    def aligned(v, n):
        return pl.ds(pl.multiple_of(v, n), n)

    def part(k, start, n):
        if k < N_EARLY:
            return aw.at[k, aligned(start, n)]
        return acc2.at[k - N_EARLY, aligned(core * half + start, n)]

    def remote(stage, k, src, dst, peer):
        return pltpu.make_async_remote_copy(src_ref=src, dst_ref=dst, send_sem=send.at[stage, k], recv_sem=recv.at[stage, k], device_id=(peer,), device_id_type=MESH)

    def copy_of(stage, k):
        (b1, p1), (b2, p2) = order(k)
        if stage == 0:
            rows = aligned((1 - core) * half, half)
            src = acc_h.at[k, rows] if k < N_EARLY else acc2.at[k - N_EARLY, rows]
            return remote(0, k, src, r1.at[k], core_peer)
        if stage == 1:
            return remote(1, k, part(k, (1 - b1) * 128, 128), r2.at[k], p1)
        if stage == 2:
            return remote(2, k, part(k, b1 * 128 + (1 - b2) * 64, 64), r3.at[k], p2)
        if stage == 3:
            mine = res.at[k, aligned(core * half + b1 * 128 + b2 * 64, 64)]
            return remote(3, k, mine, mine, p2)
        if stage == 4:
            mine = res.at[k, aligned(core * half + b1 * 128, 128)]
            return remote(4, k, mine, mine, p1)
        mine = res.at[k, aligned(core * half, half)]
        return remote(5, k, mine, mine, core_peer)

    def out_copy(k):
        if k < 4:
            dst = dn_h.at[k * UNIT:(k + 1) * UNIT]
        elif k < 8:
            dst = up_h.at[:, (k - 4) * UNIT:(k - 3) * UNIT]
        else:
            dst = (q_h, k_h, v_h, o_h)[k - 8]
        return pltpu.make_async_copy(res.at[k], dst, osem.at[k])

    def own_load(k):
        return pltpu.make_async_copy(acc_h.at[k, aligned(core * half, half)], aw.at[k], lsem.at[k])

    def late_load(k):
        return pltpu.make_async_copy(acc_h.at[k], acc2.at[k - N_EARLY], lsem.at[k])

    def serve(stage, k):
        (b1, _), (b2, _) = order(k)
        copy_of(stage, k).wait_recv()
        if stage == 0:
            if k < N_EARLY:
                own_load(k).wait()
            ref = part(k, 0, half)
            ref[...] = ref[...] + r1[k]
        elif stage == 1:
            ref = part(k, b1 * 128, 128)
            ref[...] = ref[...] + r2[k]
        elif stage == 2:
            ref = part(k, b1 * 128 + b2 * 64, 64)
            res[k, aligned(core * half + b1 * 128 + b2 * 64, 64)] = ref[...] + r3[k]
        if stage < 5:
            copy_of(stage + 1, k).start()
        else:
            out_copy(k).start()

    def serve_all(stage, units):
        for k in units:
            serve(stage, k)

    def begin(units):
        for k in units:
            copy_of(0, k).start()

    def w_loads():
        pairs = [(wdn_h, wdn), (wup_h, wup)] + [(w, wqkvT.at[j * D:(j + 1) * D]) for j, w in enumerate((wq_h, wk_h, wv_h))]
        return [pltpu.make_async_copy(s_, d_, wsem.at[j]) for j, (s_, d_) in enumerate(pairs)]

    @pl.when(step == 0)
    def _():
        barrier = pltpu.get_barrier_semaphore()
        for peer in (core_peer, x_peer, y_peer):
            pl.semaphore_signal(barrier, inc=1, device_id=(peer,), device_id_type=MESH)
        for k in range(N_EARLY):
            own_load(k).start()
        for cp in w_loads():
            cp.start()
        pl.semaphore_wait(barrier, 3)
        begin(range(N_EARLY))
        for k in range(N_EARLY, N_ALL):
            late_load(k).start()
        serve_all(0, range(N_EARLY))
        for cp in w_loads():
            cp.wait()
        for k in range(N_EARLY, N_ALL):
            late_load(k).wait()

    @pl.when(step < B)
    def _():
        d_out = dout_ref[0]
        for j in range(n_ff):
            cols = slice(j * UNIT, (j + 1) * UNIT)
            d_act = mm_nt(d_out, wdn[cols, :]).astype(BF)
            dup[:, cols] = gelu_bwd(z_ref[0, :, cols], d_act)
        d_norm = mm_nt(dup[...], wup[...]).astype(BF)
        d_mid = d_out + rms_bwd(h_ref[0], d_norm)
        dmid[step] = d_mid
        for j in range(n_ff):
            acc2[j] = acc2[j] + mm(mT_ref[0], dup[:, j * UNIT:(j + 1) * UNIT])
        acc2[7] = acc2[7] + mm(mix_ref[0], d_mid)

    @pl.when(step >= B)
    def _():
        d_mid = dmid[step - B]
        d_mix = mm_nt(d_mid, wo_ref[...]).astype(BF)
        for c in range(NQ):
            qc = slice(c * QW, (c + 1) * QW)
            kc = slice(D + c * QW, D + (c + 1) * QW)
            vc = slice(2 * D + c * QW, 2 * D + (c + 1) * QW)

            def get_p(qs, k4, cols):
                m, e, inv = soft_stats(mm_nt(k4, qs).astype(BF), scale)
                return e * inv

            dq, dk, dv = attn_bwd_quad(qkv_ref[0, :, qc], qkv_ref[0, :, kc], qkv_ref[0, :, vc], d_mix[:, qc], HW, get_p)
            dqkv[:, qc] = dq
            dqkv[:, kc] = dk
            dqkv[:, vc] = dv
        d_norm_x = mm(dqkv[...], wqkvT[...]).astype(BF)
        x = x_ref[0] + emb_ref[0:1, :]
        dx_ref[0] = d_mid + rms_bwd(x, d_norm_x)

        def attn_unit(j, carry):
            cols = pl.ds(pl.multiple_of(j * UNIT, UNIT), UNIT)
            acc2[4 + j] = acc2[4 + j] + mm_tn(dqkv[:, cols], u_ref[0])
            return carry

        lax.fori_loop(0, 3, attn_unit, 0)

    def at_step(i, events, before=None):
        @pl.when(step == i)
        def _():
            if before is not None:
                begin(before)
            for stage, k in events:
                serve(stage, k)

    at_step(1, [(1, 0), (1, 1)])
    at_step(3, [(1, 2), (1, 3)])
    at_step(4, [(2, 0), (2, 1)])
    at_step(5, [(2, 2), (2, 3), (0, 4), (0, 5), (0, 6), (0, 7), (0, 11), (3, 0), (3, 1)], before=[4, 5, 6, 7, 11])
    at_step(6, [(3, 2), (3, 3), (1, 4), (1, 5)])
    at_step(7, [(4, 0), (4, 1), (1, 6), (1, 7)])
    at_step(8, [(4, 2), (4, 3), (1, 11), (2, 4), (2, 5)])
    at_step(9, [(5, 0), (5, 1), (5, 2), (5, 3), (2, 6), (2, 7), (3, 4), (3, 5)])
    at_step(10, [(2, 11), (3, 6), (3, 7), (4, 4), (4, 5)])

    @pl.when(step == 2 * B - 1)
    def _():
        begin([8, 9, 10])
        plan = [(4, 6), (4, 7), (0, 8), (0, 9), (0, 10), (3, 11), (5, 4), (5, 5), (1, 8), (1, 9), (4, 11), (5, 6), (5, 7),
                (1, 10), (2, 8), (2, 9), (5, 11), (2, 10), (3, 8), (3, 9), (3, 10), (4, 8), (4, 9), (4, 10), (5, 8), (5, 9), (5, 10)]
        for stage, k in plan:
            serve(stage, k)
        for k in range(N_ALL):
            for stage in range(6):
                copy_of(stage, k).wait_send()
        for k in range(N_ALL):
            out_copy(k).wait()


def solution(mesh):
    batch_spec = P('data', None, None)

    def per_device(x, g, emb, w_q, w_k, w_v, w_o, wup, wdn):
        D, H, HW = w_q.shape
        B, S, _ = x.shape
        FF = wup.shape[1]
        L = emb.shape[0]
        T = L * S
        NQ = D // QW
        NS = QW // HW
        w_t = [w.transpose(1, 2, 0).reshape(D, D) for w in (w_q, w_k, w_v)]
        wo = w_o.reshape(D, D)
        const = lambda shape: pl.BlockSpec(shape, lambda b: (0,) * len(shape), pipeline_mode=pl.Buffered(1))
        per_seq = lambda cols: pl.BlockSpec((1, S, cols), lambda b: (b, 0, 0))
        col_seq = pl.BlockSpec((D, S), lambda b: (0, b))
        hbm = pl.BlockSpec(memory_space=pl.ANY)
        sds = jax.ShapeDtypeStruct
        saved = [sds((B, S, 3 * D), BF), sds((B, S, D), BF), sds((B, D, S), BF), sds((B, S, FF), BF), sds((B, D, S), BF), sds((B, S, D), BF), sds((B, S, D), BF)]
        acc, qkv0, u0, mix0, z0, mT0, h0, dout0 = pl.pallas_call(
            functools.partial(step_kernel, (S, D, FF, HW, L)),
            name='block_grads',
            grid=(B,),
            in_specs=[per_seq(D), per_seq(D), const(emb.shape), hbm, hbm, hbm, const(wo.shape), const(wup.shape), const(wdn.shape)],
            out_specs=[hbm] * 8,
            out_shape=[sds((12, UNIT, UNIT), F32)] + saved,
            scratch_shapes=[
                pltpu.VMEM((L, S, D), BF),
                pltpu.VMEM((T, D), BF),
                pltpu.VMEM((T, 3 * D), BF),
                pltpu.VMEM((L, NQ, S, NS * S), BF),
                pltpu.VMEM((L, NQ, 8, NS * S), F32),
                pltpu.VMEM((D, T), BF),
                pltpu.VMEM((L, S, D), BF),
                pltpu.VMEM((D, T), BF),
                pltpu.VMEM((T, FF), BF),
                pltpu.VMEM((T, FF), BF),
                pltpu.VMEM((T, D), BF),
                pltpu.VMEM((T, D), BF),
                pltpu.VMEM((S, D), BF),
                pltpu.VMEM((3 * D, D), BF),
                pltpu.VMEM((12, UNIT, UNIT), F32),
                pltpu.SemaphoreType.DMA((12,)),
                pltpu.SemaphoreType.DMA((3,)),
                pltpu.SemaphoreType.DMA((7,)),
            ],
            compiler_params=pltpu.CompilerParams(dimension_semantics=('arbitrary',), vmem_limit_bytes=VMEM_MAX),
        )(x, g, emb, *w_t, wo, wup, wdn)
        first = lambda *shape: pl.BlockSpec((1,) + shape, lambda i: (jnp.minimum(i, B - 1), 0, 0))
        second = lambda *shape: pl.BlockSpec((1,) + shape, lambda i: (jnp.maximum(i - B, 0), 0, 0))
        outs = pl.pallas_call(
            functools.partial(reduce_kernel, (B, S, D, FF, HW)),
            name='attn_reduce',
            grid=(2 * B,),
            in_specs=[second(S, D), const(emb.shape), second(S, 3 * D), second(S, D), first(D, S), first(S, FF), first(D, S), first(S, D), first(S, D), const(wo.shape)] + [hbm] * 6,
            out_specs=[second(S, D)] + [hbm] * 6,
            out_shape=[sds(x.shape, BF), sds((FF, D), F32), sds((D, FF), F32)] + [sds((D, D), F32)] * 4,
            scratch_shapes=[
                pltpu.VMEM((3 * D, D), BF),
                pltpu.VMEM((D, FF), BF),
                pltpu.VMEM((FF, D), BF),
                pltpu.VMEM((S, FF), BF),
                pltpu.VMEM((B, S, D), BF),
                pltpu.VMEM((S, 3 * D), BF),
                pltpu.VMEM((8, UNIT, UNIT), F32),
                pltpu.VMEM((4, UNIT // 2, UNIT), F32),
                pltpu.VMEM((12, UNIT // 2, UNIT), F32),
                pltpu.VMEM((12, 128, UNIT), F32),
                pltpu.VMEM((12, 64, UNIT), F32),
                pltpu.VMEM((12, UNIT, UNIT), F32),
                pltpu.SemaphoreType.DMA((6, 12)),
                pltpu.SemaphoreType.DMA((6, 12)),
                pltpu.SemaphoreType.DMA((12,)),
                pltpu.SemaphoreType.DMA((12,)),
                pltpu.SemaphoreType.DMA((5,)),
            ],
            compiler_params=pltpu.CompilerParams(dimension_semantics=('arbitrary',), vmem_limit_bytes=VMEM_MAX, collective_id=0, has_side_effects=True),
        )(x, emb, qkv0, u0, mix0, z0, mT0, h0, dout0, wo, *w_t, wup, wdn, acc)
        d_x, dn, up, gq, gk, gv, go = outs
        back = lambda a: a.reshape(H, HW, D).transpose(2, 0, 1)
        return back(gq), back(gk), back(gv), go.reshape(H, HW, D), up, dn, d_x

    return jax.shard_map(per_device, mesh=mesh, in_specs=(batch_spec, batch_spec, P(), P(), P(), P(), P(), P(), P()), out_specs=(P(), P(), P(), P(), P(), P(), batch_spec), check_vma=False)
```

```python
import functools

import jax
import jax.numpy as jnp
from jax import lax
from jax.experimental import pallas as pl
from jax.experimental.pallas import tpu as pltpu
from jax.sharding import PartitionSpec as P

NORM_EPS = 1e-6
BF = jnp.bfloat16
F32 = jnp.float32
GELU_C = 0.7978845608028654
GELU_A = 0.044715
LOG2E = 1.4426950408889634
MESH = pl.DeviceIdType.MESH
UNIT = 512
QW = 256
VMEM_MAX = 67043328


def mm(a, b):
    return lax.dot_general(a, b, (((1,), (0,)), ((), ())), preferred_element_type=F32)


def mm_nt(a, b):
    return lax.dot_general(a, b, (((1,), (1,)), ((), ())), preferred_element_type=F32)


def mm_tn(a, b):
    return lax.dot_general(a, b, (((0,), (0,)), ((), ())), preferred_element_type=F32)


def rms_scale(xf):
    return lax.rsqrt(jnp.mean(xf * xf, axis=-1, keepdims=True) + NORM_EPS)


def rms_bwd(x, dy):
    xf = x.astype(F32)
    gf = dy.astype(F32)
    r = rms_scale(xf)
    dot = jnp.mean(xf * gf, axis=-1, keepdims=True)
    return (gf * r - xf * (r * r * r * dot)).astype(BF)


def gelu_fwd(z):
    zf = z.astype(F32)
    t = jnp.tanh(zf * (GELU_C + (GELU_C * GELU_A) * (zf * zf)))
    half = 0.5 * zf
    return (half + half * t).astype(BF)


def gelu_bwd(z, dg):
    zf = z.astype(F32)
    z2 = zf * zf
    t = jnp.tanh(zf * (GELU_C + (GELU_C * GELU_A) * z2))
    slope = (0.5 + 0.5 * t) + ((1.0 - t * t) * zf) * ((0.5 * GELU_C) + (1.5 * GELU_C * GELU_A) * z2)
    return (dg.astype(F32) * slope).astype(BF)


def head_stack(a4, width):
    lane = lax.broadcasted_iota(jnp.int32, a4.shape, 1)
    zero = jnp.zeros_like(a4)
    n_sub = a4.shape[1] // width
    return jnp.concatenate([jnp.where((lane >= h * width) & (lane < (h + 1) * width), a4, zero) for h in range(n_sub)], axis=0)


def soft_stats(sb, scale):
    m = jnp.max(sb, axis=0, keepdims=True).astype(F32)
    e = jnp.exp2((sb.astype(F32) - m) * (scale * LOG2E))
    inv = 1.0 / jnp.sum(e, axis=0, keepdims=True)
    return m, e, inv


def weave(chunks, fill):
    ahead = chunks[0][0]()
    for i, (_, use) in enumerate(chunks):
        now = ahead
        if i + 1 < len(chunks):
            ahead = chunks[i + 1][0]()
        use(now)
        for f in fill.get(i, ()):
            f()


def attn_bwd(qkv, rows, d_mix, HW, prob, pb, db, fills):
    S, D = d_mix.shape
    ns = QW // HW
    scale = HW ** -0.5
    width = ns * S
    tails = []
    for c in range(D // QW):
        qc = slice(c * QW, (c + 1) * QW)
        kc = slice(D + c * QW, D + (c + 1) * QW)
        vc = slice(2 * D + c * QW, 2 * D + (c + 1) * QW)
        k4 = qkv[rows, kc]
        v4 = qkv[rows, vc]
        qm = head_stack(qkv[rows, qc], HW)
        dom = head_stack(d_mix[:, qc], HW)
        kT = k4.T

        def chunk(i, c=c, k4=k4, v4=v4, qm=qm, dom=dom):
            cols = slice(i * QW, (i + 1) * QW)

            def use(vals):
                p = prob(c, cols, vals[1])
                dp = vals[0].astype(BF).astype(F32)
                delta = jnp.sum(dp * p, axis=0, keepdims=True)
                pb[c, :, cols] = p.astype(BF)
                db[c, :, cols] = ((p * (dp - delta)) * scale).astype(BF)
            return (lambda: (mm_nt(v4, dom[cols]), mm_nt(k4, qm[cols]) if prob.recompute else None)), use

        fill = {i: list(f) for i, f in fills[c].items()}
        for i, f in enumerate(tails):
            fill.setdefault(i, []).insert(0, f)

        def tail_v(c=c, vc=vc, dom=dom):
            qkv[rows, vc] = mm(pb[c], dom).astype(BF)

        def tail_k(c=c, kc=kc, qm=qm):
            qkv[rows, kc] = mm(db[c], qm).astype(BF)

        def tail_q(c=c, qc=qc, kT=kT):
            dqT = [mm(kT[h * HW:(h + 1) * HW], db[c, :, h * S:(h + 1) * S]).astype(BF) for h in range(ns)]
            qkv[rows, qc] = jnp.concatenate(dqT, axis=0).T

        weave([chunk(i) for i in range(width // QW)], fill)
        tails = [tail_v, tail_k, tail_q]
    for f in tails:
        f()


def mlp_bwd(d_out, zs, rows, wup, wdn, fill):
    FF = wdn.shape[0]
    total = []

    def chunk(i):
        cols = slice(i * QW, (i + 1) * QW)

        def use(v):
            zs[1][rows, cols] = gelu_bwd(zs[0](cols), v.astype(BF))
        return (lambda: mm_nt(d_out, wdn[cols, :])), use

    def part(j):
        cols = slice(j * UNIT, (j + 1) * UNIT)

        def run():
            v = mm_nt(zs[1][rows, cols], wup[:, cols])
            total[:] = [v if not total else total[0] + v]
        return run

    fill = {i: list(f) for i, f in fill.items()}
    for j in range(FF // UNIT):
        fill.setdefault(2 * j + 1, []).append(part(j))
    weave([chunk(i) for i in range(FF // QW)], fill)
    return total[0].astype(BF)


def step_kernel(cfg, x_ref, g_ref, emb_ref, wq_h, wk_h, wv_h, wo_ref, wup_ref, wdn_ref,
                acc_h, qkv0_h, u0_h, mix0_h, z0_h, mT0_h, h0_h, dout0_h,
                xs, us, qkv, st, stat, mixT, hs, mT, zs, gs, dmid, dout, dcur, wqkvT, pb, db, acc, sem, wsem, ssem):
    S, D, FF, HW, L = cfg
    NQ = D // QW
    NS = QW // HW
    scale = HW ** -0.5
    step = pl.program_id(0)
    last = pl.num_programs(0) - 1
    n_ff = FF // UNIT

    @pl.when(step == 0)
    def _():
        loads = [pltpu.make_async_copy(w, wqkvT.at[j * D:(j + 1) * D], wsem.at[j]) for j, w in enumerate((wq_h, wk_h, wv_h))]
        for cp in loads:
            cp.start()
        acc[...] = jnp.zeros_like(acc)
        for cp in loads:
            cp.wait()

    emb = emb_ref[...].astype(F32)
    xs[0] = x_ref[0] + emb[0:1].astype(BF)

    def fwd(l, carry):
        rows = pl.ds(pl.multiple_of(l * S, S), S)
        x = xs[l]
        xf = x.astype(F32)
        u = (xf * rms_scale(xf)).astype(BF)
        us[rows, :] = u
        def proj(part, c):
            cols = slice(part * D + c * QW, part * D + (c + 1) * QW)

            def run():
                qkv[rows, cols] = mm_nt(u, wqkvT[cols, :]).astype(BF)
            return run

        def quad(c):
            k4 = qkv[rows, D + c * QW:D + (c + 1) * QW]
            qm = head_stack(qkv[rows, c * QW:(c + 1) * QW], HW)

            def chunk(i):
                cols = slice(i * QW, (i + 1) * QW)

                def use(v):
                    sb = v.astype(BF)
                    st[l, c, :, cols] = sb
                    m, e, inv = soft_stats(sb, scale)
                    stat[l, c, 0:1, cols] = m
                    stat[l, c, 1:2, cols] = inv
                    pb[c, :, cols] = (e * inv).astype(BF)
                return (lambda: mm_nt(k4, qm[cols])), use
            return [chunk(i) for i in range(NS * S // QW)]

        def head_out(c, h):
            def run():
                vT = qkv[rows, 2 * D + c * QW:2 * D + (c + 1) * QW].T
                o = mm(vT[h * HW:(h + 1) * HW], pb[c, :, h * S:(h + 1) * S])
                mixT[c * QW + h * HW:c * QW + (h + 1) * HW, rows] = o.astype(BF)
            return run

        for part in range(3):
            proj(part, 0)()
        weave(quad(0), {0: [proj(0, 1)], 1: [proj(1, 1)], 2: [proj(2, 1)], 3: [head_out(0, 0)], 4: [head_out(0, 1)]})
        weave(quad(1), {0: [head_out(0, 2)], 1: [head_out(0, 3)], 3: [head_out(1, 0)], 4: [head_out(1, 1)]})
        head_out(1, 2)()
        head_out(1, 3)()
        h_mid = x + mm_tn(mixT[:, rows], wo_ref[...]).astype(BF)
        hs[l] = h_mid
        hf = h_mid.astype(F32)
        mn = (hf * rms_scale(hf)).astype(BF)
        mT[:, rows] = mn.T
        down = []

        def up_chunk(i):
            cols = slice(i * QW, (i + 1) * QW)

            def use(v):
                z = v.astype(BF)
                zs[rows, cols] = z
                gs[rows, cols] = gelu_fwd(z)
            return (lambda: mm(mn, wup_ref[:, cols])), use

        def down_part(j):
            cols = slice(j * UNIT, (j + 1) * UNIT)

            def run():
                v = mm(gs[rows, cols], wdn_ref[cols, :])
                down[:] = [v if not down else down[0] + v]
            return run

        weave([up_chunk(i) for i in range(FF // QW)], {2 * j + 1: [down_part(j)] for j in range(n_ff)})
        y = down[0]
        nxt = emb[1:2]
        for j in range(2, L):
            nxt = jnp.where(l + 1 == j, emb[j:j + 1], nxt)
        xs[l + 1] = (h_mid + y.astype(BF)) + nxt.astype(BF)
        return carry

    lax.fori_loop(0, L, fwd, 0)
    dcur[...] = g_ref[0]
    saves = [pltpu.make_async_copy(src, dst.at[step], ssem.at[n]) for n, (src, dst) in enumerate((
        (qkv.at[0:S], qkv0_h), (us.at[0:S], u0_h), (mixT.at[:, 0:S], mix0_h), (zs.at[0:S], z0_h),
        (mT.at[:, 0:S], mT0_h), (hs.at[0], h0_h), (dout.at[0:S], dout0_h)))]
    for cp in saves[:-1]:
        cp.start()

    def bwd(i, carry):
        l = L - 1 - i
        rows = pl.ds(pl.multiple_of(l * S, S), S)
        d_out = dcur[...]
        dout[rows, :] = d_out
        def add_unit(k, make):
            def run():
                acc[k] = acc[k] + make()
            return run

        ucol = lambda j: slice(j * UNIT, (j + 1) * UNIT)
        dn_unit = lambda j: add_unit(j, lambda: mm_tn(gs[rows, ucol(j)], d_out))
        up_unit = lambda j: add_unit(4 + j, lambda: mm(mT[:, rows], zs[rows, ucol(j)]))
        o_unit = add_unit(11, lambda: mm(mixT[:, rows], dmid[rows, :]))
        d_norm = mlp_bwd(d_out, (lambda cols: zs[rows, cols], zs), rows, wup_ref, wdn_ref, {2 * j: [dn_unit(j)] for j in range(n_ff)})
        d_mid = d_out + rms_bwd(hs[l], d_norm)
        dmid[rows, :] = d_mid
        d_mix = mm_nt(d_mid, wo_ref[...]).astype(BF)

        def prob(c, cols, unused):
            s = st[l, c, :, cols].astype(F32)
            return jnp.exp2((s - stat[l, c, 0:1, cols]) * (scale * LOG2E)) * stat[l, c, 1:2, cols]

        prob.recompute = False
        attn_bwd(qkv, rows, d_mix, HW, prob, pb, db, ({0: [up_unit(0)], 2: [up_unit(1)], 3: [up_unit(2)], 4: [up_unit(3)]}, {4: [o_unit]}))
        d_norm_x = mm(qkv[rows, :], wqkvT[...]).astype(BF)
        for j in range(3):
            acc[8 + j] = acc[8 + j] + mm_tn(qkv[rows, j * UNIT:(j + 1) * UNIT], us[rows, :])
        dcur[...] = d_mid + rms_bwd(xs[l], d_norm_x)
        return carry

    lax.fori_loop(0, L - 1, bwd, 0)
    dout[0:S, :] = dcur[...]
    saves[-1].start()

    @pl.when(step == last)
    def _():
        for k in range(4, 12):
            pltpu.make_async_copy(acc.at[k], acc_h.at[k], sem.at[k]).start()

    for j in range(n_ff):
        acc[j] = acc[j] + mm_tn(gs[0:S, j * UNIT:(j + 1) * UNIT], dout[0:S, :])
    for cp in saves:
        cp.wait()

    @pl.when(step == last)
    def _():
        for k in range(4):
            pltpu.make_async_copy(acc.at[k], acc_h.at[k], sem.at[k]).start()
        for k in range(12):
            pltpu.make_async_copy(acc.at[k], acc_h.at[k], sem.at[k]).wait()


def reduce_kernel(cfg, x_ref, emb_ref, qkv_ref, u_ref, mix_ref, z_ref, mT_ref, h_ref, dout_ref, wo_ref, wq_h, wk_h, wv_h, wup_h, wdn_h, acc_h,
                  dx_ref, dn_h, up_h, q_h, k_h, v_h, o_h,
                  wqkvT, wup, wdn, dup, dmid, dqkv, pb, db, acc2, aw, r1, r2, r3, res, send, recv, lsem, osem, wsem):
    B, S, D, FF, HW = cfg
    NQ = D // QW
    n_ff = FF // UNIT
    scale = HW ** -0.5
    step = pl.program_id(0)
    me = lax.axis_index('data')
    core = lax.rem(me, 2)
    bit_x = lax.rem(me // 2, 2)
    bit_y = me // 4
    core_peer = me + 1 - 2 * core
    x_peer = me + 2 - 4 * bit_x
    y_peer = me + 4 - 8 * bit_y
    half = UNIT // 2
    N_EARLY = n_ff
    N_ALL = 12

    def order(k):
        if k % 2 == 0:
            return (bit_x, x_peer), (bit_y, y_peer)
        return (bit_y, y_peer), (bit_x, x_peer)

    def aligned(v, n):
        return pl.ds(pl.multiple_of(v, n), n)

    def part(k, start, n):
        if k < N_EARLY:
            return aw.at[k, aligned(start, n)]
        return acc2.at[k - N_EARLY, aligned(core * half + start, n)]

    def remote(stage, k, src, dst, peer):
        return pltpu.make_async_remote_copy(src_ref=src, dst_ref=dst, send_sem=send.at[stage, k], recv_sem=recv.at[stage, k], device_id=(peer,), device_id_type=MESH)

    def copy_of(stage, k):
        (b1, p1), (b2, p2) = order(k)
        if stage == 0:
            rows = aligned((1 - core) * half, half)
            src = acc_h.at[k, rows] if k < N_EARLY else acc2.at[k - N_EARLY, rows]
            return remote(0, k, src, r1.at[k], core_peer)
        if stage == 1:
            return remote(1, k, part(k, (1 - b1) * 128, 128), r2.at[k], p1)
        if stage == 2:
            return remote(2, k, part(k, b1 * 128 + (1 - b2) * 64, 64), r3.at[k], p2)
        if stage == 3:
            mine = res.at[k, aligned(core * half + b1 * 128 + b2 * 64, 64)]
            return remote(3, k, mine, mine, p2)
        if stage == 4:
            mine = res.at[k, aligned(core * half + b1 * 128, 128)]
            return remote(4, k, mine, mine, p1)
        mine = res.at[k, aligned(core * half, half)]
        return remote(5, k, mine, mine, core_peer)

    def out_copy(k):
        if k < 4:
            dst = dn_h.at[k * UNIT:(k + 1) * UNIT]
        elif k < 8:
            dst = up_h.at[:, (k - 4) * UNIT:(k - 3) * UNIT]
        else:
            dst = (q_h, k_h, v_h, o_h)[k - 8]
        return pltpu.make_async_copy(res.at[k], dst, osem.at[k])

    def own_load(k):
        return pltpu.make_async_copy(acc_h.at[k, aligned(core * half, half)], aw.at[k], lsem.at[k])

    def late_load(k):
        return pltpu.make_async_copy(acc_h.at[k], acc2.at[k - N_EARLY], lsem.at[k])

    def serve(stage, k):
        (b1, _), (b2, _) = order(k)
        copy_of(stage, k).wait_recv()
        if stage == 0:
            if k < N_EARLY:
                own_load(k).wait()
            ref = part(k, 0, half)
            ref[...] = ref[...] + r1[k]
        elif stage == 1:
            ref = part(k, b1 * 128, 128)
            ref[...] = ref[...] + r2[k]
        elif stage == 2:
            ref = part(k, b1 * 128 + b2 * 64, 64)
            res[k, aligned(core * half + b1 * 128 + b2 * 64, 64)] = ref[...] + r3[k]
        if stage < 5:
            copy_of(stage + 1, k).start()
        else:
            out_copy(k).start()

    def serve_all(stage, units):
        for k in units:
            serve(stage, k)

    def begin(units):
        for k in units:
            copy_of(0, k).start()

    def w_loads():
        pairs = [(wdn_h, wdn), (wup_h, wup)] + [(w, wqkvT.at[j * D:(j + 1) * D]) for j, w in enumerate((wq_h, wk_h, wv_h))]
        return [pltpu.make_async_copy(s_, d_, wsem.at[j]) for j, (s_, d_) in enumerate(pairs)]

    @pl.when(step == 0)
    def _():
        barrier = pltpu.get_barrier_semaphore()
        for peer in (core_peer, x_peer, y_peer):
            pl.semaphore_signal(barrier, inc=1, device_id=(peer,), device_id_type=MESH)
        for k in range(N_EARLY):
            own_load(k).start()
        for cp in w_loads():
            cp.start()
        pl.semaphore_wait(barrier, 3)
        begin(range(N_EARLY))
        for k in range(N_EARLY, N_ALL):
            late_load(k).start()
        serve_all(0, range(N_EARLY))
        for cp in w_loads():
            cp.wait()
        for k in range(N_EARLY, N_ALL):
            late_load(k).wait()

    @pl.when(step < B)
    def _():
        d_out = dout_ref[0]
        d_norm = mlp_bwd(d_out, (lambda cols: z_ref[0, :, cols], dup), slice(0, S), wup, wdn, {})
        d_mid = d_out + rms_bwd(h_ref[0], d_norm)
        dmid[step] = d_mid
        for j in range(n_ff):
            acc2[j] = acc2[j] + mm(mT_ref[0], dup[:, j * UNIT:(j + 1) * UNIT])
        acc2[7] = acc2[7] + mm(mix_ref[0], d_mid)

    @pl.when(step >= B)
    def _():
        d_mid = dmid[step - B]
        d_mix = mm_nt(d_mid, wo_ref[...]).astype(BF)
        dqkv[...] = qkv_ref[0]

        def prob(c, cols, scores):
            m, e, inv = soft_stats(scores.astype(BF), scale)
            return e * inv

        prob.recompute = True
        attn_bwd(dqkv, slice(0, S), d_mix, HW, prob, pb, db, ({}, {}))
        d_norm_x = mm(dqkv[...], wqkvT[...]).astype(BF)
        x = x_ref[0] + emb_ref[0:1, :]
        dx_ref[0] = d_mid + rms_bwd(x, d_norm_x)
        for j in range(3):
            acc2[4 + j] = acc2[4 + j] + mm_tn(dqkv[:, j * UNIT:(j + 1) * UNIT], u_ref[0])

    def at_step(i, events, before=None):
        @pl.when(step == i)
        def _():
            if before is not None:
                begin(before)
            for stage, k in events:
                serve(stage, k)

    at_step(1, [(1, 0), (1, 1)])
    at_step(2, [(1, 2), (1, 3)])
    at_step(3, [(2, 1), (2, 0)])
    at_step(4, [(2, 2), (2, 3)])
    at_step(5, [(0, 4), (0, 5), (0, 6), (0, 7), (0, 11), (3, 1), (3, 0), (3, 2), (3, 3)], before=[4, 5, 6, 7, 11])
    at_step(6, [(1, 4), (1, 5)])
    at_step(7, [(1, 6), (1, 7)])
    at_step(8, [(4, 0), (1, 11)])
    at_step(9, [(4, 2), (4, 1), (5, 0), (2, 5), (2, 7), (4, 3)])
    at_step(10, [(2, 11), (5, 2), (2, 4), (5, 1), (5, 3), (3, 5), (2, 6)])

    @pl.when(step == 2 * B - 1)
    def _():
        begin([8, 9, 10])
        plan = [(0, 8), (0, 9), (0, 10), (3, 7), (3, 11), (3, 4), (4, 5), (5, 5), (3, 6), (1, 8), (1, 9), (1, 10), (4, 7), (5, 7),
                (4, 4), (5, 4), (4, 11), (5, 11), (2, 8), (4, 6), (5, 6), (2, 10), (2, 9), (3, 8), (3, 9), (3, 10), (4, 8), (5, 8),
                (4, 9), (5, 9), (4, 10), (5, 10)]
        for stage, k in plan:
            serve(stage, k)
        for k in range(N_ALL):
            for stage in range(6):
                copy_of(stage, k).wait_send()
        for k in range(N_ALL):
            out_copy(k).wait()


def solution(mesh):
    batch_spec = P('data', None, None)

    def per_device(x, g, emb, w_q, w_k, w_v, w_o, wup, wdn):
        D, H, HW = w_q.shape
        B, S, _ = x.shape
        FF = wup.shape[1]
        L = emb.shape[0]
        T = L * S
        NQ = D // QW
        NS = QW // HW
        w_t = [w.transpose(1, 2, 0).reshape(D, D) for w in (w_q, w_k, w_v)]
        wo = w_o.reshape(D, D)
        const = lambda shape: pl.BlockSpec(shape, lambda b: (0,) * len(shape), pipeline_mode=pl.Buffered(1))
        per_seq = lambda cols: pl.BlockSpec((1, S, cols), lambda b: (b, 0, 0))
        col_seq = pl.BlockSpec((D, S), lambda b: (0, b))
        hbm = pl.BlockSpec(memory_space=pl.ANY)
        sds = jax.ShapeDtypeStruct
        saved = [sds((B, S, 3 * D), BF), sds((B, S, D), BF), sds((B, D, S), BF), sds((B, S, FF), BF), sds((B, D, S), BF), sds((B, S, D), BF), sds((B, S, D), BF)]
        acc, qkv0, u0, mix0, z0, mT0, h0, dout0 = pl.pallas_call(
            functools.partial(step_kernel, (S, D, FF, HW, L)),
            name='block_grads',
            grid=(B,),
            in_specs=[per_seq(D), per_seq(D), const(emb.shape), hbm, hbm, hbm, const(wo.shape), const(wup.shape), const(wdn.shape)],
            out_specs=[hbm] * 8,
            out_shape=[sds((12, UNIT, UNIT), F32)] + saved,
            scratch_shapes=[
                pltpu.VMEM((L + 1, S, D), BF),
                pltpu.VMEM((T, D), BF),
                pltpu.VMEM((T, 3 * D), BF),
                pltpu.VMEM((L, NQ, S, NS * S), BF),
                pltpu.VMEM((L, NQ, 8, NS * S), F32),
                pltpu.VMEM((D, T), BF),
                pltpu.VMEM((L, S, D), BF),
                pltpu.VMEM((D, T), BF),
                pltpu.VMEM((T, FF), BF),
                pltpu.VMEM((T, FF), BF),
                pltpu.VMEM((T, D), BF),
                pltpu.VMEM((T, D), BF),
                pltpu.VMEM((S, D), BF),
                pltpu.VMEM((3 * D, D), BF),
                pltpu.VMEM((NQ, S, NS * S), BF),
                pltpu.VMEM((NQ, S, NS * S), BF),
                pltpu.VMEM((12, UNIT, UNIT), F32),
                pltpu.SemaphoreType.DMA((12,)),
                pltpu.SemaphoreType.DMA((3,)),
                pltpu.SemaphoreType.DMA((7,)),
            ],
            compiler_params=pltpu.CompilerParams(dimension_semantics=('arbitrary',), vmem_limit_bytes=VMEM_MAX),
        )(x, g, emb, *w_t, wo, wup, wdn)
        first = lambda *shape: pl.BlockSpec((1,) + shape, lambda i: (jnp.minimum(i, B - 1), 0, 0))
        second = lambda *shape: pl.BlockSpec((1,) + shape, lambda i: (jnp.maximum(i - B, 0), 0, 0))
        outs = pl.pallas_call(
            functools.partial(reduce_kernel, (B, S, D, FF, HW)),
            name='attn_reduce',
            grid=(2 * B,),
            in_specs=[second(S, D), const(emb.shape), second(S, 3 * D), second(S, D), first(D, S), first(S, FF), first(D, S), first(S, D), first(S, D), const(wo.shape)] + [hbm] * 6,
            out_specs=[second(S, D)] + [hbm] * 6,
            out_shape=[sds(x.shape, BF), sds((FF, D), F32), sds((D, FF), F32)] + [sds((D, D), F32)] * 4,
            scratch_shapes=[
                pltpu.VMEM((3 * D, D), BF),
                pltpu.VMEM((D, FF), BF),
                pltpu.VMEM((FF, D), BF),
                pltpu.VMEM((S, FF), BF),
                pltpu.VMEM((B, S, D), BF),
                pltpu.VMEM((S, 3 * D), BF),
                pltpu.VMEM((NQ, S, NS * S), BF),
                pltpu.VMEM((NQ, S, NS * S), BF),
                pltpu.VMEM((8, UNIT, UNIT), F32),
                pltpu.VMEM((4, UNIT // 2, UNIT), F32),
                pltpu.VMEM((12, UNIT // 2, UNIT), F32),
                pltpu.VMEM((12, 128, UNIT), F32),
                pltpu.VMEM((12, 64, UNIT), F32),
                pltpu.VMEM((12, UNIT, UNIT), F32),
                pltpu.SemaphoreType.DMA((6, 12)),
                pltpu.SemaphoreType.DMA((6, 12)),
                pltpu.SemaphoreType.DMA((12,)),
                pltpu.SemaphoreType.DMA((12,)),
                pltpu.SemaphoreType.DMA((5,)),
            ],
            compiler_params=pltpu.CompilerParams(dimension_semantics=('arbitrary',), vmem_limit_bytes=VMEM_MAX, collective_id=0, has_side_effects=True),
        )(x, emb, qkv0, u0, mix0, z0, mT0, h0, dout0, wo, *w_t, wup, wdn, acc)
        d_x, dn, up, gq, gk, gv, go = outs
        back = lambda a: a.reshape(H, HW, D).transpose(2, 0, 1)
        return back(gq), back(gk), back(gv), go.reshape(H, HW, D), up, dn, d_x

    return jax.shard_map(per_device, mesh=mesh, in_specs=(batch_spec, batch_spec, P(), P(), P(), P(), P(), P(), P()), out_specs=(P(), P(), P(), P(), P(), P(), batch_spec), check_vma=False)
```

```python
import functools

import jax
import jax.numpy as jnp
from jax import lax
from jax.experimental import pallas as pl
from jax.experimental.pallas import tpu as pltpu
from jax.sharding import PartitionSpec as P

NORM_EPS = 1e-6
BF = jnp.bfloat16
F32 = jnp.float32
GELU_C = 0.7978845608028654
GELU_A = 0.044715
LOG2E = 1.4426950408889634
MESH = pl.DeviceIdType.MESH
UNIT = 512
QW = 256
VMEM_MAX = 67043328


def mm(a, b):
    return lax.dot_general(a, b, (((1,), (0,)), ((), ())), preferred_element_type=F32)


def mm_nt(a, b):
    return lax.dot_general(a, b, (((1,), (1,)), ((), ())), preferred_element_type=F32)


def mm_tn(a, b):
    return lax.dot_general(a, b, (((0,), (0,)), ((), ())), preferred_element_type=F32)


def rms_scale(xf):
    return lax.rsqrt(jnp.mean(xf * xf, axis=-1, keepdims=True) + NORM_EPS)


def rms_bwd(x, dy):
    xf = x.astype(F32)
    gf = dy.astype(F32)
    r = rms_scale(xf)
    dot = jnp.mean(xf * gf, axis=-1, keepdims=True)
    return (gf * r - xf * (r * r * r * dot)).astype(BF)


def gelu_fwd(z):
    zf = z.astype(F32)
    t = jnp.tanh(zf * (GELU_C + (GELU_C * GELU_A) * (zf * zf)))
    half = 0.5 * zf
    return (half + half * t).astype(BF)


def gelu_bwd(z, dg):
    zf = z.astype(F32)
    z2 = zf * zf
    t = jnp.tanh(zf * (GELU_C + (GELU_C * GELU_A) * z2))
    slope = (0.5 + 0.5 * t) + ((1.0 - t * t) * zf) * ((0.5 * GELU_C) + (1.5 * GELU_C * GELU_A) * z2)
    return (dg.astype(F32) * slope).astype(BF)


def head_stack(a4, width):
    lane = lax.broadcasted_iota(jnp.int32, a4.shape, 1)
    zero = jnp.zeros_like(a4)
    n_sub = a4.shape[1] // width
    return jnp.concatenate([jnp.where((lane >= h * width) & (lane < (h + 1) * width), a4, zero) for h in range(n_sub)], axis=0)


def soft_stats(sb, scale):
    m = jnp.max(sb, axis=0, keepdims=True).astype(F32)
    e = jnp.exp2((sb.astype(F32) - m) * (scale * LOG2E))
    inv = 1.0 / jnp.sum(e, axis=0, keepdims=True)
    return m, e, inv


def weave(chunks, fill):
    ahead = chunks[0][0]()
    for i, (_, use) in enumerate(chunks):
        now = ahead
        if i + 1 < len(chunks):
            ahead = chunks[i + 1][0]()
        use(now)
        for f in fill.get(i, ()):
            f()


def attn_bwd(qkv, rows, d_mix, HW, prob, pb, db, fills):
    S, D = d_mix.shape
    ns = QW // HW
    scale = HW ** -0.5
    width = ns * S
    tails = []
    for c in range(D // QW):
        qc = slice(c * QW, (c + 1) * QW)
        kc = slice(D + c * QW, D + (c + 1) * QW)
        vc = slice(2 * D + c * QW, 2 * D + (c + 1) * QW)
        k4 = qkv[rows, kc]
        v4 = qkv[rows, vc]
        qm = head_stack(qkv[rows, qc], HW)
        dom = head_stack(d_mix[:, qc], HW)
        kT = k4.T

        def chunk(i, c=c, k4=k4, v4=v4, qm=qm, dom=dom):
            cols = slice(i * QW, (i + 1) * QW)

            def use(vals):
                p = prob(c, cols, vals[1])
                dp = vals[0].astype(BF).astype(F32)
                delta = jnp.sum(dp * p, axis=0, keepdims=True)
                pb[c, :, cols] = p.astype(BF)
                db[c, :, cols] = ((p * (dp - delta)) * scale).astype(BF)
            return (lambda: (mm_nt(v4, dom[cols]), mm_nt(k4, qm[cols]) if prob.recompute else None)), use

        fill = {i: list(f) for i, f in fills[c].items()}
        for i, f in enumerate(tails):
            fill.setdefault(i, []).insert(0, f)

        def tail_v(c=c, vc=vc, dom=dom):
            qkv[rows, vc] = mm(pb[c], dom).astype(BF)

        def tail_k(c=c, kc=kc, qm=qm):
            qkv[rows, kc] = mm(db[c], qm).astype(BF)

        def tail_q(c=c, qc=qc, kT=kT):
            dqT = [mm(kT[h * HW:(h + 1) * HW], db[c, :, h * S:(h + 1) * S]).astype(BF) for h in range(ns)]
            qkv[rows, qc] = jnp.concatenate(dqT, axis=0).T

        weave([chunk(i) for i in range(width // QW)], fill)
        tails = [tail_v, tail_k, tail_q]
    for f in tails:
        f()


def mlp_bwd(d_out, zs, rows, wup, wdn, fill):
    FF = wdn.shape[0]
    total = []

    def chunk(i):
        cols = slice(i * QW, (i + 1) * QW)

        def use(v):
            zs[1][rows, cols] = gelu_bwd(zs[0](cols), v.astype(BF))
        return (lambda: mm_nt(d_out, wdn[cols, :])), use

    def part(j):
        cols = slice(j * UNIT, (j + 1) * UNIT)

        def run():
            v = mm_nt(zs[1][rows, cols], wup[:, cols])
            total[:] = [v if not total else total[0] + v]
        return run

    fill = {i: list(f) for i, f in fill.items()}
    for j in range(FF // UNIT):
        fill.setdefault(2 * j + 1, []).append(part(j))
    weave([chunk(i) for i in range(FF // QW)], fill)
    return total[0].astype(BF)


def step_kernel(cfg, x_ref, g_ref, emb_ref, wq_h, wk_h, wv_h, wo_ref, wup_ref, wdn_ref,
                acc_h, qkv0_h, u0_h, mix0_h, z0_h, mT0_h, h0_h, dout0_h,
                xs, us, qkv, st, stat, mixT, hs, mT, zs, gs, dmid, dout, dcur, wqkvT, pb, db, acc, sem, wsem, ssem):
    S, D, FF, HW, L = cfg
    NQ = D // QW
    NS = QW // HW
    scale = HW ** -0.5
    step = pl.program_id(0)
    last = pl.num_programs(0) - 1
    n_ff = FF // UNIT

    @pl.when(step == 0)
    def _():
        loads = [pltpu.make_async_copy(w, wqkvT.at[j * D:(j + 1) * D], wsem.at[j]) for j, w in enumerate((wq_h, wk_h, wv_h))]
        for cp in loads:
            cp.start()
        acc[...] = jnp.zeros_like(acc)
        for cp in loads:
            cp.wait()

    emb = emb_ref[...].astype(F32)
    xs[0] = x_ref[0] + emb[0:1].astype(BF)

    def fwd(l, carry):
        rows = pl.ds(pl.multiple_of(l * S, S), S)
        x = xs[l]
        xf = x.astype(F32)
        u = (xf * rms_scale(xf)).astype(BF)
        us[rows, :] = u
        def proj(part, c):
            cols = slice(part * D + c * QW, part * D + (c + 1) * QW)

            def run():
                qkv[rows, cols] = mm_nt(u, wqkvT[cols, :]).astype(BF)
            return run

        def quad(c):
            k4 = qkv[rows, D + c * QW:D + (c + 1) * QW]
            qm = head_stack(qkv[rows, c * QW:(c + 1) * QW], HW)

            def chunk(i):
                cols = slice(i * QW, (i + 1) * QW)

                def use(v):
                    sb = v.astype(BF)
                    st[l, c, :, cols] = sb
                    m, e, inv = soft_stats(sb, scale)
                    stat[l, c, 0:1, cols] = m
                    stat[l, c, 1:2, cols] = inv
                    pb[c, :, cols] = (e * inv).astype(BF)
                return (lambda: mm_nt(k4, qm[cols])), use
            return [chunk(i) for i in range(NS * S // QW)]

        def head_out(c, h):
            def run():
                vT = qkv[rows, 2 * D + c * QW:2 * D + (c + 1) * QW].T
                o = mm(vT[h * HW:(h + 1) * HW], pb[c, :, h * S:(h + 1) * S])
                mixT[c * QW + h * HW:c * QW + (h + 1) * HW, rows] = o.astype(BF)
            return run

        for part in range(3):
            proj(part, 0)()
        weave(quad(0), {0: [proj(0, 1)], 1: [proj(1, 1)], 2: [proj(2, 1)], 3: [head_out(0, 0)], 4: [head_out(0, 1)]})
        weave(quad(1), {0: [head_out(0, 2)], 1: [head_out(0, 3)], 3: [head_out(1, 0)], 4: [head_out(1, 1)]})
        head_out(1, 2)()
        head_out(1, 3)()
        h_mid = x + mm_tn(mixT[:, rows], wo_ref[...]).astype(BF)
        hs[l] = h_mid
        hf = h_mid.astype(F32)
        mn = (hf * rms_scale(hf)).astype(BF)
        mT[:, rows] = mn.T
        down = []

        def up_chunk(i):
            cols = slice(i * QW, (i + 1) * QW)

            def use(v):
                z = v.astype(BF)
                zs[rows, cols] = z
                gs[rows, cols] = gelu_fwd(z)
            return (lambda: mm(mn, wup_ref[:, cols])), use

        def down_part(j):
            cols = slice(j * UNIT, (j + 1) * UNIT)

            def run():
                v = mm(gs[rows, cols], wdn_ref[cols, :])
                down[:] = [v if not down else down[0] + v]
            return run

        weave([up_chunk(i) for i in range(FF // QW)], {2 * j + 1: [down_part(j)] for j in range(n_ff)})
        y = down[0]
        nxt = emb[1:2]
        for j in range(2, L):
            nxt = jnp.where(l + 1 == j, emb[j:j + 1], nxt)
        xs[l + 1] = (h_mid + y.astype(BF)) + nxt.astype(BF)
        return carry

    lax.fori_loop(0, L, fwd, 0)
    dcur[...] = g_ref[0]
    saves = [pltpu.make_async_copy(src, dst.at[step], ssem.at[n]) for n, (src, dst) in enumerate((
        (qkv.at[0:S], qkv0_h), (us.at[0:S], u0_h), (mixT.at[:, 0:S], mix0_h), (zs.at[0:S], z0_h),
        (mT.at[:, 0:S], mT0_h), (hs.at[0], h0_h), (dout.at[0:S], dout0_h)))]
    for cp in saves[:-1]:
        cp.start()

    def bwd(i, carry):
        l = L - 1 - i
        rows = pl.ds(pl.multiple_of(l * S, S), S)
        d_out = dcur[...]
        dout[rows, :] = d_out
        def add_unit(k, make):
            def run():
                acc[k] = acc[k] + make()
            return run

        ucol = lambda j: slice(j * UNIT, (j + 1) * UNIT)
        dn_unit = lambda j: add_unit(j, lambda: mm_tn(gs[rows, ucol(j)], d_out))
        up_unit = lambda j: add_unit(4 + j, lambda: mm(mT[:, rows], zs[rows, ucol(j)]))
        o_unit = add_unit(11, lambda: mm(mixT[:, rows], dmid[rows, :]))
        d_norm = mlp_bwd(d_out, (lambda cols: zs[rows, cols], zs), rows, wup_ref, wdn_ref, {2 * j: [dn_unit(j)] for j in range(n_ff)})
        d_mid = d_out + rms_bwd(hs[l], d_norm)
        dmid[rows, :] = d_mid
        d_mix = mm_nt(d_mid, wo_ref[...]).astype(BF)

        def prob(c, cols, unused):
            s = st[l, c, :, cols].astype(F32)
            return jnp.exp2((s - stat[l, c, 0:1, cols]) * (scale * LOG2E)) * stat[l, c, 1:2, cols]

        prob.recompute = False
        attn_bwd(qkv, rows, d_mix, HW, prob, pb, db, ({0: [up_unit(0)], 2: [up_unit(1)], 3: [up_unit(2)], 4: [up_unit(3)]}, {4: [o_unit]}))
        d_norm_x = mm(qkv[rows, :], wqkvT[...]).astype(BF)
        for j in range(3):
            acc[8 + j] = acc[8 + j] + mm_tn(qkv[rows, j * UNIT:(j + 1) * UNIT], us[rows, :])
        dcur[...] = d_mid + rms_bwd(xs[l], d_norm_x)
        return carry

    lax.fori_loop(0, L - 1, bwd, 0)
    dout[0:S, :] = dcur[...]
    saves[-1].start()

    @pl.when(step == last)
    def _():
        for k in range(4, 12):
            pltpu.make_async_copy(acc.at[k], acc_h.at[k], sem.at[k]).start()

    for j in range(n_ff):
        acc[j] = acc[j] + mm_tn(gs[0:S, j * UNIT:(j + 1) * UNIT], dout[0:S, :])
    for cp in saves:
        cp.wait()

    @pl.when(step == last)
    def _():
        for k in range(4):
            pltpu.make_async_copy(acc.at[k], acc_h.at[k], sem.at[k]).start()
        for k in range(12):
            pltpu.make_async_copy(acc.at[k], acc_h.at[k], sem.at[k]).wait()


def reduce_kernel(cfg, emb_ref, wo_ref, x_h, qkv_h, u_h, mix_h, z_h, mT_h, h_h, dout_h, wq_h, wk_h, wv_h, wup_h, wdn_h, acc_h,
                  dx_ref, r_dn, r_up, r_q, r_k, r_v, r_o,
                  xb, qkvb, ub, mixb, zb, mTb, hb, doutb,
                  wqkvT, wup, wdn, dup, dmid, pb, db, acc2, aw, r1, r2, r3, send, recv, lsem, wsem, isem):
    B, S, D, FF, HW = cfg
    NQ = D // QW
    n_ff = FF // UNIT
    scale = HW ** -0.5
    me = lax.axis_index('data')
    core = lax.rem(me, 2)
    bit_x = lax.rem(me // 2, 2)
    bit_y = me // 4
    core_peer = me + 1 - 2 * core
    x_peer = me + 2 - 4 * bit_x
    y_peer = me + 4 - 8 * bit_y
    half = UNIT // 2
    N_EARLY = n_ff
    N_ALL = 12

    def order(k):
        if k % 2 == 0:
            return (bit_x, x_peer), (bit_y, y_peer)
        return (bit_y, y_peer), (bit_x, x_peer)

    def aligned(v, n):
        return pl.ds(pl.multiple_of(v, n), n)

    def part(k, start, n):
        if k < N_EARLY:
            return aw.at[k, aligned(start, n)]
        return acc2.at[k - N_EARLY, aligned(core * half + start, n)]

    def remote(stage, k, src, dst, peer):
        return pltpu.make_async_remote_copy(src_ref=src, dst_ref=dst, send_sem=send.at[stage, k], recv_sem=recv.at[stage, k], device_id=(peer,), device_id_type=MESH)

    def copy_of(stage, k):
        (b1, p1), (b2, p2) = order(k)
        if stage == 0:
            rows = aligned((1 - core) * half, half)
            src = acc_h.at[k, rows] if k < N_EARLY else acc2.at[k - N_EARLY, rows]
            return remote(0, k, src, r1.at[k], core_peer)
        if stage == 1:
            return remote(1, k, part(k, (1 - b1) * 128, 128), r2.at[k], p1)
        if stage == 2:
            return remote(2, k, part(k, b1 * 128 + (1 - b2) * 64, 64), r3.at[k], p2)
        if stage == 3:
            mine = res_at(k, b1 * 128 + b2 * 64, 64)
            return remote(3, k, mine, mine, p2)
        if stage == 4:
            mine = res_at(k, b1 * 128, 128)
            return remote(4, k, mine, mine, p1)
        mine = res_at(k, 0, half)
        return remote(5, k, mine, mine, core_peer)

    def res_at(k, start, n):
        if k < 4:
            return r_dn.at[aligned(k * UNIT + core * half + start, n)]
        rows = aligned(core * half + start, n)
        if k < 8:
            return r_up.at[rows, (k - 4) * UNIT:(k - 3) * UNIT]
        return (r_q, r_k, r_v, r_o)[k - 8].at[rows]

    def own_load(k):
        return pltpu.make_async_copy(acc_h.at[k, aligned(core * half, half)], aw.at[k], lsem.at[k])

    def late_load(k):
        return pltpu.make_async_copy(acc_h.at[k], acc2.at[k - N_EARLY], lsem.at[k])

    def serve(stage, k):
        (b1, _), (b2, _) = order(k)
        copy_of(stage, k).wait_recv()
        if stage == 0:
            if k < N_EARLY:
                own_load(k).wait()
            ref = part(k, 0, half)
            ref[...] = ref[...] + r1[k]
        elif stage == 1:
            ref = part(k, b1 * 128, 128)
            ref[...] = ref[...] + r2[k]
        elif stage == 2:
            ref = part(k, b1 * 128 + b2 * 64, 64)
            res_at(k, b1 * 128 + b2 * 64, 64)[...] = ref[...] + r3[k]
        if stage < 5:
            copy_of(stage + 1, k).start()

    def serve_all(stage, units):
        for k in units:
            serve(stage, k)

    def begin(units):
        for k in units:
            copy_of(0, k).start()

    def fetch(phase, i):
        slot = lax.rem(i, 2)
        pairs = ((mix_h, mixb), (z_h, zb), (mT_h, mTb), (h_h, hb), (dout_h, doutb)) if phase == 0 else ((x_h, xb), (qkv_h, qkvb), (u_h, ub))
        return [pltpu.make_async_copy(s_.at[i], d_.at[slot], isem.at[phase * 5 + n, slot]) for n, (s_, d_) in enumerate(pairs)]

    def arrive(phase, i):
        for cp in fetch(phase, i):
            cp.wait()

        @pl.when(i + 1 < B)
        def _():
            for cp in fetch(phase, i + 1):
                cp.start()
        return lax.rem(i, 2)

    def w_loads():
        pairs = [(wdn_h, wdn), (wup_h, wup)] + [(w, wqkvT.at[j * D:(j + 1) * D]) for j, w in enumerate((wq_h, wk_h, wv_h))]
        return [pltpu.make_async_copy(s_, d_, wsem.at[j]) for j, (s_, d_) in enumerate(pairs)]

    barrier = pltpu.get_barrier_semaphore()
    for peer in (core_peer, x_peer, y_peer):
        pl.semaphore_signal(barrier, inc=1, device_id=(peer,), device_id_type=MESH)
    for k in range(N_EARLY):
        own_load(k).start()
    for cp in fetch(0, 0):
        cp.start()
    for cp in w_loads():
        cp.start()
    pl.semaphore_wait(barrier, 3)
    begin(range(N_EARLY))
    for k in range(N_EARLY, N_ALL):
        late_load(k).start()
    serve_all(0, range(N_EARLY))
    for cp in w_loads():
        cp.wait()
    for k in range(N_EARLY, N_ALL):
        late_load(k).wait()

    def run_events(events):
        for stage, unit in zip(events[::2], events[1::2]):
            serve(int(stage), int(unit, 16))

    def at_step(step, i, events, before=''):
        @pl.when(step == i)
        def _():
            begin([int(unit, 16) for unit in before])
            run_events(events)

    def phase1(step, carry):
        slot = arrive(0, step)
        d_out = doutb[slot]

        def up_unit(j):
            def run():
                acc2[j] = acc2[j] + mm(mTb[slot], dup[:, j * UNIT:(j + 1) * UNIT])
            return run

        d_norm = mlp_bwd(d_out, (lambda cols: zb[slot, :, cols], dup), slice(0, S), wup, wdn, {2: [up_unit(0)], 4: [up_unit(1)], 6: [up_unit(2)]})
        d_mid = d_out + rms_bwd(hb[slot], d_norm)
        dmid[step] = d_mid
        up_unit(3)()
        acc2[7] = acc2[7] + mm(mixb[slot], d_mid)

        at_step(step, 1, '1110')
        at_step(step, 2, '122113')
        at_step(step, 3, '222031')
        at_step(step, 4, '3223')
        at_step(step, 5, '060b040705414230', before='6b475')
        return carry

    for cp in fetch(1, 0):
        cp.start()
    lax.fori_loop(0, B, phase1, 0)

    def phase2(step, carry):
        slot = arrive(1, step)
        d_mid = dmid[step]
        d_mix = mm_nt(d_mid, wo_ref[...]).astype(BF)
        dqkv = qkvb.at[slot]

        def prob(c, cols, scores):
            m, e, inv = soft_stats(scores.astype(BF), scale)
            return e * inv

        prob.recompute = True
        attn_bwd(dqkv, slice(0, S), d_mix, HW, prob, pb, db, ({}, {}))
        d_norm_x = mm(dqkv[...], wqkvT[...]).astype(BF)
        x = xb[slot] + emb_ref[0:1, :]
        dx_ref[step] = d_mid + rms_bwd(x, d_norm_x)
        for j in range(3):
            acc2[4 + j] = acc2[4 + j] + mm_tn(dqkv[:, j * UNIT:(j + 1) * UNIT], ub[slot])

        at_step(step, 0, '161b335152')
        at_step(step, 1, '1417')
        at_step(step, 2, '15262b2740')
        at_step(step, 3, '2425363b4350')
        at_step(step, 4, '34353753')
        return carry

    lax.fori_loop(0, B, phase2, 0)

    begin([8, 9, 10])
    run_events('08090a464b444556475b54555718')
    run_events('19281a29382a393a4858494a595a')
    for k in range(N_ALL):
        for stage in range(6):
            copy_of(stage, k).wait_send()


def solution(mesh):
    batch_spec = P('data', None, None)

    def per_device(x, g, emb, w_q, w_k, w_v, w_o, wup, wdn):
        D, H, HW = w_q.shape
        B, S, _ = x.shape
        FF = wup.shape[1]
        L = emb.shape[0]
        T = L * S
        NQ = D // QW
        NS = QW // HW
        w_t = [w.transpose(1, 2, 0).reshape(D, D) for w in (w_q, w_k, w_v)]
        wo = w_o.reshape(D, D)
        const = lambda shape: pl.BlockSpec(shape, lambda b: (0,) * len(shape), pipeline_mode=pl.Buffered(1))
        per_seq = lambda cols: pl.BlockSpec((1, S, cols), lambda b: (b, 0, 0))
        col_seq = pl.BlockSpec((D, S), lambda b: (0, b))
        hbm = pl.BlockSpec(memory_space=pl.ANY)
        sds = jax.ShapeDtypeStruct
        saved = [sds((B, S, 3 * D), BF), sds((B, S, D), BF), sds((B, D, S), BF), sds((B, S, FF), BF), sds((B, D, S), BF), sds((B, S, D), BF), sds((B, S, D), BF)]
        acc, qkv0, u0, mix0, z0, mT0, h0, dout0 = pl.pallas_call(
            functools.partial(step_kernel, (S, D, FF, HW, L)),
            name='block_grads',
            grid=(B,),
            in_specs=[per_seq(D), per_seq(D), const(emb.shape), hbm, hbm, hbm, const(wo.shape), const(wup.shape), const(wdn.shape)],
            out_specs=[hbm] * 8,
            out_shape=[sds((12, UNIT, UNIT), F32)] + saved,
            scratch_shapes=[
                pltpu.VMEM((L + 1, S, D), BF),
                pltpu.VMEM((T, D), BF),
                pltpu.VMEM((T, 3 * D), BF),
                pltpu.VMEM((L, NQ, S, NS * S), BF),
                pltpu.VMEM((L, NQ, 8, NS * S), F32),
                pltpu.VMEM((D, T), BF),
                pltpu.VMEM((L, S, D), BF),
                pltpu.VMEM((D, T), BF),
                pltpu.VMEM((T, FF), BF),
                pltpu.VMEM((T, FF), BF),
                pltpu.VMEM((T, D), BF),
                pltpu.VMEM((T, D), BF),
                pltpu.VMEM((S, D), BF),
                pltpu.VMEM((3 * D, D), BF),
                pltpu.VMEM((NQ, S, NS * S), BF),
                pltpu.VMEM((NQ, S, NS * S), BF),
                pltpu.VMEM((12, UNIT, UNIT), F32),
                pltpu.SemaphoreType.DMA((12,)),
                pltpu.SemaphoreType.DMA((3,)),
                pltpu.SemaphoreType.DMA((7,)),
            ],
            compiler_params=pltpu.CompilerParams(dimension_semantics=('arbitrary',), vmem_limit_bytes=VMEM_MAX),
        )(x, g, emb, *w_t, wo, wup, wdn)
        vmem = pl.BlockSpec(memory_space=pltpu.VMEM)
        outs = pl.pallas_call(
            functools.partial(reduce_kernel, (B, S, D, FF, HW)),
            name='attn_reduce',
            in_specs=[vmem, vmem] + [hbm] * 14,
            out_specs=[vmem] * 7,
            out_shape=[pltpu.VMEM(x.shape, BF), pltpu.VMEM((FF, D), F32), pltpu.VMEM((D, FF), F32)] + [pltpu.VMEM((D, D), F32)] * 4,
            scratch_shapes=[
                pltpu.VMEM((2, S, D), BF),
                pltpu.VMEM((2, S, 3 * D), BF),
                pltpu.VMEM((2, S, D), BF),
                pltpu.VMEM((2, D, S), BF),
                pltpu.VMEM((2, S, FF), BF),
                pltpu.VMEM((2, D, S), BF),
                pltpu.VMEM((2, S, D), BF),
                pltpu.VMEM((2, S, D), BF),
                pltpu.VMEM((3 * D, D), BF),
                pltpu.VMEM((D, FF), BF),
                pltpu.VMEM((FF, D), BF),
                pltpu.VMEM((S, FF), BF),
                pltpu.VMEM((B, S, D), BF),
                pltpu.VMEM((NQ, S, NS * S), BF),
                pltpu.VMEM((NQ, S, NS * S), BF),
                pltpu.VMEM((8, UNIT, UNIT), F32),
                pltpu.VMEM((4, UNIT // 2, UNIT), F32),
                pltpu.VMEM((12, UNIT // 2, UNIT), F32),
                pltpu.VMEM((12, 128, UNIT), F32),
                pltpu.VMEM((12, 64, UNIT), F32),
                pltpu.SemaphoreType.DMA((6, 12)),
                pltpu.SemaphoreType.DMA((6, 12)),
                pltpu.SemaphoreType.DMA((12,)),
                pltpu.SemaphoreType.DMA((5,)),
                pltpu.SemaphoreType.DMA((8, 2)),
            ],
            compiler_params=pltpu.CompilerParams(vmem_limit_bytes=VMEM_MAX - (16 << 20), collective_id=0, has_side_effects=True),
        )(emb, wo, x, qkv0, u0, mix0, z0, mT0, h0, dout0, *w_t, wup, wdn, acc)
        d_x, dn, up, gq, gk, gv, go = outs
        back = lambda a: a.reshape(H, HW, D).transpose(2, 0, 1)
        return back(gq), back(gk), back(gv), go.reshape(H, HW, D), up, dn, d_x

    return jax.shard_map(per_device, mesh=mesh, in_specs=(batch_spec, batch_spec, P(), P(), P(), P(), P(), P(), P()), out_specs=(P(), P(), P(), P(), P(), P(), batch_spec), check_vma=False)
```

```python
import functools

import jax
import jax.numpy as jnp
from jax import lax
from jax.experimental import pallas as pl
from jax.experimental.pallas import tpu as pltpu
from jax.sharding import PartitionSpec as P

NORM_EPS = 1e-6
BF = jnp.bfloat16
F32 = jnp.float32
GELU_C = 0.7978845608028654
GELU_A = 0.044715
LOG2E = 1.4426950408889634
MESH = pl.DeviceIdType.MESH
UNIT = 512
QW = 256
VMEM_MAX = 67043328


def mm(a, b):
    return lax.dot_general(a, b, (((1,), (0,)), ((), ())), preferred_element_type=F32)


def mm_nt(a, b):
    return lax.dot_general(a, b, (((1,), (1,)), ((), ())), preferred_element_type=F32)


def mm_tn(a, b):
    return lax.dot_general(a, b, (((0,), (0,)), ((), ())), preferred_element_type=F32)


def rms_scale(xf):
    return lax.rsqrt(jnp.mean(xf * xf, axis=-1, keepdims=True) + NORM_EPS)


def rms_bwd(x, dy):
    xf = x.astype(F32)
    gf = dy.astype(F32)
    r = rms_scale(xf)
    dot = jnp.mean(xf * gf, axis=-1, keepdims=True)
    return (gf * r - xf * (r * r * r * dot)).astype(BF)


def gelu_fwd(z):
    zf = z.astype(F32)
    t = jnp.tanh(zf * (GELU_C + (GELU_C * GELU_A) * (zf * zf)))
    half = 0.5 * zf
    return (half + half * t).astype(BF)


def gelu_bwd(z, dg):
    zf = z.astype(F32)
    z2 = zf * zf
    t = jnp.tanh(zf * (GELU_C + (GELU_C * GELU_A) * z2))
    slope = (0.5 + 0.5 * t) + ((1.0 - t * t) * zf) * ((0.5 * GELU_C) + (1.5 * GELU_C * GELU_A) * z2)
    return (dg.astype(F32) * slope).astype(BF)


def head_stack(a4, width):
    lane = lax.broadcasted_iota(jnp.int32, a4.shape, 1)
    zero = jnp.zeros_like(a4)
    n_sub = a4.shape[1] // width
    return jnp.concatenate([jnp.where((lane >= h * width) & (lane < (h + 1) * width), a4, zero) for h in range(n_sub)], axis=0)


def soft_stats(sb, scale):
    m = jnp.max(sb, axis=0, keepdims=True).astype(F32)
    e = jnp.exp2((sb.astype(F32) - m) * (scale * LOG2E))
    inv = 1.0 / jnp.sum(e, axis=0, keepdims=True)
    return m, e, inv


def weave(chunks, fill):
    ahead = chunks[0][0]()
    for i, (_, use) in enumerate(chunks):
        now = ahead
        if i + 1 < len(chunks):
            ahead = chunks[i + 1][0]()
        use(now)
        for f in fill.get(i, ()):
            f()


def attn_bwd(qkv, rows, d_mix, HW, prob, pb, db, fills):
    S, D = d_mix.shape
    ns = QW // HW
    scale = HW ** -0.5
    width = ns * S
    tails = []
    for c in range(D // QW):
        qc = slice(c * QW, (c + 1) * QW)
        kc = slice(D + c * QW, D + (c + 1) * QW)
        vc = slice(2 * D + c * QW, 2 * D + (c + 1) * QW)
        k4 = qkv[rows, kc]
        v4 = qkv[rows, vc]
        qm = head_stack(qkv[rows, qc], HW)
        dom = head_stack(d_mix[:, qc], HW)
        kT = k4.T

        def chunk(i, c=c, k4=k4, v4=v4, qm=qm, dom=dom):
            cols = slice(i * QW, (i + 1) * QW)

            def use(vals):
                p = prob(c, cols, vals[1])
                dp = vals[0].astype(BF).astype(F32)
                delta = jnp.sum(dp * p, axis=0, keepdims=True)
                pb[c, :, cols] = p.astype(BF)
                db[c, :, cols] = ((p * (dp - delta)) * scale).astype(BF)
            return (lambda: (mm_nt(v4, dom[cols]), mm_nt(k4, qm[cols]) if prob.recompute else None)), use

        fill = {i: list(f) for i, f in fills[c].items()}
        for i, f in enumerate(tails):
            fill.setdefault(i, []).insert(0, f)

        def tail_v(c=c, vc=vc, dom=dom):
            qkv[rows, vc] = mm(pb[c], dom).astype(BF)

        def tail_k(c=c, kc=kc, qm=qm):
            qkv[rows, kc] = mm(db[c], qm).astype(BF)

        def tail_q(c=c, qc=qc, kT=kT):
            dqT = [mm(kT[h * HW:(h + 1) * HW], db[c, :, h * S:(h + 1) * S]).astype(BF) for h in range(ns)]
            qkv[rows, qc] = jnp.concatenate(dqT, axis=0).T

        weave([chunk(i) for i in range(width // QW)], fill)
        tails = [tail_v, tail_k, tail_q]
    for f in tails:
        f()


def mlp_bwd(d_out, zs, rows, wup, wdn, fill):
    FF = wdn.shape[0]
    total = []

    def chunk(i):
        cols = slice(i * QW, (i + 1) * QW)

        def use(v):
            zs[1][rows, cols] = gelu_bwd(zs[0](cols), v.astype(BF))
        return (lambda: mm_nt(d_out, wdn[cols, :])), use

    def part(j):
        cols = slice(j * UNIT, (j + 1) * UNIT)

        def run():
            v = mm_nt(zs[1][rows, cols], wup[:, cols])
            total[:] = [v if not total else total[0] + v]
        return run

    fill = {i: list(f) for i, f in fill.items()}
    for j in range(FF // UNIT):
        fill.setdefault(2 * j + 1, []).append(part(j))
    weave([chunk(i) for i in range(FF // QW)], fill)
    return total[0].astype(BF)


def step_kernel(cfg, x_ref, g_ref, emb_ref, wq_h, wk_h, wv_h, wo_ref, wup_ref, wdn_ref,
                acc_h, qkv0_h, u0_h, mix0_h, z0_h, mT0_h, h0_h, dout0_h,
                xs, us, qkv, st, stat, mixT, hs, mT, zs, gs, dmid, dout, dcur, wqkvT, pb, db, acc, sem, wsem, ssem):
    S, D, FF, HW, L = cfg
    NQ = D // QW
    NS = QW // HW
    scale = HW ** -0.5
    step = pl.program_id(0)
    last = pl.num_programs(0) - 1
    n_ff = FF // UNIT

    @pl.when(step == 0)
    def _():
        loads = [pltpu.make_async_copy(w, wqkvT.at[j * D:(j + 1) * D], wsem.at[j]) for j, w in enumerate((wq_h, wk_h, wv_h))]
        for cp in loads:
            cp.start()
        acc[...] = jnp.zeros_like(acc)
        for cp in loads:
            cp.wait()

    emb = emb_ref[...].astype(F32)
    xs[0] = x_ref[0] + emb[0:1].astype(BF)

    def fwd(l, carry):
        rows = pl.ds(pl.multiple_of(l * S, S), S)
        x = xs[l]
        xf = x.astype(F32)
        u = (xf * rms_scale(xf)).astype(BF)
        us[rows, :] = u
        def proj(part, c):
            cols = slice(part * D + c * QW, part * D + (c + 1) * QW)

            def run():
                qkv[rows, cols] = mm_nt(u, wqkvT[cols, :]).astype(BF)
            return run

        def quad(c):
            k4 = qkv[rows, D + c * QW:D + (c + 1) * QW]
            qm = head_stack(qkv[rows, c * QW:(c + 1) * QW], HW)

            def chunk(i):
                cols = slice(i * QW, (i + 1) * QW)

                def use(v):
                    sb = v.astype(BF)
                    st[l, c, :, cols] = sb
                    m, e, inv = soft_stats(sb, scale)
                    stat[l, c, 0:1, cols] = m
                    stat[l, c, 1:2, cols] = inv
                    pb[c, :, cols] = (e * inv).astype(BF)
                return (lambda: mm_nt(k4, qm[cols])), use
            return [chunk(i) for i in range(NS * S // QW)]

        def head_out(c, h):
            def run():
                vT = qkv[rows, 2 * D + c * QW:2 * D + (c + 1) * QW].T
                o = mm(vT[h * HW:(h + 1) * HW], pb[c, :, h * S:(h + 1) * S])
                mixT[c * QW + h * HW:c * QW + (h + 1) * HW, rows] = o.astype(BF)
            return run

        for part in range(3):
            proj(part, 0)()
        weave(quad(0), {0: [proj(0, 1)], 1: [proj(1, 1)], 2: [proj(2, 1)], 3: [head_out(0, 0)], 4: [head_out(0, 1)]})
        weave(quad(1), {0: [head_out(0, 2)], 1: [head_out(0, 3)], 3: [head_out(1, 0)], 4: [head_out(1, 1)]})
        head_out(1, 2)()
        head_out(1, 3)()
        h_mid = x + mm_tn(mixT[:, rows], wo_ref[...]).astype(BF)
        hs[l] = h_mid
        hf = h_mid.astype(F32)
        mn = (hf * rms_scale(hf)).astype(BF)
        mT[:, rows] = mn.T
        down = []

        def up_chunk(i):
            cols = slice(i * QW, (i + 1) * QW)

            def use(v):
                z = v.astype(BF)
                zs[rows, cols] = z
                gs[rows, cols] = gelu_fwd(z)
            return (lambda: mm(mn, wup_ref[:, cols])), use

        def down_part(j):
            cols = slice(j * UNIT, (j + 1) * UNIT)

            def run():
                v = mm(gs[rows, cols], wdn_ref[cols, :])
                down[:] = [v if not down else down[0] + v]
            return run

        weave([up_chunk(i) for i in range(FF // QW)], {2 * j + 1: [down_part(j)] for j in range(n_ff)})
        y = down[0]
        nxt = emb[1:2]
        for j in range(2, L):
            nxt = jnp.where(l + 1 == j, emb[j:j + 1], nxt)
        xs[l + 1] = (h_mid + y.astype(BF)) + nxt.astype(BF)
        return carry

    lax.fori_loop(0, L, fwd, 0)
    dcur[...] = g_ref[0]
    saves = [pltpu.make_async_copy(src, dst.at[step], ssem.at[n]) for n, (src, dst) in enumerate((
        (qkv.at[0:S], qkv0_h), (us.at[0:S], u0_h), (mixT.at[:, 0:S], mix0_h), (zs.at[0:S], z0_h),
        (mT.at[:, 0:S], mT0_h), (hs.at[0], h0_h), (dout.at[0:S], dout0_h)))]
    for cp in saves[:-1]:
        cp.start()

    def bwd(i, carry):
        l = L - 1 - i
        rows = pl.ds(pl.multiple_of(l * S, S), S)
        d_out = dcur[...]
        dout[rows, :] = d_out
        def add_unit(k, make):
            def run():
                acc[k] = acc[k] + make()
            return run

        ucol = lambda j: slice(j * UNIT, (j + 1) * UNIT)
        dn_unit = lambda j: add_unit(j, lambda: mm_tn(gs[rows, ucol(j)], d_out))
        up_unit = lambda j: add_unit(4 + j, lambda: mm(mT[:, rows], zs[rows, ucol(j)]))
        o_unit = add_unit(11, lambda: mm(mixT[:, rows], dmid[rows, :]))
        d_norm = mlp_bwd(d_out, (lambda cols: zs[rows, cols], zs), rows, wup_ref, wdn_ref, {2 * j: [dn_unit(j)] for j in range(n_ff)})
        d_mid = d_out + rms_bwd(hs[l], d_norm)
        dmid[rows, :] = d_mid
        d_mix = mm_nt(d_mid, wo_ref[...]).astype(BF)

        def prob(c, cols, unused):
            s = st[l, c, :, cols].astype(F32)
            return jnp.exp2((s - stat[l, c, 0:1, cols]) * (scale * LOG2E)) * stat[l, c, 1:2, cols]

        prob.recompute = False
        attn_bwd(qkv, rows, d_mix, HW, prob, pb, db, ({0: [up_unit(0)], 2: [up_unit(1)], 3: [up_unit(2)], 4: [up_unit(3)]}, {4: [o_unit]}))
        d_norm_x = mm(qkv[rows, :], wqkvT[...]).astype(BF)
        for j in range(3):
            acc[8 + j] = acc[8 + j] + mm_tn(qkv[rows, j * UNIT:(j + 1) * UNIT], us[rows, :])
        dcur[...] = d_mid + rms_bwd(xs[l], d_norm_x)
        return carry

    lax.fori_loop(0, L - 1, bwd, 0)
    dout[0:S, :] = dcur[...]
    saves[-1].start()

    @pl.when(step == last)
    def _():
        for k in range(4, 12):
            pltpu.make_async_copy(acc.at[k], acc_h.at[k], sem.at[k]).start()

    for j in range(n_ff):
        acc[j] = acc[j] + mm_tn(gs[0:S, j * UNIT:(j + 1) * UNIT], dout[0:S, :])
    for cp in saves:
        cp.wait()

    @pl.when(step == last)
    def _():
        for k in range(4):
            pltpu.make_async_copy(acc.at[k], acc_h.at[k], sem.at[k]).start()
        for k in range(12):
            pltpu.make_async_copy(acc.at[k], acc_h.at[k], sem.at[k]).wait()


def reduce_kernel(cfg, emb_ref, wo_ref, x_h, qkv_h, u_h, mix_h, z_h, mT_h, h_h, dout_h, wq_h, wk_h, wv_h, wup_h, wdn_h, acc_h,
                  dx_ref, r_dn, r_up, r_q, r_k, r_v, r_o,
                  xb, qkvb, ub, mixb, zb, mTb, hb, doutb,
                  wqkvT, wup, wdn, dup, dmid, pb, db, acc2, aw, r1, r2, r3, send, recv, lsem, wsem, isem):
    B, S, D, FF, HW = cfg
    NQ = D // QW
    n_ff = FF // UNIT
    scale = HW ** -0.5
    me = lax.axis_index('data')
    core = lax.rem(me, 2)
    bit_x = lax.rem(me // 2, 2)
    bit_y = me // 4
    core_peer = me + 1 - 2 * core
    x_peer = me + 2 - 4 * bit_x
    y_peer = me + 4 - 8 * bit_y
    half = UNIT // 2
    N_EARLY = n_ff
    N_ALL = 12

    def order(k):
        if k % 2 == 0:
            return (bit_x, x_peer), (bit_y, y_peer)
        return (bit_y, y_peer), (bit_x, x_peer)

    def aligned(v, n):
        return pl.ds(pl.multiple_of(v, n), n)

    def part(k, start, n):
        if k < N_EARLY:
            return aw.at[k, aligned(start, n)]
        return acc2.at[k - N_EARLY, aligned(core * half + start, n)]

    def remote(stage, k, src, dst, peer):
        return pltpu.make_async_remote_copy(src_ref=src, dst_ref=dst, send_sem=send.at[stage, k], recv_sem=recv.at[stage, k], device_id=(peer,), device_id_type=MESH)

    def copy_of(stage, k):
        (b1, p1), (b2, p2) = order(k)
        if stage == 0:
            rows = aligned((1 - core) * half, half)
            src = acc_h.at[k, rows] if k < N_EARLY else acc2.at[k - N_EARLY, rows]
            return remote(0, k, src, r1.at[k], core_peer)
        if stage == 1:
            return remote(1, k, part(k, (1 - b1) * 128, 128), r2.at[k], p1)
        if stage == 2:
            return remote(2, k, part(k, b1 * 128 + (1 - b2) * 64, 64), r3.at[k], p2)
        if stage == 3:
            mine = res_at(k, b1 * 128 + b2 * 64, 64)
            return remote(3, k, mine, mine, p2)
        if stage == 4:
            mine = res_at(k, b1 * 128, 128)
            return remote(4, k, mine, mine, p1)
        mine = res_at(k, 0, half)
        return remote(5, k, mine, mine, core_peer)

    def res_at(k, start, n):
        if k < 4:
            return r_dn.at[aligned(k * UNIT + core * half + start, n)]
        rows = aligned(core * half + start, n)
        if k < 8:
            return r_up.at[rows, (k - 4) * UNIT:(k - 3) * UNIT]
        return (r_q, r_k, r_v, r_o)[k - 8].at[rows]

    def own_load(k):
        return pltpu.make_async_copy(acc_h.at[k, aligned(core * half, half)], aw.at[k], lsem.at[k])

    def late_load(k):
        return pltpu.make_async_copy(acc_h.at[k], acc2.at[k - N_EARLY], lsem.at[k])

    def serve(stage, k):
        (b1, _), (b2, _) = order(k)
        copy_of(stage, k).wait_recv()
        if stage == 0:
            if k < N_EARLY:
                own_load(k).wait()
            ref = part(k, 0, half)
            ref[...] = ref[...] + r1[k]
        elif stage == 1:
            ref = part(k, b1 * 128, 128)
            ref[...] = ref[...] + r2[k]
        elif stage == 2:
            ref = part(k, b1 * 128 + b2 * 64, 64)
            res_at(k, b1 * 128 + b2 * 64, 64)[...] = ref[...] + r3[k]
        if stage < 5:
            copy_of(stage + 1, k).start()

    def serve_all(stage, units):
        for k in units:
            serve(stage, k)

    def begin(units):
        for k in units:
            copy_of(0, k).start()

    def fetch(phase, i):
        slot = lax.rem(i, 2)
        pairs = ((mix_h, mixb), (z_h, zb), (mT_h, mTb), (h_h, hb), (dout_h, doutb)) if phase == 0 else ((x_h, xb), (qkv_h, qkvb), (u_h, ub))
        return [pltpu.make_async_copy(s_.at[i], d_.at[slot], isem.at[phase * 5 + n, slot]) for n, (s_, d_) in enumerate(pairs)]

    def arrive(phase, i):
        for cp in fetch(phase, i):
            cp.wait()

        @pl.when(i + 1 < B)
        def _():
            for cp in fetch(phase, i + 1):
                cp.start()
        return lax.rem(i, 2)

    def w_loads():
        pairs = [(wdn_h, wdn), (wup_h, wup)] + [(w, wqkvT.at[j * D:(j + 1) * D]) for j, w in enumerate((wq_h, wk_h, wv_h))]
        return [pltpu.make_async_copy(s_, d_, wsem.at[j]) for j, (s_, d_) in enumerate(pairs)]

    barrier = pltpu.get_barrier_semaphore()
    for peer in (core_peer, x_peer, y_peer):
        pl.semaphore_signal(barrier, inc=1, device_id=(peer,), device_id_type=MESH)
    for k in range(N_EARLY):
        own_load(k).start()
    for cp in fetch(0, 0):
        cp.start()
    for cp in w_loads():
        cp.start()
    pl.semaphore_wait(barrier, 3)
    begin(range(N_EARLY))
    for k in range(N_EARLY, N_ALL):
        late_load(k).start()
    serve_all(0, range(N_EARLY))
    for cp in w_loads():
        cp.wait()
    for k in range(N_EARLY, N_ALL):
        late_load(k).wait()

    def run_events(events):
        for stage, unit in zip(events[::2], events[1::2]):
            serve(int(stage), int(unit, 16))

    def at_step(step, i, events, before=''):
        @pl.when(step == i)
        def _():
            begin([int(unit, 16) for unit in before])
            run_events(events)

    def phase1(step, carry):
        slot = arrive(0, step)
        d_out = doutb[slot]

        def up_unit(j):
            def run():
                acc2[j] = acc2[j] + mm(mTb[slot], dup[:, j * UNIT:(j + 1) * UNIT])
            return run

        d_norm = mlp_bwd(d_out, (lambda cols: zb[slot, :, cols], dup), slice(0, S), wup, wdn, {2: [up_unit(0)], 4: [up_unit(1)], 6: [up_unit(2)]})
        d_mid = d_out + rms_bwd(hb[slot], d_norm)
        dmid[step] = d_mid
        up_unit(3)()
        acc2[7] = acc2[7] + mm(mixb[slot], d_mid)

        at_step(step, 1, '1110')
        at_step(step, 2, '122113')
        at_step(step, 3, '222031')
        at_step(step, 4, '3223')
        at_step(step, 5, '060b040705414230', before='6b475')
        return carry

    for cp in fetch(1, 0):
        cp.start()
    lax.fori_loop(0, B, phase1, 0)

    def phase2(step, carry):
        slot = arrive(1, step)
        d_mid = dmid[step]
        d_mix = mm_nt(d_mid, wo_ref[...]).astype(BF)
        dqkv = qkvb.at[slot]

        def prob(c, cols, scores):
            m, e, inv = soft_stats(scores.astype(BF), scale)
            return e * inv

        prob.recompute = True
        attn_bwd(dqkv, slice(0, S), d_mix, HW, prob, pb, db, ({}, {}))
        d_norm_x = mm(dqkv[...], wqkvT[...]).astype(BF)
        x = xb[slot] + emb_ref[0:1, :]
        dx_ref[step] = d_mid + rms_bwd(x, d_norm_x)
        for j in range(3):
            acc2[4 + j] = acc2[4 + j] + mm_tn(dqkv[:, j * UNIT:(j + 1) * UNIT], ub[slot])

        at_step(step, 0, '161b335152')
        at_step(step, 1, '1417')
        at_step(step, 2, '15262b2740')
        at_step(step, 3, '2425363b4350')
        at_step(step, 4, '34353753')
        return carry

    lax.fori_loop(0, B, phase2, 0)

    begin([8, 9, 10])
    run_events('08090a464b444556475b54555718')
    run_events('19281a29382a393a4858494a595a')
    for k in range(N_ALL):
        for stage in range(6):
            copy_of(stage, k).wait_send()


def store_kernel(*refs):
    n = len(refs) // 2
    copies = [pltpu.make_async_copy(refs[i], refs[n + i], refs[-1].at[i]) for i in range(n)]
    for cp in copies:
        cp.start()
    for cp in copies:
        cp.wait()


def solution(mesh):
    batch_spec = P('data', None, None)

    def per_device(x, g, emb, w_q, w_k, w_v, w_o, wup, wdn):
        D, H, HW = w_q.shape
        B, S, _ = x.shape
        FF = wup.shape[1]
        L = emb.shape[0]
        T = L * S
        NQ = D // QW
        NS = QW // HW
        w_t = [w.transpose(1, 2, 0).reshape(D, D) for w in (w_q, w_k, w_v)]
        wo = w_o.reshape(D, D)
        const = lambda shape: pl.BlockSpec(shape, lambda b: (0,) * len(shape), pipeline_mode=pl.Buffered(1))
        per_seq = lambda cols: pl.BlockSpec((1, S, cols), lambda b: (b, 0, 0))
        col_seq = pl.BlockSpec((D, S), lambda b: (0, b))
        hbm = pl.BlockSpec(memory_space=pl.ANY)
        sds = jax.ShapeDtypeStruct
        saved = [sds((B, S, 3 * D), BF), sds((B, S, D), BF), sds((B, D, S), BF), sds((B, S, FF), BF), sds((B, D, S), BF), sds((B, S, D), BF), sds((B, S, D), BF)]
        acc, qkv0, u0, mix0, z0, mT0, h0, dout0 = pl.pallas_call(
            functools.partial(step_kernel, (S, D, FF, HW, L)),
            name='block_grads',
            grid=(B,),
            in_specs=[per_seq(D), per_seq(D), const(emb.shape), hbm, hbm, hbm, const(wo.shape), const(wup.shape), const(wdn.shape)],
            out_specs=[hbm] * 8,
            out_shape=[sds((12, UNIT, UNIT), F32)] + saved,
            scratch_shapes=[
                pltpu.VMEM((L + 1, S, D), BF),
                pltpu.VMEM((T, D), BF),
                pltpu.VMEM((T, 3 * D), BF),
                pltpu.VMEM((L, NQ, S, NS * S), BF),
                pltpu.VMEM((L, NQ, 8, NS * S), F32),
                pltpu.VMEM((D, T), BF),
                pltpu.VMEM((L, S, D), BF),
                pltpu.VMEM((D, T), BF),
                pltpu.VMEM((T, FF), BF),
                pltpu.VMEM((T, FF), BF),
                pltpu.VMEM((T, D), BF),
                pltpu.VMEM((T, D), BF),
                pltpu.VMEM((S, D), BF),
                pltpu.VMEM((3 * D, D), BF),
                pltpu.VMEM((NQ, S, NS * S), BF),
                pltpu.VMEM((NQ, S, NS * S), BF),
                pltpu.VMEM((12, UNIT, UNIT), F32),
                pltpu.SemaphoreType.DMA((12,)),
                pltpu.SemaphoreType.DMA((3,)),
                pltpu.SemaphoreType.DMA((7,)),
            ],
            compiler_params=pltpu.CompilerParams(dimension_semantics=('arbitrary',), vmem_limit_bytes=VMEM_MAX),
        )(x, g, emb, *w_t, wo, wup, wdn)
        vmem = pl.BlockSpec(memory_space=pltpu.VMEM)
        outs = pl.pallas_call(
            functools.partial(reduce_kernel, (B, S, D, FF, HW)),
            name='attn_reduce',
            in_specs=[vmem, vmem] + [hbm] * 14,
            out_specs=[vmem] * 7,
            out_shape=[pltpu.VMEM(x.shape, BF), pltpu.VMEM((FF, D), F32), pltpu.VMEM((D, FF), F32)] + [pltpu.VMEM((D, D), F32)] * 4,
            scratch_shapes=[
                pltpu.VMEM((2, S, D), BF),
                pltpu.VMEM((2, S, 3 * D), BF),
                pltpu.VMEM((2, S, D), BF),
                pltpu.VMEM((2, D, S), BF),
                pltpu.VMEM((2, S, FF), BF),
                pltpu.VMEM((2, D, S), BF),
                pltpu.VMEM((2, S, D), BF),
                pltpu.VMEM((2, S, D), BF),
                pltpu.VMEM((3 * D, D), BF),
                pltpu.VMEM((D, FF), BF),
                pltpu.VMEM((FF, D), BF),
                pltpu.VMEM((S, FF), BF),
                pltpu.VMEM((B, S, D), BF),
                pltpu.VMEM((NQ, S, NS * S), BF),
                pltpu.VMEM((NQ, S, NS * S), BF),
                pltpu.VMEM((8, UNIT, UNIT), F32),
                pltpu.VMEM((4, UNIT // 2, UNIT), F32),
                pltpu.VMEM((12, UNIT // 2, UNIT), F32),
                pltpu.VMEM((12, 128, UNIT), F32),
                pltpu.VMEM((12, 64, UNIT), F32),
                pltpu.SemaphoreType.DMA((6, 12)),
                pltpu.SemaphoreType.DMA((6, 12)),
                pltpu.SemaphoreType.DMA((12,)),
                pltpu.SemaphoreType.DMA((5,)),
                pltpu.SemaphoreType.DMA((8, 2)),
            ],
            compiler_params=pltpu.CompilerParams(vmem_limit_bytes=VMEM_MAX - (16 << 20), collective_id=0, has_side_effects=True),
        )(emb, wo, x, qkv0, u0, mix0, z0, mT0, h0, dout0, *w_t, wup, wdn, acc)
        d_x, dn, up, gq, gk, gv, go = pl.pallas_call(
            store_kernel,
            name='store',
            in_specs=[vmem] * 7,
            out_specs=[hbm] * 7,
            out_shape=[sds(o.shape, o.dtype) for o in outs],
            scratch_shapes=[pltpu.SemaphoreType.DMA((7,))],
            compiler_params=pltpu.CompilerParams(vmem_limit_bytes=1 << 20),
        )(*outs)
        back = lambda a: a.reshape(H, HW, D).transpose(2, 0, 1)
        return back(gq), back(gk), back(gv), go.reshape(H, HW, D), up, dn, d_x

    return jax.shard_map(per_device, mesh=mesh, in_specs=(batch_spec, batch_spec, P(), P(), P(), P(), P(), P(), P()), out_specs=(P(), P(), P(), P(), P(), P(), batch_spec), check_vma=False)
```

```python
import functools

import jax
import jax.numpy as jnp
from jax import lax
from jax.experimental import pallas as pl
from jax.experimental.pallas import tpu as pltpu
from jax.sharding import PartitionSpec as P

NORM_EPS = 1e-6
BF = jnp.bfloat16
F32 = jnp.float32
GELU_C = 0.7978845608028654
GELU_A = 0.044715
LOG2E = 1.4426950408889634
MESH = pl.DeviceIdType.MESH
UNIT = 512
QW = 256
VMEM_MAX = 67043328


def mm(a, b):
    return lax.dot_general(a, b, (((1,), (0,)), ((), ())), preferred_element_type=F32)


def mm_nt(a, b):
    return lax.dot_general(a, b, (((1,), (1,)), ((), ())), preferred_element_type=F32)


def mm_tn(a, b):
    return lax.dot_general(a, b, (((0,), (0,)), ((), ())), preferred_element_type=F32)


def rms_scale(xf):
    return lax.rsqrt(jnp.mean(xf * xf, axis=-1, keepdims=True) + NORM_EPS)


def rms_bwd(x, dy):
    xf = x.astype(F32)
    gf = dy.astype(F32)
    r = rms_scale(xf)
    dot = jnp.mean(xf * gf, axis=-1, keepdims=True)
    return (gf * r - xf * (r * r * r * dot)).astype(BF)


def gelu_fwd(z):
    zf = z.astype(F32)
    t = jnp.tanh(zf * (GELU_C + (GELU_C * GELU_A) * (zf * zf)))
    half = 0.5 * zf
    return (half + half * t).astype(BF)


def gelu_bwd(z, dg):
    zf = z.astype(F32)
    z2 = zf * zf
    t = jnp.tanh(zf * (GELU_C + (GELU_C * GELU_A) * z2))
    slope = (0.5 + 0.5 * t) + ((1.0 - t * t) * zf) * ((0.5 * GELU_C) + (1.5 * GELU_C * GELU_A) * z2)
    return (dg.astype(F32) * slope).astype(BF)


def head_stack(a4, width):
    lane = lax.broadcasted_iota(jnp.int32, a4.shape, 1)
    zero = jnp.zeros_like(a4)
    n_sub = a4.shape[1] // width
    return jnp.concatenate([jnp.where((lane >= h * width) & (lane < (h + 1) * width), a4, zero) for h in range(n_sub)], axis=0)


def soft_stats(sb, scale):
    m = jnp.max(sb, axis=0, keepdims=True).astype(F32)
    e = jnp.exp2((sb.astype(F32) - m) * (scale * LOG2E))
    inv = 1.0 / jnp.sum(e, axis=0, keepdims=True)
    return m, e, inv


def weave(chunks, fill):
    ahead = chunks[0][0]()
    for i, (_, use) in enumerate(chunks):
        now = ahead
        if i + 1 < len(chunks):
            ahead = chunks[i + 1][0]()
        use(now)
        for f in fill.get(i, ()):
            f()


def attn_bwd(qkv, rows, d_mix, HW, prob, pb, db, fills):
    S, D = d_mix.shape
    ns = QW // HW
    scale = HW ** -0.5
    width = ns * S
    tails = []
    for c in range(D // QW):
        qc = slice(c * QW, (c + 1) * QW)
        kc = slice(D + c * QW, D + (c + 1) * QW)
        vc = slice(2 * D + c * QW, 2 * D + (c + 1) * QW)
        k4 = qkv[rows, kc]
        v4 = qkv[rows, vc]
        qm = head_stack(qkv[rows, qc], HW)
        dom = head_stack(d_mix[:, qc], HW)
        kT = k4.T

        def chunk(i, c=c, k4=k4, v4=v4, qm=qm, dom=dom):
            cols = slice(i * QW, (i + 1) * QW)

            def use(vals):
                p = prob(c, cols, vals[1])
                dp = vals[0].astype(BF).astype(F32)
                delta = jnp.sum(dp * p, axis=0, keepdims=True)
                pb[c, :, cols] = p.astype(BF)
                db[c, :, cols] = ((p * (dp - delta)) * scale).astype(BF)
            return (lambda: (mm_nt(v4, dom[cols]), mm_nt(k4, qm[cols]) if prob.recompute else None)), use

        fill = {i: list(f) for i, f in fills[c].items()}
        for i, f in enumerate(tails):
            fill.setdefault(i, []).insert(0, f)

        def tail_v(c=c, vc=vc, dom=dom):
            qkv[rows, vc] = mm(pb[c], dom).astype(BF)

        def tail_k(c=c, kc=kc, qm=qm):
            qkv[rows, kc] = mm(db[c], qm).astype(BF)

        def tail_q(c=c, qc=qc, kT=kT):
            dqT = [mm(kT[h * HW:(h + 1) * HW], db[c, :, h * S:(h + 1) * S]).astype(BF) for h in range(ns)]
            qkv[rows, qc] = jnp.concatenate(dqT, axis=0).T

        weave([chunk(i) for i in range(width // QW)], fill)
        tails = [tail_v, tail_k, tail_q]
    for f in tails:
        f()


def mlp_bwd(d_out, zs, rows, wup, wdn, fill):
    FF = wdn.shape[0]
    total = []

    def chunk(i):
        cols = slice(i * QW, (i + 1) * QW)

        def use(v):
            zs[1][rows, cols] = gelu_bwd(zs[0](cols), v.astype(BF))
        return (lambda: mm_nt(d_out, wdn[cols, :])), use

    def part(j):
        cols = slice(j * UNIT, (j + 1) * UNIT)

        def run():
            v = mm_nt(zs[1][rows, cols], wup[:, cols])
            total[:] = [v if not total else total[0] + v]
        return run

    fill = {i: list(f) for i, f in fill.items()}
    for j in range(FF // UNIT):
        fill.setdefault(2 * j + 1, []).append(part(j))
    weave([chunk(i) for i in range(FF // QW)], fill)
    return total[0].astype(BF)


def step_kernel(cfg, x_ref, g_ref, emb_ref, wq_h, wk_h, wv_h, wo_ref, wup_ref, wdn_ref,
                acc_h, qkv0_h, u0_h, mix0_h, z0_h, mT0_h, h0_h, dout0_h,
                xs, us, qkv, st, stat, mixT, hs, mT, zs, gs, dmid, dout, dcur, wqkvT, pb, db, acc, sem, wsem, ssem):
    S, D, FF, HW, L = cfg
    NQ = D // QW
    NS = QW // HW
    scale = HW ** -0.5
    step = pl.program_id(0)
    last = pl.num_programs(0) - 1
    n_ff = FF // UNIT

    @pl.when(step == 0)
    def _():
        loads = [pltpu.make_async_copy(w, wqkvT.at[j * D:(j + 1) * D], wsem.at[j]) for j, w in enumerate((wq_h, wk_h, wv_h))]
        for cp in loads:
            cp.start()
        acc[...] = jnp.zeros_like(acc)
        for cp in loads:
            cp.wait()

    emb = emb_ref[...].astype(F32)
    xs[0] = x_ref[0] + emb[0:1].astype(BF)

    def fwd(l, carry):
        rows = pl.ds(pl.multiple_of(l * S, S), S)
        x = xs[l]
        xf = x.astype(F32)
        u = (xf * rms_scale(xf)).astype(BF)
        us[rows, :] = u
        def proj(part, c):
            cols = slice(part * D + c * QW, part * D + (c + 1) * QW)

            def run():
                qkv[rows, cols] = mm_nt(u, wqkvT[cols, :]).astype(BF)
            return run

        def quad(c):
            k4 = qkv[rows, D + c * QW:D + (c + 1) * QW]
            qm = head_stack(qkv[rows, c * QW:(c + 1) * QW], HW)

            def chunk(i):
                cols = slice(i * QW, (i + 1) * QW)

                def use(v):
                    sb = v.astype(BF)
                    st[l, c, :, cols] = sb
                    m, e, inv = soft_stats(sb, scale)
                    stat[l, c, 0:1, cols] = m
                    stat[l, c, 1:2, cols] = inv
                    pb[c, :, cols] = (e * inv).astype(BF)
                return (lambda: mm_nt(k4, qm[cols])), use
            return [chunk(i) for i in range(NS * S // QW)]

        def head_out(c, h):
            def run():
                vT = qkv[rows, 2 * D + c * QW:2 * D + (c + 1) * QW].T
                o = mm(vT[h * HW:(h + 1) * HW], pb[c, :, h * S:(h + 1) * S])
                mixT[c * QW + h * HW:c * QW + (h + 1) * HW, rows] = o.astype(BF)
            return run

        for part in range(3):
            proj(part, 0)()
        weave(quad(0), {0: [proj(0, 1)], 1: [proj(1, 1)], 2: [proj(2, 1)], 3: [head_out(0, 0)], 4: [head_out(0, 1)]})
        weave(quad(1), {0: [head_out(0, 2)], 1: [head_out(0, 3)], 3: [head_out(1, 0)], 4: [head_out(1, 1)]})
        head_out(1, 2)()
        head_out(1, 3)()
        h_mid = x + mm_tn(mixT[:, rows], wo_ref[...]).astype(BF)
        hs[l] = h_mid
        hf = h_mid.astype(F32)
        mn = (hf * rms_scale(hf)).astype(BF)
        mT[:, rows] = mn.T
        down = []

        def up_chunk(i):
            cols = slice(i * QW, (i + 1) * QW)

            def use(v):
                z = v.astype(BF)
                zs[rows, cols] = z
                gs[rows, cols] = gelu_fwd(z)
            return (lambda: mm(mn, wup_ref[:, cols])), use

        def down_part(j):
            cols = slice(j * UNIT, (j + 1) * UNIT)

            def run():
                v = mm(gs[rows, cols], wdn_ref[cols, :])
                down[:] = [v if not down else down[0] + v]
            return run

        weave([up_chunk(i) for i in range(FF // QW)], {2 * j + 1: [down_part(j)] for j in range(n_ff)})
        y = down[0]
        nxt = emb[1:2]
        for j in range(2, L):
            nxt = jnp.where(l + 1 == j, emb[j:j + 1], nxt)
        xs[l + 1] = (h_mid + y.astype(BF)) + nxt.astype(BF)
        return carry

    lax.fori_loop(0, L, fwd, 0)
    dcur[...] = g_ref[0]
    saves = [pltpu.make_async_copy(src, dst.at[step], ssem.at[n]) for n, (src, dst) in enumerate((
        (qkv.at[0:S], qkv0_h), (us.at[0:S], u0_h), (mixT.at[:, 0:S], mix0_h), (zs.at[0:S], z0_h),
        (mT.at[:, 0:S], mT0_h), (hs.at[0], h0_h), (dout.at[0:S], dout0_h)))]
    for cp in saves[:-1]:
        cp.start()

    def bwd(i, carry):
        l = L - 1 - i
        rows = pl.ds(pl.multiple_of(l * S, S), S)
        d_out = dcur[...]
        dout[rows, :] = d_out
        def add_unit(k, make):
            def run():
                acc[k] = acc[k] + make()
            return run

        ucol = lambda j: slice(j * UNIT, (j + 1) * UNIT)
        dn_unit = lambda j: add_unit(j, lambda: mm_tn(gs[rows, ucol(j)], d_out))
        up_unit = lambda j: add_unit(4 + j, lambda: mm(mT[:, rows], zs[rows, ucol(j)]))
        o_unit = add_unit(11, lambda: mm(mixT[:, rows], dmid[rows, :]))
        d_norm = mlp_bwd(d_out, (lambda cols: zs[rows, cols], zs), rows, wup_ref, wdn_ref, {2 * j: [dn_unit(j)] for j in range(n_ff)})
        d_mid = d_out + rms_bwd(hs[l], d_norm)
        dmid[rows, :] = d_mid
        d_mix = mm_nt(d_mid, wo_ref[...]).astype(BF)

        def prob(c, cols, unused):
            s = st[l, c, :, cols].astype(F32)
            return jnp.exp2((s - stat[l, c, 0:1, cols]) * (scale * LOG2E)) * stat[l, c, 1:2, cols]

        prob.recompute = False
        attn_bwd(qkv, rows, d_mix, HW, prob, pb, db, ({0: [up_unit(0)], 2: [up_unit(1)], 3: [up_unit(2)], 4: [up_unit(3)]}, {4: [o_unit]}))
        d_norm_x = mm(qkv[rows, :], wqkvT[...]).astype(BF)
        for j in range(3):
            acc[8 + j] = acc[8 + j] + mm_tn(qkv[rows, j * UNIT:(j + 1) * UNIT], us[rows, :])
        dcur[...] = d_mid + rms_bwd(xs[l], d_norm_x)
        return carry

    lax.fori_loop(0, L - 1, bwd, 0)
    dout[0:S, :] = dcur[...]
    saves[-1].start()

    @pl.when(step == last)
    def _():
        for k in range(4, 12):
            pltpu.make_async_copy(acc.at[k], acc_h.at[k], sem.at[k]).start()

    for j in range(n_ff):
        acc[j] = acc[j] + mm_tn(gs[0:S, j * UNIT:(j + 1) * UNIT], dout[0:S, :])
    for cp in saves:
        cp.wait()

    @pl.when(step == last)
    def _():
        for k in range(4):
            pltpu.make_async_copy(acc.at[k], acc_h.at[k], sem.at[k]).start()
        for k in range(12):
            pltpu.make_async_copy(acc.at[k], acc_h.at[k], sem.at[k]).wait()


def reduce_kernel(cfg, emb_ref, wo_ref, x_h, qkv_h, u_h, mix_h, z_h, mT_h, h_h, dout_h, wq_h, wk_h, wv_h, wup_h, wdn_h, acc_h,
                  dx_ref, r_dn, r_up, r_q, r_k, r_v, r_o,
                  xb, qkvb, ub, mixb, zb, mTb, hb, doutb,
                  wqkvT, wup, wdn, dup, dmid, pb, db, acc2, aw, r1, r2, r3, send, recv, lsem, wsem, isem):
    B, S, D, FF, HW = cfg
    NQ = D // QW
    n_ff = FF // UNIT
    scale = HW ** -0.5
    me = lax.axis_index('data')
    core = lax.rem(me, 2)
    bit_x = lax.rem(me // 2, 2)
    bit_y = me // 4
    core_peer = me + 1 - 2 * core
    x_peer = me + 2 - 4 * bit_x
    y_peer = me + 4 - 8 * bit_y
    SUB = UNIT // 2
    KEEP = SUB // 2
    N_EARLY = 2 * n_ff
    N_ALL = 24

    def order(u):
        if u % 2 == 0:
            return (bit_x, x_peer), (bit_y, y_peer)
        return (bit_y, y_peer), (bit_x, x_peer)

    def aligned(v, n):
        return pl.ds(pl.multiple_of(v, n), n)

    def part(u, start, n):
        if u < N_EARLY:
            return aw.at[u, aligned(start, n)]
        return acc2.at[u // 2 - n_ff, aligned(u % 2 * SUB + core * KEEP + start, n)]

    def remote(stage, u, src, dst, peer):
        return pltpu.make_async_remote_copy(src_ref=src, dst_ref=dst, send_sem=send.at[stage, u], recv_sem=recv.at[stage, u], device_id=(peer,), device_id_type=MESH)

    def copy_of(stage, u):
        (b1, p1), (b2, p2) = order(u)
        if stage == 0:
            rows = aligned(u % 2 * SUB + (1 - core) * KEEP, KEEP)
            src = acc_h.at[u // 2, rows] if u < N_EARLY else acc2.at[u // 2 - n_ff, rows]
            return remote(0, u, src, r1.at[u], core_peer)
        if stage == 1:
            return remote(1, u, part(u, (1 - b1) * 64, 64), r2.at[u], p1)
        if stage == 2:
            return remote(2, u, part(u, b1 * 64 + (1 - b2) * 32, 32), r3.at[u], p2)
        if stage == 3:
            mine = res_at(u, b1 * 64 + b2 * 32, 32)
            return remote(3, u, mine, mine, p2)
        if stage == 4:
            mine = res_at(u, b1 * 64, 64)
            return remote(4, u, mine, mine, p1)
        mine = res_at(u, 0, KEEP)
        return remote(5, u, mine, mine, core_peer)

    def res_at(u, start, n):
        k = u // 2
        row = u % 2 * SUB + core * KEEP + start
        if k < n_ff:
            return r_dn.at[aligned(k * UNIT + row, n)]
        if k < 8:
            return r_up.at[aligned(row, n), (k - 4) * UNIT:(k - 3) * UNIT]
        return (r_q, r_k, r_v, r_o)[k - 8].at[aligned(row, n)]

    def own_load(u):
        return pltpu.make_async_copy(acc_h.at[u // 2, aligned(u % 2 * SUB + core * KEEP, KEEP)], aw.at[u], lsem.at[u])

    def late_load(k):
        return pltpu.make_async_copy(acc_h.at[k], acc2.at[k - n_ff], lsem.at[n_ff + k])

    def serve(stage, u):
        (b1, _), (b2, _) = order(u)
        copy_of(stage, u).wait_recv()
        if stage == 0:
            if u < N_EARLY:
                own_load(u).wait()
            ref = part(u, 0, KEEP)
            ref[...] = ref[...] + r1[u]
        elif stage == 1:
            ref = part(u, b1 * 64, 64)
            ref[...] = ref[...] + r2[u]
        elif stage == 2:
            row = b1 * 64 + b2 * 32
            res_at(u, row, 32)[...] = part(u, row, 32)[...] + r3[u]
        if stage < 5:
            copy_of(stage + 1, u).start()

    def serve_all(stage, units):
        for u in units:
            serve(stage, u)

    def begin(units):
        for u in units:
            copy_of(0, u).start()

    def fetch(phase, i):
        slot = lax.rem(i, 2)
        pairs = ((mix_h, mixb), (z_h, zb), (mT_h, mTb), (h_h, hb), (dout_h, doutb)) if phase == 0 else ((x_h, xb), (qkv_h, qkvb), (u_h, ub))
        return [pltpu.make_async_copy(s_.at[i], d_.at[slot], isem.at[phase * 5 + n, slot]) for n, (s_, d_) in enumerate(pairs)]

    def arrive(phase, i):
        for cp in fetch(phase, i):
            cp.wait()

        @pl.when(i + 1 < B)
        def _():
            for cp in fetch(phase, i + 1):
                cp.start()
        return lax.rem(i, 2)

    def w_loads():
        pairs = [(wdn_h, wdn), (wup_h, wup)] + [(w, wqkvT.at[j * D:(j + 1) * D]) for j, w in enumerate((wq_h, wk_h, wv_h))]
        return [pltpu.make_async_copy(s_, d_, wsem.at[j]) for j, (s_, d_) in enumerate(pairs)]

    barrier = pltpu.get_barrier_semaphore()
    for peer in (core_peer, x_peer, y_peer):
        pl.semaphore_signal(barrier, inc=1, device_id=(peer,), device_id_type=MESH)
    for k in range(N_EARLY):
        own_load(k).start()
    for cp in fetch(0, 0):
        cp.start()
    for cp in w_loads():
        cp.start()
    pl.semaphore_wait(barrier, 3)
    begin(range(N_EARLY))
    for k in range(n_ff, 12):
        late_load(k).start()
    serve_all(0, range(N_EARLY))
    for cp in w_loads():
        cp.wait()
    for k in range(n_ff, 12):
        late_load(k).wait()

    def run_events(events):
        for stage, unit in zip(events[::2], events[1::2]):
            serve(int(stage), int(unit, 36))

    def at_step(step, i, events, before=''):
        @pl.when(step == i)
        def _():
            begin([int(unit, 36) for unit in before])
            run_events(events)

    def phase1(step, carry):
        slot = arrive(0, step)
        d_out = doutb[slot]

        def up_unit(j):
            def run():
                acc2[j] = acc2[j] + mm(mTb[slot], dup[:, j * UNIT:(j + 1) * UNIT])
            return run

        d_norm = mlp_bwd(d_out, (lambda cols: zb[slot, :, cols], dup), slice(0, S), wup, wdn, {2: [up_unit(0)], 4: [up_unit(1)], 6: [up_unit(2)]})
        d_mid = d_out + rms_bwd(hb[slot], d_norm)
        dmid[step] = d_mid
        up_unit(3)()
        acc2[7] = acc2[7] + mm(mixb[slot], d_mid)

        at_step(step, 0, '1110')
        at_step(step, 1, '12141315')
        at_step(step, 2, '172116232022')
        at_step(step, 3, '272425263130')
        at_step(step, 4, '373234333536')
        at_step(step, 5, '0n0e0m0b090c0a0d080f414742444340', before='nemb9cad8f')
        return carry

    for cp in fetch(1, 0):
        cp.start()
    lax.fori_loop(0, B, phase1, 0)

    def phase2(step, carry):
        slot = arrive(1, step)
        d_mid = dmid[step]
        d_mix = mm_nt(d_mid, wo_ref[...]).astype(BF)
        dqkv = qkvb.at[slot]

        def prob(c, cols, scores):
            m, e, inv = soft_stats(scores.astype(BF), scale)
            return e * inv

        prob.recompute = True
        attn_bwd(dqkv, slice(0, S), d_mix, HW, prob, pb, db, ({}, {}))
        d_norm_x = mm(dqkv[...], wqkvT[...]).astype(BF)
        x = xb[slot] + emb_ref[0:1, :]
        dx_ref[step] = d_mid + rms_bwd(x, d_norm_x)
        for j in range(3):
            acc2[4 + j] = acc2[4 + j] + mm_tn(dqkv[:, j * UNIT:(j + 1) * UNIT], ub[slot])

        at_step(step, 0, '51575254535045461n1e1m1b')
        at_step(step, 1, '5556191a1d1c')
        at_step(step, 2, '2n2e292a1f2d182m2c2b')
        at_step(step, 3, '2f283n3e393a3d3m')
        at_step(step, 4, '4n4e3c3b3f38')
        return carry

    lax.fori_loop(0, B, phase2, 0)

    begin([20, 17, 16, 18, 19, 21])
    run_events('0k0h0g0i0j0l5n5e494a4d4m4c4b4f48595a5d1k5m1h5c5b5f581g1j1i1l')
    run_events('2h2k2j2g2l2i3h3k3j3g3l3i4k4h5k5h4g4j5g5j4i4l5i5l')
    for k in range(N_ALL):
        for stage in range(6):
            copy_of(stage, k).wait_send()


def store_kernel(*refs):
    n = len(refs) // 2
    copies = [pltpu.make_async_copy(refs[i], refs[n + i], refs[-1].at[i]) for i in range(n)]
    for cp in copies:
        cp.start()
    for cp in copies:
        cp.wait()


def solution(mesh):
    batch_spec = P('data', None, None)

    def per_device(x, g, emb, w_q, w_k, w_v, w_o, wup, wdn):
        D, H, HW = w_q.shape
        B, S, _ = x.shape
        FF = wup.shape[1]
        L = emb.shape[0]
        T = L * S
        NQ = D // QW
        NS = QW // HW
        w_t = [w.transpose(1, 2, 0).reshape(D, D) for w in (w_q, w_k, w_v)]
        wo = w_o.reshape(D, D)
        const = lambda shape: pl.BlockSpec(shape, lambda b: (0,) * len(shape), pipeline_mode=pl.Buffered(1))
        per_seq = lambda cols: pl.BlockSpec((1, S, cols), lambda b: (b, 0, 0))
        col_seq = pl.BlockSpec((D, S), lambda b: (0, b))
        hbm = pl.BlockSpec(memory_space=pl.ANY)
        sds = jax.ShapeDtypeStruct
        saved = [sds((B, S, 3 * D), BF), sds((B, S, D), BF), sds((B, D, S), BF), sds((B, S, FF), BF), sds((B, D, S), BF), sds((B, S, D), BF), sds((B, S, D), BF)]
        acc, qkv0, u0, mix0, z0, mT0, h0, dout0 = pl.pallas_call(
            functools.partial(step_kernel, (S, D, FF, HW, L)),
            name='block_grads',
            grid=(B,),
            in_specs=[per_seq(D), per_seq(D), const(emb.shape), hbm, hbm, hbm, const(wo.shape), const(wup.shape), const(wdn.shape)],
            out_specs=[hbm] * 8,
            out_shape=[sds((12, UNIT, UNIT), F32)] + saved,
            scratch_shapes=[
                pltpu.VMEM((L + 1, S, D), BF),
                pltpu.VMEM((T, D), BF),
                pltpu.VMEM((T, 3 * D), BF),
                pltpu.VMEM((L, NQ, S, NS * S), BF),
                pltpu.VMEM((L, NQ, 8, NS * S), F32),
                pltpu.VMEM((D, T), BF),
                pltpu.VMEM((L, S, D), BF),
                pltpu.VMEM((D, T), BF),
                pltpu.VMEM((T, FF), BF),
                pltpu.VMEM((T, FF), BF),
                pltpu.VMEM((T, D), BF),
                pltpu.VMEM((T, D), BF),
                pltpu.VMEM((S, D), BF),
                pltpu.VMEM((3 * D, D), BF),
                pltpu.VMEM((NQ, S, NS * S), BF),
                pltpu.VMEM((NQ, S, NS * S), BF),
                pltpu.VMEM((12, UNIT, UNIT), F32),
                pltpu.SemaphoreType.DMA((12,)),
                pltpu.SemaphoreType.DMA((3,)),
                pltpu.SemaphoreType.DMA((7,)),
            ],
            compiler_params=pltpu.CompilerParams(dimension_semantics=('arbitrary',), vmem_limit_bytes=VMEM_MAX),
        )(x, g, emb, *w_t, wo, wup, wdn)
        vmem = pl.BlockSpec(memory_space=pltpu.VMEM)
        outs = pl.pallas_call(
            functools.partial(reduce_kernel, (B, S, D, FF, HW)),
            name='attn_reduce',
            in_specs=[vmem, vmem] + [hbm] * 14,
            out_specs=[vmem] * 7,
            out_shape=[pltpu.VMEM(x.shape, BF), pltpu.VMEM((FF, D), F32), pltpu.VMEM((D, FF), F32)] + [pltpu.VMEM((D, D), F32)] * 4,
            scratch_shapes=[
                pltpu.VMEM((2, S, D), BF),
                pltpu.VMEM((2, S, 3 * D), BF),
                pltpu.VMEM((2, S, D), BF),
                pltpu.VMEM((2, D, S), BF),
                pltpu.VMEM((2, S, FF), BF),
                pltpu.VMEM((2, D, S), BF),
                pltpu.VMEM((2, S, D), BF),
                pltpu.VMEM((2, S, D), BF),
                pltpu.VMEM((3 * D, D), BF),
                pltpu.VMEM((D, FF), BF),
                pltpu.VMEM((FF, D), BF),
                pltpu.VMEM((S, FF), BF),
                pltpu.VMEM((B, S, D), BF),
                pltpu.VMEM((NQ, S, NS * S), BF),
                pltpu.VMEM((NQ, S, NS * S), BF),
                pltpu.VMEM((8, UNIT, UNIT), F32),
                pltpu.VMEM((8, 128, UNIT), F32),
                pltpu.VMEM((24, 128, UNIT), F32),
                pltpu.VMEM((24, 64, UNIT), F32),
                pltpu.VMEM((24, 32, UNIT), F32),
                pltpu.SemaphoreType.DMA((6, 24)),
                pltpu.SemaphoreType.DMA((6, 24)),
                pltpu.SemaphoreType.DMA((16,)),
                pltpu.SemaphoreType.DMA((5,)),
                pltpu.SemaphoreType.DMA((8, 2)),
            ],
            compiler_params=pltpu.CompilerParams(vmem_limit_bytes=VMEM_MAX - (16 << 20), collective_id=0, has_side_effects=True),
        )(emb, wo, x, qkv0, u0, mix0, z0, mT0, h0, dout0, *w_t, wup, wdn, acc)
        d_x, dn, up, gq, gk, gv, go = pl.pallas_call(
            store_kernel,
            name='store',
            in_specs=[vmem] * 7,
            out_specs=[hbm] * 7,
            out_shape=[sds(o.shape, o.dtype) for o in outs],
            scratch_shapes=[pltpu.SemaphoreType.DMA((7,))],
            compiler_params=pltpu.CompilerParams(vmem_limit_bytes=1 << 20),
        )(*outs)
        back = lambda a: a.reshape(H, HW, D).transpose(2, 0, 1)
        return back(gq), back(gk), back(gv), go.reshape(H, HW, D), up, dn, d_x

    return jax.shard_map(per_device, mesh=mesh, in_specs=(batch_spec, batch_spec, P(), P(), P(), P(), P(), P(), P()), out_specs=(P(), P(), P(), P(), P(), P(), batch_spec), check_vma=False)
```

```python
import functools

import jax
import jax.numpy as jnp
from jax import lax
from jax.experimental import pallas as pl
from jax.experimental.pallas import tpu as pltpu
from jax.sharding import PartitionSpec as P

NORM_EPS = 1e-6
BF = jnp.bfloat16
F32 = jnp.float32
GELU_C = 0.7978845608028654
GELU_A = 0.044715
LOG2E = 1.4426950408889634
MESH = pl.DeviceIdType.MESH
UNIT = 512
QW = 256
VMEM_MAX = 67043328


def mm(a, b):
    return lax.dot_general(a, b, (((1,), (0,)), ((), ())), preferred_element_type=F32)


def mm_nt(a, b):
    return lax.dot_general(a, b, (((1,), (1,)), ((), ())), preferred_element_type=F32)


def mm_tn(a, b):
    return lax.dot_general(a, b, (((0,), (0,)), ((), ())), preferred_element_type=F32)


def rms_scale(xf):
    return lax.rsqrt(jnp.mean(xf * xf, axis=-1, keepdims=True) + NORM_EPS)


def rms_bwd(x, dy):
    xf = x.astype(F32)
    gf = dy.astype(F32)
    r = rms_scale(xf)
    dot = jnp.mean(xf * gf, axis=-1, keepdims=True)
    return (gf * r - xf * (r * r * r * dot)).astype(BF)


def gelu_fwd(z):
    zf = z.astype(F32)
    t = jnp.tanh(zf * (GELU_C + (GELU_C * GELU_A) * (zf * zf)))
    half = 0.5 * zf
    return (half + half * t).astype(BF)


def gelu_bwd(z, dg):
    zf = z.astype(F32)
    z2 = zf * zf
    t = jnp.tanh(zf * (GELU_C + (GELU_C * GELU_A) * z2))
    slope = (0.5 + 0.5 * t) + ((1.0 - t * t) * zf) * ((0.5 * GELU_C) + (1.5 * GELU_C * GELU_A) * z2)
    return (dg.astype(F32) * slope).astype(BF)


def head_stack(a4, width):
    lane = lax.broadcasted_iota(jnp.int32, a4.shape, 1)
    zero = jnp.zeros_like(a4)
    n_sub = a4.shape[1] // width
    return jnp.concatenate([jnp.where((lane >= h * width) & (lane < (h + 1) * width), a4, zero) for h in range(n_sub)], axis=0)


def soft_stats(sb, scale):
    m = jnp.max(sb, axis=0, keepdims=True).astype(F32)
    e = jnp.exp2((sb.astype(F32) - m) * (scale * LOG2E))
    inv = 1.0 / jnp.sum(e, axis=0, keepdims=True)
    return m, e, inv


def weave(chunks, fill):
    ahead = chunks[0][0]()
    for i, (_, use) in enumerate(chunks):
        now = ahead
        if i + 1 < len(chunks):
            ahead = chunks[i + 1][0]()
        use(now)
        for f in fill.get(i, ()):
            f()


def attn_bwd(qkv, rows, d_mix, HW, prob, pb, db, fills):
    S, D = d_mix.shape
    ns = QW // HW
    scale = HW ** -0.5
    width = ns * S
    tails = []
    for c in range(D // QW):
        qc = slice(c * QW, (c + 1) * QW)
        kc = slice(D + c * QW, D + (c + 1) * QW)
        vc = slice(2 * D + c * QW, 2 * D + (c + 1) * QW)
        k4 = qkv[rows, kc]
        v4 = qkv[rows, vc]
        qm = head_stack(qkv[rows, qc], HW)
        dom = head_stack(d_mix[:, qc], HW)
        kT = k4.T

        def chunk(i, c=c, k4=k4, v4=v4, qm=qm, dom=dom):
            cols = slice(i * QW, (i + 1) * QW)

            def use(vals):
                p = prob(c, cols, vals[1])
                dp = vals[0].astype(BF).astype(F32)
                delta = jnp.sum(dp * p, axis=0, keepdims=True)
                pb[c, :, cols] = p.astype(BF)
                db[c, :, cols] = ((p * (dp - delta)) * scale).astype(BF)
            return (lambda: (mm_nt(v4, dom[cols]), mm_nt(k4, qm[cols]) if prob.recompute else None)), use

        fill = {i: list(f) for i, f in fills[c].items()}
        for i, f in enumerate(tails):
            fill.setdefault(i, []).insert(0, f)

        def tail_v(c=c, vc=vc, dom=dom):
            qkv[rows, vc] = mm(pb[c], dom).astype(BF)

        def tail_k(c=c, kc=kc, qm=qm):
            qkv[rows, kc] = mm(db[c], qm).astype(BF)

        def tail_q(c=c, qc=qc, kT=kT):
            dqT = [mm(kT[h * HW:(h + 1) * HW], db[c, :, h * S:(h + 1) * S]).astype(BF) for h in range(ns)]
            qkv[rows, qc] = jnp.concatenate(dqT, axis=0).T

        weave([chunk(i) for i in range(width // QW)], fill)
        tails = [tail_v, tail_k, tail_q]
    for f in tails:
        f()


def mlp_bwd(d_out, zs, rows, wup, wdn, fill):
    FF = wdn.shape[0]
    total = []

    def chunk(i):
        cols = slice(i * QW, (i + 1) * QW)

        def use(v):
            zs[1][rows, cols] = gelu_bwd(zs[0](cols), v.astype(BF))
        return (lambda: mm_nt(d_out, wdn[cols, :])), use

    def part(j):
        cols = slice(j * UNIT, (j + 1) * UNIT)

        def run():
            v = mm_nt(zs[1][rows, cols], wup[:, cols])
            total[:] = [v if not total else total[0] + v]
        return run

    fill = {i: list(f) for i, f in fill.items()}
    for j in range(FF // UNIT):
        fill.setdefault(2 * j + 1, []).append(part(j))
    weave([chunk(i) for i in range(FF // QW)], fill)
    return total[0].astype(BF)


def step_kernel(cfg, x_ref, g_ref, emb_ref, wq_h, wk_h, wv_h, wo_ref, wup_ref, wdn_ref,
                acc_h, qkv0_h, u0_h, mix0_h, z0_h, mT0_h, h0_h, dout0_h,
                xs, us, qkv, st, stat, mixT, hs, mT, zs, gs, dmid, dout, dcur, wqkvT, pb, db, acc, sem, wsem, ssem):
    S, D, FF, HW, L = cfg
    NQ = D // QW
    NS = QW // HW
    scale = HW ** -0.5
    step = pl.program_id(0)
    last = pl.num_programs(0) - 1
    n_ff = FF // UNIT

    @pl.when(step == 0)
    def _():
        loads = [pltpu.make_async_copy(w, wqkvT.at[j * D:(j + 1) * D], wsem.at[j]) for j, w in enumerate((wq_h, wk_h, wv_h))]
        for cp in loads:
            cp.start()
        acc[...] = jnp.zeros_like(acc)
        for cp in loads:
            cp.wait()

    emb = emb_ref[...].astype(F32)
    xs[0] = x_ref[0] + emb[0:1].astype(BF)

    def fwd(l, carry, more=True):
        rows = pl.ds(pl.multiple_of(l * S, S), S) if more else slice(l * S, (l + 1) * S)
        x = xs[l]
        xf = x.astype(F32)
        u = (xf * rms_scale(xf)).astype(BF)
        us[rows, :] = u
        def proj(part, c):
            cols = slice(part * D + c * QW, part * D + (c + 1) * QW)

            def run():
                qkv[rows, cols] = mm_nt(u, wqkvT[cols, :]).astype(BF)
            return run

        def quad(c):
            k4 = qkv[rows, D + c * QW:D + (c + 1) * QW]
            qm = head_stack(qkv[rows, c * QW:(c + 1) * QW], HW)

            def chunk(i):
                cols = slice(i * QW, (i + 1) * QW)

                def use(v):
                    sb = v.astype(BF)
                    st[l, c, :, cols] = sb
                    m, e, inv = soft_stats(sb, scale)
                    stat[l, c, 0:1, cols] = m
                    stat[l, c, 1:2, cols] = inv
                    pb[c, :, cols] = (e * inv).astype(BF)
                return (lambda: mm_nt(k4, qm[cols])), use
            return [chunk(i) for i in range(NS * S // QW)]

        def head_out(c, h):
            def run():
                vT = qkv[rows, 2 * D + c * QW:2 * D + (c + 1) * QW].T
                o = mm(vT[h * HW:(h + 1) * HW], pb[c, :, h * S:(h + 1) * S])
                mixT[c * QW + h * HW:c * QW + (h + 1) * HW, rows] = o.astype(BF)
            return run

        for part in range(3):
            proj(part, 0)()
        weave(quad(0), {0: [proj(0, 1)], 1: [proj(1, 1)], 2: [proj(2, 1)], 3: [head_out(0, 0)], 4: [head_out(0, 1)]})
        weave(quad(1), {0: [head_out(0, 2)], 1: [head_out(0, 3)], 3: [head_out(1, 0)], 4: [head_out(1, 1)]})
        head_out(1, 2)()
        head_out(1, 3)()
        h_mid = x + mm_tn(mixT[:, rows], wo_ref[...]).astype(BF)
        hs[l] = h_mid
        hf = h_mid.astype(F32)
        mn = (hf * rms_scale(hf)).astype(BF)
        mT[:, rows] = mn.T
        down = []

        def up_chunk(i):
            cols = slice(i * QW, (i + 1) * QW)

            def use(v):
                z = v.astype(BF)
                zs[rows, cols] = z
                gs[rows, cols] = gelu_fwd(z)
            return (lambda: mm(mn, wup_ref[:, cols])), use

        def down_part(j):
            cols = slice(j * UNIT, (j + 1) * UNIT)

            def run():
                v = mm(gs[rows, cols], wdn_ref[cols, :])
                down[:] = [v if not down else down[0] + v]
            return run

        weave([up_chunk(i) for i in range(FF // QW)], {2 * j + 1: [down_part(j)] for j in range(n_ff)} if more else {})
        if not more:
            return carry
        y = down[0]
        nxt = emb[1:2]
        for j in range(2, L):
            nxt = jnp.where(l + 1 == j, emb[j:j + 1], nxt)
        xs[l + 1] = (h_mid + y.astype(BF)) + nxt.astype(BF)
        return carry

    lax.fori_loop(0, L - 1, fwd, 0)
    fwd(L - 1, 0, more=False)
    dcur[...] = g_ref[0]
    saves = [pltpu.make_async_copy(src, dst.at[step], ssem.at[n]) for n, (src, dst) in enumerate((
        (qkv.at[0:S], qkv0_h), (us.at[0:S], u0_h), (mixT.at[:, 0:S], mix0_h), (zs.at[0:S], z0_h),
        (mT.at[:, 0:S], mT0_h), (hs.at[0], h0_h), (dout.at[0:S], dout0_h)))]
    for cp in saves[:-1]:
        cp.start()

    def bwd(i, carry):
        l = L - 1 - i
        rows = pl.ds(pl.multiple_of(l * S, S), S)
        d_out = dcur[...]
        dout[rows, :] = d_out
        def add_unit(k, make):
            def run():
                acc[k] = acc[k] + make()
            return run

        ucol = lambda j: slice(j * UNIT, (j + 1) * UNIT)
        dn_unit = lambda j: add_unit(j, lambda: mm_tn(gs[rows, ucol(j)], d_out))
        up_unit = lambda j: add_unit(4 + j, lambda: mm(mT[:, rows], zs[rows, ucol(j)]))
        o_unit = add_unit(11, lambda: mm(mixT[:, rows], dmid[rows, :]))
        d_norm = mlp_bwd(d_out, (lambda cols: zs[rows, cols], zs), rows, wup_ref, wdn_ref, {2 * j: [dn_unit(j)] for j in range(n_ff)})
        d_mid = d_out + rms_bwd(hs[l], d_norm)
        dmid[rows, :] = d_mid
        d_mix = mm_nt(d_mid, wo_ref[...]).astype(BF)

        def prob(c, cols, unused):
            s = st[l, c, :, cols].astype(F32)
            return jnp.exp2((s - stat[l, c, 0:1, cols]) * (scale * LOG2E)) * stat[l, c, 1:2, cols]

        prob.recompute = False
        attn_bwd(qkv, rows, d_mix, HW, prob, pb, db, ({0: [up_unit(0)], 2: [up_unit(1)], 3: [up_unit(2)], 4: [up_unit(3)]}, {4: [o_unit]}))
        d_norm_x = mm(qkv[rows, :], wqkvT[...]).astype(BF)
        for j in range(3):
            acc[8 + j] = acc[8 + j] + mm_tn(qkv[rows, j * UNIT:(j + 1) * UNIT], us[rows, :])
        dcur[...] = d_mid + rms_bwd(xs[l], d_norm_x)
        return carry

    lax.fori_loop(0, L - 1, bwd, 0)
    dout[0:S, :] = dcur[...]
    saves[-1].start()

    @pl.when(step == last)
    def _():
        for k in range(4, 12):
            pltpu.make_async_copy(acc.at[k], acc_h.at[k], sem.at[k]).start()

    for j in range(n_ff):
        acc[j] = acc[j] + mm_tn(gs[0:S, j * UNIT:(j + 1) * UNIT], dout[0:S, :])
    for cp in saves:
        cp.wait()

    @pl.when(step == last)
    def _():
        for k in range(4):
            pltpu.make_async_copy(acc.at[k], acc_h.at[k], sem.at[k]).start()
        for k in range(12):
            pltpu.make_async_copy(acc.at[k], acc_h.at[k], sem.at[k]).wait()


def reduce_kernel(cfg, emb_ref, wo_ref, x_h, qkv_h, u_h, mix_h, z_h, mT_h, h_h, dout_h, wq_h, wk_h, wv_h, wup_h, wdn_h, acc_h,
                  dx_ref, r_dn, r_up, r_q, r_k, r_v, r_o,
                  xb, qkvb, ub, mixb, zb, mTb, hb, doutb,
                  wqkvT, wup, wdn, dup, dmid, pb, db, acc2, aw, r1, r2, r3, send, recv, lsem, wsem, isem):
    B, S, D, FF, HW = cfg
    NQ = D // QW
    n_ff = FF // UNIT
    scale = HW ** -0.5
    me = lax.axis_index('data')
    core = lax.rem(me, 2)
    bit_x = lax.rem(me // 2, 2)
    bit_y = me // 4
    core_peer = me + 1 - 2 * core
    x_peer = me + 2 - 4 * bit_x
    y_peer = me + 4 - 8 * bit_y
    SUB = UNIT // 2
    KEEP = SUB // 2
    N_EARLY = 2 * n_ff
    N_ALL = 24

    def order(u):
        if u % 2 == 0:
            return (bit_x, x_peer), (bit_y, y_peer)
        return (bit_y, y_peer), (bit_x, x_peer)

    def aligned(v, n):
        return pl.ds(pl.multiple_of(v, n), n)

    def part(u, start, n):
        if u < N_EARLY:
            return aw.at[u, aligned(start, n)]
        return acc2.at[u // 2 - n_ff, aligned(u % 2 * SUB + core * KEEP + start, n)]

    def remote(stage, u, src, dst, peer):
        return pltpu.make_async_remote_copy(src_ref=src, dst_ref=dst, send_sem=send.at[stage, u], recv_sem=recv.at[stage, u], device_id=(peer,), device_id_type=MESH)

    def copy_of(stage, u):
        (b1, p1), (b2, p2) = order(u)
        if stage == 0:
            rows = aligned(u % 2 * SUB + (1 - core) * KEEP, KEEP)
            src = acc_h.at[u // 2, rows] if u < N_EARLY else acc2.at[u // 2 - n_ff, rows]
            return remote(0, u, src, r1.at[u], core_peer)
        if stage == 1:
            return remote(1, u, part(u, (1 - b1) * 64, 64), r2.at[u], p1)
        if stage == 2:
            return remote(2, u, part(u, b1 * 64 + (1 - b2) * 32, 32), r3.at[u], p2)
        if stage == 3:
            mine = res_at(u, b1 * 64 + b2 * 32, 32)
            return remote(3, u, mine, mine, p2)
        if stage == 4:
            mine = res_at(u, b1 * 64, 64)
            return remote(4, u, mine, mine, p1)
        mine = res_at(u, 0, KEEP)
        return remote(5, u, mine, mine, core_peer)

    def res_at(u, start, n):
        k = u // 2
        row = u % 2 * SUB + core * KEEP + start
        if k < n_ff:
            return r_dn.at[aligned(k * UNIT + row, n)]
        if k < 8:
            return r_up.at[aligned(row, n), (k - 4) * UNIT:(k - 3) * UNIT]
        return (r_q, r_k, r_v, r_o)[k - 8].at[aligned(row, n)]

    def own_load(u):
        return pltpu.make_async_copy(acc_h.at[u // 2, aligned(u % 2 * SUB + core * KEEP, KEEP)], aw.at[u], lsem.at[u])

    def late_load(k):
        return pltpu.make_async_copy(acc_h.at[k], acc2.at[k - n_ff], lsem.at[n_ff + k])

    def serve(stage, u):
        (b1, _), (b2, _) = order(u)
        copy_of(stage, u).wait_recv()
        if stage == 0:
            if u < N_EARLY:
                own_load(u).wait()
            ref = part(u, 0, KEEP)
            ref[...] = ref[...] + r1[u]
        elif stage == 1:
            ref = part(u, b1 * 64, 64)
            ref[...] = ref[...] + r2[u]
        elif stage == 2:
            row = b1 * 64 + b2 * 32
            res_at(u, row, 32)[...] = part(u, row, 32)[...] + r3[u]
        if stage < 5:
            copy_of(stage + 1, u).start()

    def serve_all(stage, units):
        for u in units:
            serve(stage, u)

    def begin(units):
        for u in units:
            copy_of(0, u).start()

    def fetch(phase, i):
        slot = lax.rem(i, 2)
        pairs = ((mix_h, mixb), (z_h, zb), (mT_h, mTb), (h_h, hb), (dout_h, doutb)) if phase == 0 else ((x_h, xb), (qkv_h, qkvb), (u_h, ub))
        return [pltpu.make_async_copy(s_.at[i], d_.at[slot], isem.at[phase * 5 + n, slot]) for n, (s_, d_) in enumerate(pairs)]

    def arrive(phase, i):
        for cp in fetch(phase, i):
            cp.wait()

        @pl.when(i + 1 < B)
        def _():
            for cp in fetch(phase, i + 1):
                cp.start()
        return lax.rem(i, 2)

    def w_loads():
        pairs = [(wdn_h, wdn), (wup_h, wup)] + [(w, wqkvT.at[j * D:(j + 1) * D]) for j, w in enumerate((wq_h, wk_h, wv_h))]
        return [pltpu.make_async_copy(s_, d_, wsem.at[j]) for j, (s_, d_) in enumerate(pairs)]

    barrier = pltpu.get_barrier_semaphore()
    for peer in (core_peer, x_peer, y_peer):
        pl.semaphore_signal(barrier, inc=1, device_id=(peer,), device_id_type=MESH)
    for k in range(N_EARLY):
        own_load(k).start()
    for cp in fetch(0, 0):
        cp.start()
    for cp in w_loads():
        cp.start()
    pl.semaphore_wait(barrier, 3)
    begin(range(N_EARLY))
    for k in range(n_ff, 12):
        late_load(k).start()
    serve_all(0, range(N_EARLY))
    for cp in w_loads():
        cp.wait()
    for k in range(n_ff, 12):
        late_load(k).wait()

    def run_events(events):
        for stage, unit in zip(events[::2], events[1::2]):
            serve(int(stage), int(unit, 36))

    def at_step(step, i, events, before=''):
        @pl.when(step == i)
        def _():
            begin([int(unit, 36) for unit in before])
            run_events(events)

    def phase1(step, carry):
        slot = arrive(0, step)
        d_out = doutb[slot]

        def up_unit(j):
            def run():
                acc2[j] = acc2[j] + mm(mTb[slot], dup[:, j * UNIT:(j + 1) * UNIT])
            return run

        d_norm = mlp_bwd(d_out, (lambda cols: zb[slot, :, cols], dup), slice(0, S), wup, wdn, {2: [up_unit(0)], 4: [up_unit(1)], 6: [up_unit(2)]})
        d_mid = d_out + rms_bwd(hb[slot], d_norm)
        dmid[step] = d_mid
        up_unit(3)()
        acc2[7] = acc2[7] + mm(mixb[slot], d_mid)

        at_step(step, 0, '1110')
        at_step(step, 1, '12141315')
        at_step(step, 2, '172116232022')
        at_step(step, 3, '272425263130')
        at_step(step, 4, '373234333536')
        at_step(step, 5, '0n0e0m0b090c0a0d080f414742444340', before='nemb9cad8f')
        return carry

    for cp in fetch(1, 0):
        cp.start()
    lax.fori_loop(0, B, phase1, 0)

    def phase2(step, carry):
        slot = arrive(1, step)
        d_mid = dmid[step]
        d_mix = mm_nt(d_mid, wo_ref[...]).astype(BF)
        dqkv = qkvb.at[slot]

        def prob(c, cols, scores):
            m, e, inv = soft_stats(scores.astype(BF), scale)
            return e * inv

        prob.recompute = True
        attn_bwd(dqkv, slice(0, S), d_mix, HW, prob, pb, db, ({}, {}))
        d_norm_x = mm(dqkv[...], wqkvT[...]).astype(BF)
        x = xb[slot] + emb_ref[0:1, :]
        dx_ref[step] = d_mid + rms_bwd(x, d_norm_x)
        for j in range(3):
            acc2[4 + j] = acc2[4 + j] + mm_tn(dqkv[:, j * UNIT:(j + 1) * UNIT], ub[slot])

        at_step(step, 0, '51575254535045461n1e1m1b')
        at_step(step, 1, '5556191a1d1c')
        at_step(step, 2, '2n2e292a1f2d182m2c2b')
        at_step(step, 3, '2f283n3e393a3d3m')
        at_step(step, 4, '4n4e3c3b3f38')
        return carry

    lax.fori_loop(0, B, phase2, 0)

    begin([20, 17, 16, 18, 19, 21])
    run_events('0k0h0g0i0j0l5n5e494a4d4m4c4b4f48595a5d1k5m1h5c5b5f581g1j1i1l')
    run_events('2h2k2j2g2l2i3h3k3j3g3l3i4k4h5k5h4g4j5g5j4i4l5i5l')
    for k in range(N_ALL):
        for stage in range(6):
            copy_of(stage, k).wait_send()


def store_kernel(*refs):
    n = len(refs) // 2
    copies = [pltpu.make_async_copy(refs[i], refs[n + i], refs[-1].at[i]) for i in range(n)]
    for cp in copies:
        cp.start()
    for cp in copies:
        cp.wait()


def solution(mesh):
    batch_spec = P('data', None, None)

    def per_device(x, g, emb, w_q, w_k, w_v, w_o, wup, wdn):
        D, H, HW = w_q.shape
        B, S, _ = x.shape
        FF = wup.shape[1]
        L = emb.shape[0]
        T = L * S
        NQ = D // QW
        NS = QW // HW
        w_t = [w.transpose(1, 2, 0).reshape(D, D) for w in (w_q, w_k, w_v)]
        wo = w_o.reshape(D, D)
        const = lambda shape: pl.BlockSpec(shape, lambda b: (0,) * len(shape), pipeline_mode=pl.Buffered(1))
        per_seq = lambda cols: pl.BlockSpec((1, S, cols), lambda b: (b, 0, 0))
        col_seq = pl.BlockSpec((D, S), lambda b: (0, b))
        hbm = pl.BlockSpec(memory_space=pl.ANY)
        sds = jax.ShapeDtypeStruct
        saved = [sds((B, S, 3 * D), BF), sds((B, S, D), BF), sds((B, D, S), BF), sds((B, S, FF), BF), sds((B, D, S), BF), sds((B, S, D), BF), sds((B, S, D), BF)]
        acc, qkv0, u0, mix0, z0, mT0, h0, dout0 = pl.pallas_call(
            functools.partial(step_kernel, (S, D, FF, HW, L)),
            name='block_grads',
            grid=(B,),
            in_specs=[per_seq(D), per_seq(D), const(emb.shape), hbm, hbm, hbm, const(wo.shape), const(wup.shape), const(wdn.shape)],
            out_specs=[hbm] * 8,
            out_shape=[sds((12, UNIT, UNIT), F32)] + saved,
            scratch_shapes=[
                pltpu.VMEM((L, S, D), BF),
                pltpu.VMEM((T, D), BF),
                pltpu.VMEM((T, 3 * D), BF),
                pltpu.VMEM((L, NQ, S, NS * S), BF),
                pltpu.VMEM((L, NQ, 8, NS * S), F32),
                pltpu.VMEM((D, T), BF),
                pltpu.VMEM((L, S, D), BF),
                pltpu.VMEM((D, T), BF),
                pltpu.VMEM((T, FF), BF),
                pltpu.VMEM((T, FF), BF),
                pltpu.VMEM((T, D), BF),
                pltpu.VMEM((T, D), BF),
                pltpu.VMEM((S, D), BF),
                pltpu.VMEM((3 * D, D), BF),
                pltpu.VMEM((NQ, S, NS * S), BF),
                pltpu.VMEM((NQ, S, NS * S), BF),
                pltpu.VMEM((12, UNIT, UNIT), F32),
                pltpu.SemaphoreType.DMA((12,)),
                pltpu.SemaphoreType.DMA((3,)),
                pltpu.SemaphoreType.DMA((7,)),
            ],
            compiler_params=pltpu.CompilerParams(dimension_semantics=('arbitrary',), vmem_limit_bytes=VMEM_MAX),
        )(x, g, emb, *w_t, wo, wup, wdn)
        vmem = pl.BlockSpec(memory_space=pltpu.VMEM)
        outs = pl.pallas_call(
            functools.partial(reduce_kernel, (B, S, D, FF, HW)),
            name='attn_reduce',
            in_specs=[vmem, vmem] + [hbm] * 14,
            out_specs=[vmem] * 7,
            out_shape=[pltpu.VMEM(x.shape, BF), pltpu.VMEM((FF, D), F32), pltpu.VMEM((D, FF), F32)] + [pltpu.VMEM((D, D), F32)] * 4,
            scratch_shapes=[
                pltpu.VMEM((2, S, D), BF),
                pltpu.VMEM((2, S, 3 * D), BF),
                pltpu.VMEM((2, S, D), BF),
                pltpu.VMEM((2, D, S), BF),
                pltpu.VMEM((2, S, FF), BF),
                pltpu.VMEM((2, D, S), BF),
                pltpu.VMEM((2, S, D), BF),
                pltpu.VMEM((2, S, D), BF),
                pltpu.VMEM((3 * D, D), BF),
                pltpu.VMEM((D, FF), BF),
                pltpu.VMEM((FF, D), BF),
                pltpu.VMEM((S, FF), BF),
                pltpu.VMEM((B, S, D), BF),
                pltpu.VMEM((NQ, S, NS * S), BF),
                pltpu.VMEM((NQ, S, NS * S), BF),
                pltpu.VMEM((8, UNIT, UNIT), F32),
                pltpu.VMEM((8, 128, UNIT), F32),
                pltpu.VMEM((24, 128, UNIT), F32),
                pltpu.VMEM((24, 64, UNIT), F32),
                pltpu.VMEM((24, 32, UNIT), F32),
                pltpu.SemaphoreType.DMA((6, 24)),
                pltpu.SemaphoreType.DMA((6, 24)),
                pltpu.SemaphoreType.DMA((16,)),
                pltpu.SemaphoreType.DMA((5,)),
                pltpu.SemaphoreType.DMA((8, 2)),
            ],
            compiler_params=pltpu.CompilerParams(vmem_limit_bytes=VMEM_MAX - (16 << 20), collective_id=0, has_side_effects=True),
        )(emb, wo, x, qkv0, u0, mix0, z0, mT0, h0, dout0, *w_t, wup, wdn, acc)
        d_x, dn, up, gq, gk, gv, go = pl.pallas_call(
            store_kernel,
            name='store',
            in_specs=[vmem] * 7,
            out_specs=[hbm] * 7,
            out_shape=[sds(o.shape, o.dtype) for o in outs],
            scratch_shapes=[pltpu.SemaphoreType.DMA((7,))],
            compiler_params=pltpu.CompilerParams(vmem_limit_bytes=1 << 20),
        )(*outs)
        back = lambda a: a.reshape(H, HW, D).transpose(2, 0, 1)
        return back(gq), back(gk), back(gv), go.reshape(H, HW, D), up, dn, d_x

    return jax.shard_map(per_device, mesh=mesh, in_specs=(batch_spec, batch_spec, P(), P(), P(), P(), P(), P(), P()), out_specs=(P(), P(), P(), P(), P(), P(), batch_spec), check_vma=False)
```

```python
import functools

import jax
import jax.numpy as jnp
from jax import lax
from jax.experimental import pallas as pl
from jax.experimental.pallas import tpu as pltpu
from jax.sharding import PartitionSpec as P

NORM_EPS = 1e-6
BF = jnp.bfloat16
F32 = jnp.float32
GELU_C = 0.7978845608028654
GELU_A = 0.044715
LOG2E = 1.4426950408889634
MESH = pl.DeviceIdType.MESH
UNIT = 512
QW = 256
VMEM_MAX = 67043328


def mm(a, b):
    return lax.dot_general(a, b, (((1,), (0,)), ((), ())), preferred_element_type=F32)


def mm_nt(a, b):
    return lax.dot_general(a, b, (((1,), (1,)), ((), ())), preferred_element_type=F32)


def mm_tn(a, b):
    return lax.dot_general(a, b, (((0,), (0,)), ((), ())), preferred_element_type=F32)


def rms_scale(xf):
    return lax.rsqrt(jnp.mean(xf * xf, axis=-1, keepdims=True) + NORM_EPS)


def rms_bwd(x, dy):
    xf = x.astype(F32)
    gf = dy.astype(F32)
    r = rms_scale(xf)
    dot = jnp.mean(xf * gf, axis=-1, keepdims=True)
    return (gf * r - xf * (r * r * r * dot)).astype(BF)


def gelu_fwd(z):
    zf = z.astype(F32)
    t = jnp.tanh(zf * (GELU_C + (GELU_C * GELU_A) * (zf * zf)))
    half = 0.5 * zf
    return (half + half * t).astype(BF)


def gelu_bwd(z, dg):
    zf = z.astype(F32)
    z2 = zf * zf
    t = jnp.tanh(zf * (GELU_C + (GELU_C * GELU_A) * z2))
    slope = (0.5 + 0.5 * t) + ((1.0 - t * t) * zf) * ((0.5 * GELU_C) + (1.5 * GELU_C * GELU_A) * z2)
    return (dg.astype(F32) * slope).astype(BF)


def head_stack(a4, width):
    lane = lax.broadcasted_iota(jnp.int32, a4.shape, 1)
    zero = jnp.zeros_like(a4)
    n_sub = a4.shape[1] // width
    return jnp.concatenate([jnp.where((lane >= h * width) & (lane < (h + 1) * width), a4, zero) for h in range(n_sub)], axis=0)


def soft_stats(sb, scale):
    m = jnp.max(sb, axis=0, keepdims=True).astype(F32)
    e = jnp.exp2((sb.astype(F32) - m) * (scale * LOG2E))
    inv = 1.0 / jnp.sum(e, axis=0, keepdims=True)
    return m, e, inv


def weave(chunks, fill):
    ahead = chunks[0][0]()
    for i, (_, use) in enumerate(chunks):
        now = ahead
        if i + 1 < len(chunks):
            ahead = chunks[i + 1][0]()
        use(now)
        for f in fill.get(i, ()):
            f()


def attn_bwd(qkv, rows, d_mix, HW, prob, pb, db, fills):
    S, D = d_mix.shape
    ns = QW // HW
    scale = HW ** -0.5
    width = ns * S
    tails = []
    for c in range(D // QW):
        qc = slice(c * QW, (c + 1) * QW)
        kc = slice(D + c * QW, D + (c + 1) * QW)
        vc = slice(2 * D + c * QW, 2 * D + (c + 1) * QW)
        k4 = qkv[rows, kc]
        v4 = qkv[rows, vc]
        qm = head_stack(qkv[rows, qc], HW)
        dom = head_stack(d_mix[:, qc], HW)
        kT = k4.T

        def chunk(i, c=c, k4=k4, v4=v4, qm=qm, dom=dom):
            cols = slice(i * QW, (i + 1) * QW)

            def use(vals):
                p = prob(c, cols, vals[1])
                dp = vals[0].astype(BF).astype(F32)
                delta = jnp.sum(dp * p, axis=0, keepdims=True)
                pb[c, :, cols] = p.astype(BF)
                db[c, :, cols] = ((p * (dp - delta)) * scale).astype(BF)
            return (lambda: (mm_nt(v4, dom[cols]), mm_nt(k4, qm[cols]) if prob.recompute else None)), use

        fill = {i: list(f) for i, f in fills[c].items()}
        for i, f in enumerate(tails):
            fill.setdefault(i, []).insert(0, f)

        def tail_v(c=c, vc=vc, dom=dom):
            qkv[rows, vc] = mm(pb[c], dom).astype(BF)

        def tail_k(c=c, kc=kc, qm=qm):
            qkv[rows, kc] = mm(db[c], qm).astype(BF)

        def tail_q(c=c, qc=qc, kT=kT):
            dqT = [mm(kT[h * HW:(h + 1) * HW], db[c, :, h * S:(h + 1) * S]).astype(BF) for h in range(ns)]
            qkv[rows, qc] = jnp.concatenate(dqT, axis=0).T

        weave([chunk(i) for i in range(width // QW)], fill)
        tails = [tail_v, tail_k, tail_q]
    for f in tails:
        f()


def mlp_bwd(d_out, zs, rows, wup, wdn, fill):
    FF = wdn.shape[0]
    total = []

    def chunk(i):
        cols = slice(i * QW, (i + 1) * QW)

        def use(v):
            zs[1][rows, cols] = gelu_bwd(zs[0](cols), v.astype(BF))
        return (lambda: mm_nt(d_out, wdn[cols, :])), use

    def part(j):
        cols = slice(j * UNIT, (j + 1) * UNIT)

        def run():
            v = mm_nt(zs[1][rows, cols], wup[:, cols])
            total[:] = [v if not total else total[0] + v]
        return run

    fill = {i: list(f) for i, f in fill.items()}
    for j in range(FF // UNIT):
        fill.setdefault(2 * j + 1, []).append(part(j))
    weave([chunk(i) for i in range(FF // QW)], fill)
    return total[0].astype(BF)


def step_kernel(cfg, x_ref, g_ref, emb_ref, wq_h, wk_h, wv_h, wo_h, wup_h, wdn_h,
                acc_h, qkv0_h, u0_h, mix0_h, z0_h, mT0_h, h0_h, dout0_h,
                wo_ref, wup_ref, wdn_ref, xs, us, qkv, st, stat, mixT, hs, mT, zs, gs, dmid, dout, dcur, wqkvT, pb, db, acc, sem, wsem, ssem):
    S, D, FF, HW, L = cfg
    NQ = D // QW
    NS = QW // HW
    scale = HW ** -0.5
    step = pl.program_id(0)
    last = pl.num_programs(0) - 1
    n_ff = FF // UNIT

    @pl.when(step == 0)
    def _():
        loads = [pltpu.make_async_copy(w, wqkvT.at[j * D:(j + 1) * D], wsem.at[j]) for j, w in enumerate((wq_h, wk_h, wv_h))]
        loads += [pltpu.make_async_copy(w, d_, wsem.at[3 + j]) for j, (w, d_) in enumerate(((wo_h, wo_ref), (wup_h, wup_ref), (wdn_h, wdn_ref)))]
        for cp in loads:
            cp.start()
        acc[...] = jnp.zeros_like(acc)
        for cp in loads:
            cp.wait()

    emb = emb_ref[...].astype(F32)
    xs[0] = x_ref[0] + emb[0:1].astype(BF)

    def fwd(l, carry, more=True):
        rows = pl.ds(pl.multiple_of(l * S, S), S) if more else slice(l * S, (l + 1) * S)
        x = xs[l]
        xf = x.astype(F32)
        u = (xf * rms_scale(xf)).astype(BF)
        us[rows, :] = u
        def proj(part, c):
            cols = slice(part * D + c * QW, part * D + (c + 1) * QW)

            def run():
                qkv[rows, cols] = mm_nt(u, wqkvT[cols, :]).astype(BF)
            return run

        def quad(c):
            k4 = qkv[rows, D + c * QW:D + (c + 1) * QW]
            qm = head_stack(qkv[rows, c * QW:(c + 1) * QW], HW)

            def chunk(i):
                cols = slice(i * QW, (i + 1) * QW)

                def use(v):
                    sb = v.astype(BF)
                    st[l, c, :, cols] = sb
                    m, e, inv = soft_stats(sb, scale)
                    stat[l, c, 0:1, cols] = m
                    stat[l, c, 1:2, cols] = inv
                    pb[c, :, cols] = (e * inv).astype(BF)
                return (lambda: mm_nt(k4, qm[cols])), use
            return [chunk(i) for i in range(NS * S // QW)]

        def head_out(c, h):
            def run():
                vT = qkv[rows, 2 * D + c * QW:2 * D + (c + 1) * QW].T
                o = mm(vT[h * HW:(h + 1) * HW], pb[c, :, h * S:(h + 1) * S])
                mixT[c * QW + h * HW:c * QW + (h + 1) * HW, rows] = o.astype(BF)
            return run

        for part in range(3):
            proj(part, 0)()
        weave(quad(0), {0: [proj(0, 1)], 1: [proj(1, 1)], 2: [proj(2, 1)], 3: [head_out(0, 0)], 4: [head_out(0, 1)]})
        weave(quad(1), {0: [head_out(0, 2)], 1: [head_out(0, 3)], 3: [head_out(1, 0)], 4: [head_out(1, 1)]})
        head_out(1, 2)()
        head_out(1, 3)()
        h_mid = x + mm_tn(mixT[:, rows], wo_ref[...]).astype(BF)
        hs[l] = h_mid
        hf = h_mid.astype(F32)
        mn = (hf * rms_scale(hf)).astype(BF)
        mT[:, rows] = mn.T
        down = []

        def up_chunk(i):
            cols = slice(i * QW, (i + 1) * QW)

            def use(v):
                z = v.astype(BF)
                zs[rows, cols] = z
                gs[rows, cols] = gelu_fwd(z)
            return (lambda: mm(mn, wup_ref[:, cols])), use

        def down_part(j):
            cols = slice(j * UNIT, (j + 1) * UNIT)

            def run():
                v = mm(gs[rows, cols], wdn_ref[cols, :])
                down[:] = [v if not down else down[0] + v]
            return run

        weave([up_chunk(i) for i in range(FF // QW)], {2 * j + 1: [down_part(j)] for j in range(n_ff)} if more else {})
        if not more:
            return carry
        y = down[0]
        nxt = emb[1:2]
        for j in range(2, L):
            nxt = jnp.where(l + 1 == j, emb[j:j + 1], nxt)
        xs[l + 1] = (h_mid + y.astype(BF)) + nxt.astype(BF)
        return carry

    lax.fori_loop(0, L - 1, fwd, 0)
    fwd(L - 1, 0, more=False)
    dcur[...] = g_ref[0]
    saves = [pltpu.make_async_copy(src, dst.at[step], ssem.at[n]) for n, (src, dst) in enumerate((
        (qkv.at[0:S], qkv0_h), (us.at[0:S], u0_h), (mixT.at[:, 0:S], mix0_h), (zs.at[0:S], z0_h),
        (mT.at[:, 0:S], mT0_h), (hs.at[0], h0_h), (dout.at[0:S], dout0_h)))]
    for cp in saves[:-1]:
        cp.start()

    def bwd(i, carry):
        l = L - 1 - i
        rows = pl.ds(pl.multiple_of(l * S, S), S)
        d_out = dcur[...]
        dout[rows, :] = d_out
        def add_unit(k, make):
            def run():
                acc[k] = acc[k] + make()
            return run

        ucol = lambda j: slice(j * UNIT, (j + 1) * UNIT)
        dn_unit = lambda j: add_unit(j, lambda: mm_tn(gs[rows, ucol(j)], d_out))
        up_unit = lambda j: add_unit(4 + j, lambda: mm(mT[:, rows], zs[rows, ucol(j)]))
        o_unit = add_unit(11, lambda: mm(mixT[:, rows], dmid[rows, :]))
        d_norm = mlp_bwd(d_out, (lambda cols: zs[rows, cols], zs), rows, wup_ref, wdn_ref, {2 * j: [dn_unit(j)] for j in range(n_ff)})
        d_mid = d_out + rms_bwd(hs[l], d_norm)
        dmid[rows, :] = d_mid
        d_mix = mm_nt(d_mid, wo_ref[...]).astype(BF)

        def prob(c, cols, unused):
            s = st[l, c, :, cols].astype(F32)
            return jnp.exp2((s - stat[l, c, 0:1, cols]) * (scale * LOG2E)) * stat[l, c, 1:2, cols]

        prob.recompute = False
        attn_bwd(qkv, rows, d_mix, HW, prob, pb, db, ({0: [up_unit(0)], 2: [up_unit(1)], 3: [up_unit(2)], 4: [up_unit(3)]}, {4: [o_unit]}))
        d_norm_x = mm(qkv[rows, :], wqkvT[...]).astype(BF)
        for j in range(3):
            acc[8 + j] = acc[8 + j] + mm_tn(qkv[rows, j * UNIT:(j + 1) * UNIT], us[rows, :])
        dcur[...] = d_mid + rms_bwd(xs[l], d_norm_x)
        return carry

    lax.fori_loop(0, L - 1, bwd, 0)
    dout[0:S, :] = dcur[...]
    saves[-1].start()

    @pl.when(step == last)
    def _():
        for k in range(4, 12):
            pltpu.make_async_copy(acc.at[k], acc_h.at[k], sem.at[k]).start()

    for j in range(n_ff):
        acc[j] = acc[j] + mm_tn(gs[0:S, j * UNIT:(j + 1) * UNIT], dout[0:S, :])
    for cp in saves:
        cp.wait()

    @pl.when(step == last)
    def _():
        for k in range(4):
            pltpu.make_async_copy(acc.at[k], acc_h.at[k], sem.at[k]).start()
        for k in range(12):
            pltpu.make_async_copy(acc.at[k], acc_h.at[k], sem.at[k]).wait()


def reduce_kernel(cfg, emb_ref, wo_ref, x_h, qkv_h, u_h, mix_h, z_h, mT_h, h_h, dout_h, wq_h, wk_h, wv_h, wup_h, wdn_h, acc_h,
                  dx_ref, r_dn, r_up, r_q, r_k, r_v, r_o,
                  xb, qkvb, ub, mixb, zb, mTb, hb, doutb,
                  wqkvT, wup, wdn, dup, dmid, pb, db, acc2, aw, r1, r2, r3, send, recv, lsem, wsem, isem):
    B, S, D, FF, HW = cfg
    NQ = D // QW
    n_ff = FF // UNIT
    scale = HW ** -0.5
    me = lax.axis_index('data')
    core = lax.rem(me, 2)
    bit_x = lax.rem(me // 2, 2)
    bit_y = me // 4
    core_peer = me + 1 - 2 * core
    x_peer = me + 2 - 4 * bit_x
    y_peer = me + 4 - 8 * bit_y
    SUB = UNIT // 2
    KEEP = SUB // 2
    N_EARLY = 2 * n_ff
    N_ALL = 24

    def order(u):
        if u % 2 == 0:
            return (bit_x, x_peer), (bit_y, y_peer)
        return (bit_y, y_peer), (bit_x, x_peer)

    def aligned(v, n):
        return pl.ds(pl.multiple_of(v, n), n)

    def part(u, start, n):
        if u < N_EARLY:
            return aw.at[u, aligned(start, n)]
        return acc2.at[u // 2 - n_ff, aligned(u % 2 * SUB + core * KEEP + start, n)]

    def remote(stage, u, src, dst, peer):
        return pltpu.make_async_remote_copy(src_ref=src, dst_ref=dst, send_sem=send.at[stage, u], recv_sem=recv.at[stage, u], device_id=(peer,), device_id_type=MESH)

    def copy_of(stage, u):
        (b1, p1), (b2, p2) = order(u)
        if stage == 0:
            rows = aligned(u % 2 * SUB + (1 - core) * KEEP, KEEP)
            src = acc_h.at[u // 2, rows] if u < N_EARLY else acc2.at[u // 2 - n_ff, rows]
            return remote(0, u, src, r1.at[u], core_peer)
        if stage == 1:
            return remote(1, u, part(u, (1 - b1) * 64, 64), r2.at[u], p1)
        if stage == 2:
            return remote(2, u, part(u, b1 * 64 + (1 - b2) * 32, 32), r3.at[u], p2)
        if stage == 3:
            mine = res_at(u, b1 * 64 + b2 * 32, 32)
            return remote(3, u, mine, mine, p2)
        if stage == 4:
            mine = res_at(u, b1 * 64, 64)
            return remote(4, u, mine, mine, p1)
        mine = res_at(u, 0, KEEP)
        return remote(5, u, mine, mine, core_peer)

    def res_at(u, start, n):
        k = u // 2
        row = u % 2 * SUB + core * KEEP + start
        if k < n_ff:
            return r_dn.at[aligned(k * UNIT + row, n)]
        if k < 8:
            return r_up.at[aligned(row, n), (k - 4) * UNIT:(k - 3) * UNIT]
        return (r_q, r_k, r_v, r_o)[k - 8].at[aligned(row, n)]

    def own_load(u):
        return pltpu.make_async_copy(acc_h.at[u // 2, aligned(u % 2 * SUB + core * KEEP, KEEP)], aw.at[u], lsem.at[u])

    def late_load(k):
        return pltpu.make_async_copy(acc_h.at[k], acc2.at[k - n_ff], lsem.at[n_ff + k])

    def serve(stage, u):
        (b1, _), (b2, _) = order(u)
        copy_of(stage, u).wait_recv()
        if stage == 0:
            if u < N_EARLY:
                own_load(u).wait()
            ref = part(u, 0, KEEP)
            ref[...] = ref[...] + r1[u]
        elif stage == 1:
            ref = part(u, b1 * 64, 64)
            ref[...] = ref[...] + r2[u]
        elif stage == 2:
            row = b1 * 64 + b2 * 32
            res_at(u, row, 32)[...] = part(u, row, 32)[...] + r3[u]
        if stage < 5:
            copy_of(stage + 1, u).start()

    def serve_all(stage, units):
        for u in units:
            serve(stage, u)

    def begin(units):
        for u in units:
            copy_of(0, u).start()

    def fetch(phase, i):
        slot = lax.rem(i, 2)
        pairs = ((mix_h, mixb), (z_h, zb), (mT_h, mTb), (h_h, hb), (dout_h, doutb)) if phase == 0 else ((x_h, xb), (qkv_h, qkvb), (u_h, ub))
        return [pltpu.make_async_copy(s_.at[i], d_.at[slot], isem.at[phase * 5 + n, slot]) for n, (s_, d_) in enumerate(pairs)]

    def arrive(phase, i):
        for cp in fetch(phase, i):
            cp.wait()

        @pl.when(i + 1 < B)
        def _():
            for cp in fetch(phase, i + 1):
                cp.start()
        return lax.rem(i, 2)

    def w_loads():
        pairs = [(wdn_h, wdn), (wup_h, wup)] + [(w, wqkvT.at[j * D:(j + 1) * D]) for j, w in enumerate((wq_h, wk_h, wv_h))]
        return [pltpu.make_async_copy(s_, d_, wsem.at[j]) for j, (s_, d_) in enumerate(pairs)]

    barrier = pltpu.get_barrier_semaphore()
    for peer in (core_peer, x_peer, y_peer):
        pl.semaphore_signal(barrier, inc=1, device_id=(peer,), device_id_type=MESH)
    for k in range(N_EARLY):
        own_load(k).start()
    for cp in fetch(0, 0):
        cp.start()
    for cp in w_loads():
        cp.start()
    pl.semaphore_wait(barrier, 3)
    begin(range(N_EARLY))
    for k in range(n_ff, 12):
        late_load(k).start()
    serve_all(0, range(N_EARLY))
    for cp in w_loads():
        cp.wait()
    for k in range(n_ff, 12):
        late_load(k).wait()

    def run_events(events):
        for stage, unit in zip(events[::2], events[1::2]):
            serve(int(stage), int(unit, 36))

    def at_step(step, i, events, before=''):
        @pl.when(step == i)
        def _():
            begin([int(unit, 36) for unit in before])
            run_events(events)

    def phase1(step, carry):
        slot = arrive(0, step)
        d_out = doutb[slot]

        def up_unit(j):
            def run():
                acc2[j] = acc2[j] + mm(mTb[slot], dup[:, j * UNIT:(j + 1) * UNIT])
            return run

        d_norm = mlp_bwd(d_out, (lambda cols: zb[slot, :, cols], dup), slice(0, S), wup, wdn, {2: [up_unit(0)], 4: [up_unit(1)], 6: [up_unit(2)]})
        d_mid = d_out + rms_bwd(hb[slot], d_norm)
        dmid[step] = d_mid
        up_unit(3)()
        acc2[7] = acc2[7] + mm(mixb[slot], d_mid)

        at_step(step, 0, '1110')
        at_step(step, 1, '12141315')
        at_step(step, 2, '172116232022')
        at_step(step, 3, '272425263130')
        at_step(step, 4, '373234333536')
        at_step(step, 5, '0n0e0m0b090c0a0d080f414742444340', before='nemb9cad8f')
        return carry

    for cp in fetch(1, 0):
        cp.start()
    lax.fori_loop(0, B, phase1, 0)

    def phase2(step, carry):
        slot = arrive(1, step)
        d_mid = dmid[step]
        d_mix = mm_nt(d_mid, wo_ref[...]).astype(BF)
        dqkv = qkvb.at[slot]

        def prob(c, cols, scores):
            m, e, inv = soft_stats(scores.astype(BF), scale)
            return e * inv

        prob.recompute = True
        attn_bwd(dqkv, slice(0, S), d_mix, HW, prob, pb, db, ({}, {}))
        d_norm_x = mm(dqkv[...], wqkvT[...]).astype(BF)
        x = xb[slot] + emb_ref[0:1, :]
        dx_ref[step] = d_mid + rms_bwd(x, d_norm_x)
        for j in range(3):
            acc2[4 + j] = acc2[4 + j] + mm_tn(dqkv[:, j * UNIT:(j + 1) * UNIT], ub[slot])

        at_step(step, 0, '51575254535045461n1e1m1b')
        at_step(step, 1, '5556191a1d1c')
        at_step(step, 2, '2n2e292a1f2d182m2c2b')
        at_step(step, 3, '2f283n3e393a3d3m')
        at_step(step, 4, '4n4e3c3b3f38')
        return carry

    lax.fori_loop(0, B, phase2, 0)

    begin([20, 17, 16, 18, 19, 21])
    run_events('0k0h0g0i0j0l5n5e494a4d4m4c4b4f48595a5d1k5m1h5c5b5f581g1j1i1l')
    run_events('2h2k2j2g2l2i3h3k3j3g3l3i4k4h5k5h4g4j5g5j4i4l5i5l')
    for k in range(N_ALL):
        for stage in range(6):
            copy_of(stage, k).wait_send()


def store_kernel(*refs):
    n = len(refs) // 2
    copies = [pltpu.make_async_copy(refs[i], refs[n + i], refs[-1].at[i]) for i in range(n)]
    for cp in copies:
        cp.start()
    for cp in copies:
        cp.wait()


def solution(mesh):
    batch_spec = P('data', None, None)

    def per_device(x, g, emb, w_q, w_k, w_v, w_o, wup, wdn):
        D, H, HW = w_q.shape
        B, S, _ = x.shape
        FF = wup.shape[1]
        L = emb.shape[0]
        T = L * S
        NQ = D // QW
        NS = QW // HW
        w_t = [w.transpose(1, 2, 0).reshape(D, D) for w in (w_q, w_k, w_v)]
        wo = w_o.reshape(D, D)
        const = lambda shape: pl.BlockSpec(shape, lambda b: (0,) * len(shape), pipeline_mode=pl.Buffered(1))
        per_seq = lambda cols: pl.BlockSpec((1, S, cols), lambda b: (b, 0, 0))
        col_seq = pl.BlockSpec((D, S), lambda b: (0, b))
        hbm = pl.BlockSpec(memory_space=pl.ANY)
        sds = jax.ShapeDtypeStruct
        saved = [sds((B, S, 3 * D), BF), sds((B, S, D), BF), sds((B, D, S), BF), sds((B, S, FF), BF), sds((B, D, S), BF), sds((B, S, D), BF), sds((B, S, D), BF)]
        acc, qkv0, u0, mix0, z0, mT0, h0, dout0 = pl.pallas_call(
            functools.partial(step_kernel, (S, D, FF, HW, L)),
            name='block_grads',
            grid=(B,),
            in_specs=[per_seq(D), per_seq(D), const(emb.shape)] + [hbm] * 6,
            out_specs=[hbm] * 8,
            out_shape=[sds((12, UNIT, UNIT), F32)] + saved,
            scratch_shapes=[
                pltpu.VMEM(wo.shape, BF),
                pltpu.VMEM(wup.shape, BF),
                pltpu.VMEM(wdn.shape, BF),
                pltpu.VMEM((L, S, D), BF),
                pltpu.VMEM((T, D), BF),
                pltpu.VMEM((T, 3 * D), BF),
                pltpu.VMEM((L, NQ, S, NS * S), BF),
                pltpu.VMEM((L, NQ, 8, NS * S), F32),
                pltpu.VMEM((D, T), BF),
                pltpu.VMEM((L, S, D), BF),
                pltpu.VMEM((D, T), BF),
                pltpu.VMEM((T, FF), BF),
                pltpu.VMEM((T, FF), BF),
                pltpu.VMEM((T, D), BF),
                pltpu.VMEM((T, D), BF),
                pltpu.VMEM((S, D), BF),
                pltpu.VMEM((3 * D, D), BF),
                pltpu.VMEM((NQ, S, NS * S), BF),
                pltpu.VMEM((NQ, S, NS * S), BF),
                pltpu.VMEM((12, UNIT, UNIT), F32),
                pltpu.SemaphoreType.DMA((12,)),
                pltpu.SemaphoreType.DMA((6,)),
                pltpu.SemaphoreType.DMA((7,)),
            ],
            compiler_params=pltpu.CompilerParams(dimension_semantics=('arbitrary',), vmem_limit_bytes=VMEM_MAX),
        )(x, g, emb, *w_t, wo, wup, wdn)
        vmem = pl.BlockSpec(memory_space=pltpu.VMEM)
        outs = pl.pallas_call(
            functools.partial(reduce_kernel, (B, S, D, FF, HW)),
            name='attn_reduce',
            in_specs=[vmem, vmem] + [hbm] * 14,
            out_specs=[vmem] * 7,
            out_shape=[pltpu.VMEM(x.shape, BF), pltpu.VMEM((FF, D), F32), pltpu.VMEM((D, FF), F32)] + [pltpu.VMEM((D, D), F32)] * 4,
            scratch_shapes=[
                pltpu.VMEM((2, S, D), BF),
                pltpu.VMEM((2, S, 3 * D), BF),
                pltpu.VMEM((2, S, D), BF),
                pltpu.VMEM((2, D, S), BF),
                pltpu.VMEM((2, S, FF), BF),
                pltpu.VMEM((2, D, S), BF),
                pltpu.VMEM((2, S, D), BF),
                pltpu.VMEM((2, S, D), BF),
                pltpu.VMEM((3 * D, D), BF),
                pltpu.VMEM((D, FF), BF),
                pltpu.VMEM((FF, D), BF),
                pltpu.VMEM((S, FF), BF),
                pltpu.VMEM((B, S, D), BF),
                pltpu.VMEM((NQ, S, NS * S), BF),
                pltpu.VMEM((NQ, S, NS * S), BF),
                pltpu.VMEM((8, UNIT, UNIT), F32),
                pltpu.VMEM((8, 128, UNIT), F32),
                pltpu.VMEM((24, 128, UNIT), F32),
                pltpu.VMEM((24, 64, UNIT), F32),
                pltpu.VMEM((24, 32, UNIT), F32),
                pltpu.SemaphoreType.DMA((6, 24)),
                pltpu.SemaphoreType.DMA((6, 24)),
                pltpu.SemaphoreType.DMA((16,)),
                pltpu.SemaphoreType.DMA((5,)),
                pltpu.SemaphoreType.DMA((8, 2)),
            ],
            compiler_params=pltpu.CompilerParams(vmem_limit_bytes=VMEM_MAX - (16 << 20), collective_id=0, has_side_effects=True),
        )(emb, wo, x, qkv0, u0, mix0, z0, mT0, h0, dout0, *w_t, wup, wdn, acc)
        d_x, dn, up, gq, gk, gv, go = pl.pallas_call(
            store_kernel,
            name='store',
            in_specs=[vmem] * 7,
            out_specs=[hbm] * 7,
            out_shape=[sds(o.shape, o.dtype) for o in outs],
            scratch_shapes=[pltpu.SemaphoreType.DMA((7,))],
            compiler_params=pltpu.CompilerParams(vmem_limit_bytes=1 << 20),
        )(*outs)
        back = lambda a: a.reshape(H, HW, D).transpose(2, 0, 1)
        return back(gq), back(gk), back(gv), go.reshape(H, HW, D), up, dn, d_x

    return jax.shard_map(per_device, mesh=mesh, in_specs=(batch_spec, batch_spec, P(), P(), P(), P(), P(), P(), P()), out_specs=(P(), P(), P(), P(), P(), P(), batch_spec), check_vma=False)
```
